32 devices in a mesh: row: 4 (over y, core), col: 8 (over z, x).
Axes of the slice: x: 2, y: 2, z: 4, core: 2. Of those that a mesh axis runs over, the one named last changes fastest.
Arguments:
- values: bfloat16 [8192, 128], P('row'), may hold values from -30 to 30
- points0: bfloat16 [2, 8192], P(None, 'row'), may hold values from 0 to 1
- points1: bfloat16 [2, 2048], P(None, 'row'), may hold values from 0 to 1
- points2: bfloat16 [2, 256], P(None, 'row'), may hold values from 0 to 1
- tiles_a0: int32 [4, 8, 2, 48], P('row', 'col'), may hold values from 0 to 15, as said below
- tiles_e1: int32 [4, 8, 2, 20], P('row', 'col'), may hold values from 0 to 15, as said below
- tiles_a1: int32 [4, 8, 2, 4], P('row', 'col'), may hold values from 0 to 3, as said below
- factor: bfloat16 [256, 256], P('row', 'col'), as said below
Outputs:
- fine_coef: float32 [8192, 128], P(('row', 'col'))
- mid_coef: float32 [2048, 128], P('col')
- coarse_coef: float32 [256, 128], P('row')
- norms: float32 [1], replicated
The draws below stay inside these ranges and needn't reach their ends.
Inputs may be any that keep to these rules, and one draw needn't show every extreme that they name: `tiles_a0`: within each block the 48 listed tile pairs are distinct; tile rows are below 16 and tile columns below 8. `tiles_e1`: within each block the 20 listed tile pairs are distinct; tile rows are below 16 and tile columns below 2. `tiles_a1`: within each block the 4 listed tile pairs are distinct; tile rows are below 4 and tile columns below 2. `factor`: upper triangular; diagonal entries from 1 to 2.
All inputs are finite; a program needn't handle non-finite values.
Results may differ from the reference program's by a relative error of at most 0.0042.
Values may be sent and summed in bfloat16 or wider, within the bound.
A program may use at most 64 MiB of HBM per device.

```python
import jax
import jax.numpy as jnp
from jax import lax

TILE = 128
FIELDS = 128
N0 = 8192
N1 = 2048
N2 = 256
ROWS0 = 2048
COLS0 = 1024
ROWS1 = 512
COLS1 = 256
ROWS2 = 64
MAXT_A0 = 48
MAXT_E1 = 20
MAXT_A1 = 4
N_ROW = 4
N_COL = 8


def pick_tiles(key, stream, row_range, col_range, listed):
    subkeys = jax.random.split(jax.random.fold_in(key, stream), N_ROW * N_COL)

    def choose_one(subkey):
        return jax.random.permutation(subkey, row_range * col_range)[:listed]
    chosen = jax.vmap(choose_one)(subkeys).astype(jnp.int32)
    chosen = chosen.reshape(N_ROW, N_COL, 1, listed)
    return jnp.concatenate([chosen // col_range, chosen % col_range], axis=2)


def draw_values(key, part):
    base = jax.random.fold_in(key, 505)
    entry_key, row_key = jax.random.split(base)
    position = jnp.arange(N0, dtype=jnp.float32) / N0
    jitter = jnp.exp(jax.random.uniform(row_key, (N0,), jnp.float32, -0.22, 0.22))
    entries = jnp.clip(jax.random.normal(entry_key, (N0, FIELDS), jnp.float32), -6.0, 6.0)
    scale = jnp.exp(position * jnp.log(3.5)) * jitter
    return (entries * scale[:, None]).astype(jnp.bfloat16)


def draw_tiles_a0(key, part):
    return pick_tiles(key, 101, ROWS0 // TILE, COLS0 // TILE, MAXT_A0)


def draw_tiles_e1(key, part):
    return pick_tiles(key, 202, ROWS0 // TILE, COLS1 // TILE, MAXT_E1)


def draw_tiles_a1(key, part):
    return pick_tiles(key, 303, ROWS1 // TILE, COLS1 // TILE, MAXT_A1)


def draw_factor(key, part):
    base = jax.random.fold_in(key, 404)
    diag_key, upper_key = jax.random.split(base)
    index = jnp.arange(N2)
    upper = index[None, :] > index[:, None]
    spread = jax.random.normal(upper_key, (N2, N2), jnp.float32)
    diagonal = jax.random.uniform(diag_key, (N2,), jnp.float32, 1.0, 2.0)
    matrix = jnp.where(upper, spread * (0.6 / N2 ** 0.5), 0.0) + jnp.diag(diagonal)
    return matrix.astype(jnp.bfloat16)


def shard_levels(stream_key, extent, pieces, smallest, top_value):
    factor_of, own = 1.0, jax.random.fold_in(stream_key, 6)
    for dim, shards_of in pieces:
        steps = jnp.exp(jax.random.uniform(jax.random.fold_in(own, dim), (shards_of,), jnp.float32, smallest / len(pieces), top_value / len(pieces)))
        factor_of = factor_of * jnp.repeat(steps, extent[dim] // shards_of).reshape([-1 if axis == dim else 1 for axis in range(len(extent))])
    return factor_of


def setup_inputs(seed: int = 0) -> dict:
    key_of = jax.random.split(jax.random.key(seed), 9)
    return {
        "values": draw_values(jax.random.fold_in(key_of[8], 71), 0),
        "points0": jnp.clip(1.0 * jax.random.uniform(key_of[1], (2, N0), jnp.float32) ** shard_levels(key_of[1], (2, N0), ((1, 4),), -0.2, 0.2), 0.0, 1.0).astype(jnp.bfloat16),
        "points1": jnp.clip(1.0 * jax.random.uniform(key_of[2], (2, N1), jnp.float32) ** shard_levels(key_of[2], (2, N1), ((1, 4),), -0.2, 0.2), 0.0, 1.0).astype(jnp.bfloat16),
        "points2": jnp.clip(1.0 * jax.random.uniform(key_of[3], (2, N2), jnp.float32) ** shard_levels(key_of[3], (2, N2), ((1, 4),), -0.2, 0.2), 0.0, 1.0).astype(jnp.bfloat16),
        "tiles_a0": draw_tiles_a0(jax.random.fold_in(key_of[8], 71), 0),
        "tiles_e1": draw_tiles_e1(jax.random.fold_in(key_of[8], 71), 0),
        "tiles_a1": draw_tiles_a1(jax.random.fold_in(key_of[8], 71), 0),
        "factor": draw_factor(jax.random.fold_in(key_of[8], 71), 0),
    }


support_fine = 0.35
support_mid = 0.55
support_coarse = 0.8

def wendland(left_pts, right_pts, support):
    left = left_pts.astype(jnp.float32)
    right = right_pts.astype(jnp.float32)
    across = left[0][..., :, None] - right[0][..., None, :]
    upward = left[1][..., :, None] - right[1][..., None, :]
    ratio_t = jnp.sqrt(across * across + upward * upward) / support
    margin = jnp.maximum(1.0 - ratio_t, 0.0)
    squared = margin * margin
    return (squared * squared * (4.0 * ratio_t + 1.0)).astype(jnp.bfloat16)

def listed_all(row_pts, col_pts, listing, vector, support, flipped):
    row_tiles = row_pts.reshape(2, -1, TILE)
    col_tiles = col_pts.reshape(2, -1, TILE)
    rows_block = row_tiles.shape[1] // N_ROW
    cols_block = col_tiles.shape[1] // N_COL
    row_start = (jnp.arange(N_ROW, dtype=jnp.int32) * rows_block)[:, None, None]
    col_start = (jnp.arange(N_COL, dtype=jnp.int32) * cols_block)[None, :, None]
    global_rows = (listing[:, :, 0, :].astype(jnp.int32) + row_start).reshape(N_ROW * N_COL, -1)
    global_cols = (listing[:, :, 1, :].astype(jnp.int32) + col_start).reshape(N_ROW * N_COL, -1)
    fields = vector.shape[-1]
    inputs = vector.astype(jnp.float32).reshape(-1, TILE, fields)
    target = col_tiles.shape[1] if flipped else row_tiles.shape[1]
    total = jnp.zeros((target, TILE, fields), jnp.float32)

    def add_block(total, pair):
        tile_rows, tile_cols = pair
        kernel = wendland(row_tiles[:, tile_rows], col_tiles[:, tile_cols], support).astype(jnp.float32)
        if flipped:
            contrib = jnp.einsum('gij,gir->gjr', kernel, inputs[tile_rows])
            return (total.at[tile_cols].add(contrib), None)
        contrib = jnp.einsum('gij,gjr->gir', kernel, inputs[tile_cols])
        return (total.at[tile_rows].add(contrib), None)
    total, unused = lax.scan(add_block, total, (global_rows, global_cols))
    return total.reshape(-1, fields)

def reference(values, points0, points1, points2, tiles_a0, tiles_e1, tiles_a1, factor):
    scale_a0 = (ROWS0 / (N_COL * MAXT_A0 * TILE * TILE)) ** 0.5
    scale_e1 = (ROWS0 / (N_COL * MAXT_E1 * TILE * TILE)) ** 0.5
    scale_a1 = (ROWS1 / (N_COL * MAXT_A1 * TILE * TILE)) ** 0.5
    scale_e2 = (1.0 / N1) ** 0.5
    fine_data = values.astype(jnp.float32)
    fine_res = fine_data - 0.5 * (scale_a0 * listed_all(points0, points0, tiles_a0, values, support_fine, False))
    mid_data = scale_e1 * listed_all(points0, points1, tiles_e1, fine_res.astype(jnp.bfloat16), support_mid, True)
    mid_prod = (scale_a1 * listed_all(points1, points1, tiles_a1, mid_data.astype(jnp.bfloat16), support_mid, False)).astype(jnp.bfloat16)
    mid_res = mid_data - 0.5 * mid_prod.astype(jnp.float32)
    mid_low = mid_res.astype(jnp.bfloat16)
    coarse_blocks = points2.reshape(2, N_ROW, ROWS2).transpose(1, 0, 2)

    def restrict_block(block_pts):
        kernel = wendland(block_pts, points1, support_coarse)
        return jnp.dot(kernel, mid_low, preferred_element_type=jnp.float32)
    coarse_raw = lax.map(restrict_block, coarse_blocks).reshape(N2, -1)
    coarse_data = (scale_e2 * coarse_raw).astype(jnp.bfloat16)
    halfway = jnp.dot(factor.T, coarse_data, preferred_element_type=jnp.float32).astype(jnp.bfloat16)
    coarse_coef = jnp.dot(factor, halfway, preferred_element_type=jnp.float32)
    coarse_low = coarse_coef.astype(jnp.bfloat16).reshape(N_ROW, ROWS2, -1)

    def prolong_block(total, pair):
        block_pts, block_coef = pair
        kernel = wendland(block_pts, points1, support_coarse)
        return (total + jnp.dot(kernel.T, block_coef, preferred_element_type=jnp.float32), None)
    mid_corr, unused = lax.scan(prolong_block, jnp.zeros((N1, FIELDS), jnp.float32), (coarse_blocks, coarse_low))
    mid_coef = 0.5 * mid_data + scale_e2 * mid_corr
    fine_coef = 0.5 * fine_data + scale_e1 * listed_all(points0, points1, tiles_e1, mid_coef.astype(jnp.bfloat16), support_mid, False)
    norms = jnp.stack([jnp.mean(fine_res * fine_res)])
    return (fine_coef, mid_coef, coarse_coef, norms)
```

```python
import functools
import math

import jax
import jax.numpy as jnp
from jax import lax
from jax.experimental import pallas as pl
from jax.experimental.pallas import tpu as pltpu
from jax.sharding import PartitionSpec as P

TILE = 128


support_fine = 0.35
support_mid = 0.55
support_coarse = 0.8


def spread(x, axis, root):
    mine = lax.axis_index(axis) == root
    return lax.psum(jnp.where(mine, x, jnp.zeros_like(x)), axis)


def wendland(left_pts, right_pts, support):
    left = left_pts.astype(jnp.float32)
    right = right_pts.astype(jnp.float32)
    across = left[0][..., :, None] - right[0][..., None, :]
    upward = left[1][..., :, None] - right[1][..., None, :]
    ratio_t = jnp.sqrt(across * across + upward * upward) / support
    margin = jnp.maximum(1.0 - ratio_t, 0.0)
    squared = margin * margin
    return (squared * squared * (4.0 * ratio_t + 1.0)).astype(jnp.bfloat16)


def listed_terms(row_pts, col_pts, listing, vector, support, flipped):
    row_tiles = row_pts.reshape(2, -1, TILE)
    col_tiles = col_pts.reshape(2, -1, TILE)
    listed = listing.shape[-1]
    group = math.gcd(listed, 32)
    order = listing.reshape(2, listed // group, group)
    fields = vector.shape[-1]
    inputs = vector.reshape(-1, TILE, fields)
    target = col_tiles.shape[1] if flipped else row_tiles.shape[1]
    total = jnp.zeros((target, TILE, fields), jnp.float32)

    def add_group(total, pair):
        tile_rows, tile_cols = pair
        kernel = wendland(row_tiles[:, tile_rows], col_tiles[:, tile_cols], support)
        if flipped:
            contrib = jnp.einsum(
                "gij,gir->gjr", kernel, inputs[tile_rows], preferred_element_type=jnp.float32
            )
            return (total.at[tile_cols].add(contrib), None)
        contrib = jnp.einsum(
            "gij,gjr->gir", kernel, inputs[tile_cols], preferred_element_type=jnp.float32
        )
        return (total.at[tile_rows].add(contrib), None)

    total, unused = lax.scan(add_group, total, (order[0], order[1]))
    return total.reshape(-1, fields)


def per_device(values, points0, points1, points2, tiles_a0, tiles_e1, tiles_a1, factor):
    row_count = lax.axis_size("row")
    col_count = lax.axis_size("col")
    col_id = lax.axis_index("col")
    col_per_row = col_count // row_count
    rows_fine, fields = values.shape
    rows_mid = points1.shape[1]
    share = rows_fine // col_count
    cols_fine = rows_fine // col_per_row
    cols_mid = rows_mid // col_per_row
    source = col_id // col_per_row
    part_index = col_id % col_per_row
    value_piece = lax.dynamic_slice_in_dim(values, part_index * cols_fine, cols_fine, 0)
    fine_piece = lax.dynamic_slice_in_dim(points0, part_index * cols_fine, cols_fine, 1)
    mid_piece = lax.dynamic_slice_in_dim(points1, part_index * cols_mid, cols_mid, 1)
    value_cols, fine_cols, mid_cols = (
        spread(value_piece, "row", source),
        spread(fine_piece, "row", source),
        spread(mid_piece, "row", source),
    )
    scale_a0 = (rows_fine / (col_count * tiles_a0.shape[-1] * TILE * TILE)) ** 0.5
    scale_e1 = (rows_fine / (col_count * tiles_e1.shape[-1] * TILE * TILE)) ** 0.5
    scale_a1 = (rows_mid / (col_count * tiles_a1.shape[-1] * TILE * TILE)) ** 0.5
    scale_e2 = (1.0 / (rows_mid * row_count)) ** 0.5
    fine_data = values.astype(jnp.float32)
    own_data = lax.dynamic_slice_in_dim(values, col_id * share, share, 0).astype(jnp.float32)
    product_part = listed_terms(points0, fine_cols, tiles_a0[0, 0], value_cols, support_fine, False)
    product_whole = lax.psum(product_part, "col")
    fine_residual = fine_data - 0.5 * (scale_a0 * product_whole)
    fine_square = jnp.sum(fine_residual * fine_residual)
    restrict_part = listed_terms(
        points0, mid_cols, tiles_e1[0, 0], fine_residual.astype(jnp.bfloat16), support_mid, True
    )
    restrict_sum = lax.psum(restrict_part, "row")
    mid_data = scale_e1 * restrict_sum
    mid_part = listed_terms(
        points1, mid_cols, tiles_a1[0, 0], mid_data.astype(jnp.bfloat16), support_mid, False
    )
    mid_whole = (scale_a1 * lax.psum(mid_part, "col")).astype(jnp.bfloat16)
    mid_slice = lax.dynamic_slice_in_dim(mid_whole, part_index * cols_mid, cols_mid, 0)
    mid_turned = spread(mid_slice, "row", source)
    mid_residual = mid_data - 0.5 * mid_turned.astype(jnp.float32)
    coarse_kernel = wendland(points2, mid_cols, support_coarse)
    coarse_part = jnp.dot(
        coarse_kernel, mid_residual.astype(jnp.bfloat16), preferred_element_type=jnp.float32
    )
    coarse_sum = lax.psum(coarse_part, "col")
    coarse_data = (scale_e2 * coarse_sum).astype(jnp.bfloat16)
    halfway_part = lax.dot_general(
        factor, coarse_data, (((0,), (0,)), ((), ())), preferred_element_type=jnp.float32
    )
    halfway = lax.psum(halfway_part, "row").astype(jnp.bfloat16)
    coarse_part_two = jnp.dot(factor, halfway, preferred_element_type=jnp.float32)
    coarse_coef = lax.psum(coarse_part_two, "col")
    prolong_part = lax.dot_general(
        coarse_kernel,
        coarse_coef.astype(jnp.bfloat16),
        (((0,), (0,)), ((), ())),
        preferred_element_type=jnp.float32,
    )
    mid_coef = 0.5 * mid_data + scale_e2 * lax.psum(prolong_part, "row")
    fine_part = listed_terms(
        points0, mid_cols, tiles_e1[0, 0], mid_coef.astype(jnp.bfloat16), support_mid, False
    )
    fine_coef = 0.5 * own_data + scale_e1 * lax.psum_scatter(
        fine_part, "col", scatter_dimension=0, tiled=True
    )
    fine_total = lax.psum(fine_square / col_count, ("row", "col"))
    fine_norm = fine_total / (rows_fine * row_count * fields)
    return (fine_coef, mid_coef, coarse_coef, jnp.stack([fine_norm]))


FAR = 1024.0
CHUNKS = 4
MESH = pl.DeviceIdType.MESH


def phi_tile(cx, cy, rx, ry, inv_square):
    across = cx - rx
    upward = cy - ry
    square = (across * across + upward * upward) * inv_square
    t = square * lax.rsqrt(jnp.maximum(square, 1e-30))
    margin = jnp.maximum(1.0 - t, 0.0)
    squared = margin * margin
    return (squared * squared * (4.0 * t + 1.0)).astype(jnp.bfloat16)


def dot(a, b):
    return jnp.dot(a, b, preferred_element_type=jnp.float32)


def far_rows(tiles, row_tiles, col_tiles, by_col):
    row, col = tiles[0, 0, 0:1, :], tiles[0, 0, 1:2, :]
    key = col * row_tiles + row if by_col else row * col_tiles + col
    count = row_tiles * col_tiles
    place = lax.broadcasted_iota(jnp.int32, (count, key.shape[1]), 0)
    near = jnp.max(jnp.where(place == key, 1.0, 0.0), axis=1, keepdims=True)
    return jnp.broadcast_to(FAR * (1.0 - near), (count, TILE))


def halves(x):
    high = x.astype(jnp.bfloat16)
    return high, (x - high.astype(jnp.float32)).astype(jnp.bfloat16)


def cycle_kernel(g, vals_h, points0_h, points1_h, points2_h, tiles_a0_h, tiles_e1_h, tiles_a1_h, factor_h,
                 fine_o, mid_o, coarse_o, norm_o,
                 points0, points1, points2, tiles_a0, tiles_e1, tiles_a1, factor,
                 pts, offs, fac, offe, offa, ptsg, offg, facg, offag, gtg, vall, a0, e1own, e1t, e2t, a1t, cf, cm, cc2,
                 resg, part_buf, rsin, midc, mida, csend, crecv, cg, wcat, zcat, mcb,
                 l_s, p_m, o_m, f_m, oa_m, g_m, v_s, vy_r, vx_r, vg_r, vp_r, re_s, rez_r, rex_r,
                 rs_m, mc_m, mq_m, mf_s, mf_r, cr_m, ca_m):
    nr, nc, R0, R1, R2 = g["nr"], g["nc"], g["R0"], g["R1"], g["R2"]
    D = nr * nc
    T0, T1 = R0 // TILE, R1 // TILE
    C0, C1 = R0 * nr // nc, R1 * nr // nc
    B0, B1 = C0 // TILE, C1 // TILE
    S0 = R0 // nc
    I0 = S0 // TILE
    Q1 = C1 // nr
    N2 = g["N2"]
    CR = N2 // D
    NT1 = nr * T1
    NT2 = N2 // TILE
    X1, Y1, X2 = 2 * T0, 2 * T0 + T1, 2 * T0 + 2 * T1
    fine_inv, mid_inv, coarse_inv = (1.0 / (s * s) for s in (support_fine, support_mid, support_coarse))
    r = lax.axis_index("row")
    c = lax.axis_index("col")
    d = r * nc + c
    mate = r + 1 - 2 * lax.rem(r, 2)
    yp = lax.rem(r + 2, nr)
    diag = lax.rem(mate + 2, nr)
    h = lax.rem(c, 2)
    xp = c + 1 - 2 * h

    def rc(src, dst, ssem, rsem, rr, cc):
        return pltpu.make_async_remote_copy(src_ref=src, dst_ref=dst, send_sem=ssem, recv_sem=rsem,
                                            device_id=(rr, cc), device_id_type=MESH)

    def each(lo, hi, f):
        def body(k, carry):
            f(k)
            return carry
        lax.fori_loop(lo, hi, body, 0)

    barrier = pltpu.get_barrier_semaphore()

    def greet(k):
        q = lax.rem(c + k, nc)
        for j in range(nr):
            pl.semaphore_signal(barrier, inc=1, device_id=(lax.rem(r + j, nr), q), device_id_type=MESH)

    each(1, nc, greet)
    for j in range(1, nr):
        pl.semaphore_signal(barrier, inc=1, device_id=(lax.rem(r + j, nr), c), device_id_type=MESH)
    loads = [pltpu.make_async_copy(s, t, l_s.at[k]) for k, (s, t) in enumerate((
        (points0_h, points0), (points1_h, points1), (points2_h, points2), (tiles_a0_h, tiles_a0),
        (tiles_e1_h, tiles_e1), (tiles_a1_h, tiles_a1), (factor_h, factor), (vals_h, vall.at[r])))]
    for load in loads:
        load.start()

    pts[...] = jnp.zeros_like(pts)
    offs[...] = jnp.zeros_like(offs)
    for load in loads[:-1]:
        load.wait()
    for way in range(2):
        for ref, at, count in ((points0, way * T0, T0), (points1, X1 + way * T1, T1)):
            line = ref[way:way + 1, :].astype(jnp.float32)
            for k in range(count):
                pts[at + k:at + k + 1, :] = line[:, k * TILE:(k + 1) * TILE]
        line = points2[way:way + 1, :].astype(jnp.float32)
        blank = jnp.zeros((1, TILE - R2), jnp.float32)
        pts[X2 + way:X2 + way + 1, :] = jnp.concatenate([line, blank], axis=1)
        pts[X2 + 2 + way:X2 + 3 + way, :] = jnp.concatenate([blank, line], axis=1)
    far_a0 = far_rows(tiles_a0, T0, B0, False)
    far_e1 = far_rows(tiles_e1, T0, B1, False)
    for q in range(nc):
        offs[q, :I0 * B0] = far_a0[q * I0 * B0:(q + 1) * I0 * B0]
        offs[q, I0 * B0:I0 * (B0 + B1)] = far_e1[q * I0 * B1:(q + 1) * I0 * B1]
    half_of = lax.rem(r, TILE // R2)
    raw = factor[...].astype(jnp.float32)
    fac[...] = jnp.concatenate([jnp.where(half_of == k, raw, 0.0) for k in range(TILE // R2)], axis=1).astype(jnp.bfloat16)
    offe[...] = far_rows(tiles_e1, T0, B1, True)
    offa[...] = far_rows(tiles_a1, T1, B1, False)
    loads[-1].wait()
    pl.semaphore_wait(barrier, D - 1)

    def row_send(src_of, dst, m):
        for k in range(1, nr):
            q = lax.rem(r + k, nr)
            rc(src_of(q), dst, m.at[0], m.at[1], q, c).start()

    def row_wait(slots, m):
        rc(slots, slots, m.at[0], m.at[1], mate, c).wait()

    def col_send(src_of, dst, m):
        def go(k):
            q = lax.rem(c + k, nc)
            rc(src_of(q), dst, m.at[0], m.at[1], r, q).start()
        each(1, nc, go)

    HALF = R0 // 2
    CH = HALF // CHUNKS

    def chunk(half, q):
        return pl.ds(pl.multiple_of(half * HALF + q * CH, CH), CH)

    def y_copy(q):
        return rc(vall.at[r, chunk(h, q)], vall.at[r, chunk(h, q)], v_s.at[0], vy_r.at[q], yp, c)

    def y_in(q):
        return rc(vall.at[yp, chunk(h, q)], vall.at[yp, chunk(h, q)], v_s.at[0], vy_r.at[q], yp, c)

    def x_copy(q):
        return rc(vall.at[yp, chunk(h, q)], vall.at[yp, chunk(h, q)], v_s.at[0], vx_r.at[q], r, xp)

    def x_in(q):
        return rc(vall.at[yp, chunk(1 - h, q)], vall.at[yp, chunk(1 - h, q)], v_s.at[0], vx_r.at[q], r, xp)

    def g_copy(half, q):
        return rc(vall.at[yp, chunk(half, q)], vall.at[yp, chunk(half, q)], v_s.at[0], vg_r.at[0], mate, c)

    row_send(lambda q: pts, ptsg.at[r], p_m)
    col_send(lambda q: offs.at[q], offg.at[c], o_m)
    for q in range(CHUNKS):
        y_copy(q).start()
    rc(vall.at[r], vall.at[r], v_s.at[0], vp_r.at[0], mate, c).start()
    row_send(lambda q: offa, offag.at[r], oa_m)
    row_send(lambda q: fac, facg.at[r], f_m)
    ptsg[r] = pts[...]
    offg[c] = offs[c]
    offag[r] = offa[...]
    facg[r] = fac[...]

    def turned(row):
        return jnp.broadcast_to(row, (TILE, TILE)).T

    for i in range(I0):
        for way in range(2):
            cf[2 * i + way] = turned(pts[pl.ds(way * T0 + c * I0 + i, 1), :])
    row_wait(ptsg.at[pl.ds(0, nr - 1)], p_m)

    def turn_mid(k):
        for way in range(2):
            cm[k, way] = turned(ptsg[k // T1, pl.ds(X1 + way * T1 + lax.rem(k, T1), 1), :])
    each(0, NT1, turn_mid)
    rc(offg.at[pl.ds(0, nc - 1)], offg.at[pl.ds(0, nc - 1)], o_m.at[0], o_m.at[1], r, xp).wait()

    blocks = (r, mate, yp, diag)
    for s, rb in enumerate(blocks):
        def build_a0(kk, s=s, rb=rb):
            rx = ptsg[rb, pl.ds(kk, 1), :]
            ry = ptsg[rb, pl.ds(T0 + kk, 1), :]
            cb = rb * (nc // nr) + kk // B0
            j = lax.rem(kk, B0)
            for i in range(I0):
                off = offg[cb, pl.ds(i * B0 + j, 1), :]
                a0[s, i * TILE:(i + 1) * TILE, pl.ds(pl.multiple_of(kk * TILE, TILE), TILE)] = phi_tile(
                    cf[2 * i], cf[2 * i + 1], rx + off, ry, fine_inv)
        each(0, T0, build_a0)
        if s < CHUNKS:
            y_in(s).wait_recv()
            x_copy(s).start()
            g_copy(h, s).start()
    acc = dot(a0[0], vall[r])
    for q in range(CHUNKS):
        x_in(q).wait_recv()
        g_copy(1 - h, q).start()
    rc(vall.at[mate], vall.at[mate], v_s.at[0], vp_r.at[0], mate, c).wait_recv()
    acc = acc + dot(a0[1], vall[mate])
    acc = acc + dot(a0[2], vall[yp])
    rc(vall.at[diag], vall.at[diag], v_s.at[0], vg_r.at[0], mate, c).wait_recv()
    acc = acc + dot(a0[3], vall[diag])
    own_vals = vall[r, pl.ds(pl.multiple_of(c * S0, S0), S0), :].astype(jnp.float32)
    res = own_vals - (0.5 * g["scale_a0"]) * acc

    def res_at(q):
        return resg.at[pl.ds(pl.multiple_of(q * S0, S0), S0)]

    resg[pl.ds(pl.multiple_of(c * S0, S0), S0), :] = res.astype(jnp.bfloat16)
    for k in range(1, nc // 2):
        q = lax.rem(c + 2 * k, nc)
        rc(res_at(c), res_at(c), re_s.at[0], rez_r.at[nc // 2 - k], r, q).start()
    rc(res_at(c), res_at(c), re_s.at[0], rex_r.at[0], r, xp).start()

    def res_pass(k):
        q = lax.rem(c + 2 * k, nc)
        rc(res_at(q), res_at(q), re_s.at[0], rez_r.at[k], r, q).wait_recv()
        rc(res_at(q), res_at(q), re_s.at[0], rex_r.at[0], r, xp).start()

    def build_e1t(i):
        rx, ry = pts[pl.ds(i, 1), :], pts[pl.ds(T0 + i, 1), :]
        for j in range(B1):
            off = offe[pl.ds(j * T0 + i, 1), :]
            e1t[j * TILE:(j + 1) * TILE, pl.ds(pl.multiple_of(i * TILE, TILE), TILE)] = phi_tile(
                cm[c * B1 + j, 0], cm[c * B1 + j, 1], rx + off, ry, mid_inv)
    each(0, T0, build_e1t)
    row_wait(facg.at[pl.ds(0, nr - 1)], f_m)
    strips = []
    per = TILE // R2
    for lane in range(N2 // TILE):
        total = facg[lane * per].astype(jnp.float32)
        for k in range(1, per):
            total = total + facg[lane * per + k].astype(jnp.float32)
        strips.append(total)
    gtg[c] = jnp.concatenate(strips, axis=1).astype(jnp.bfloat16)
    col_send(lambda q: gtg.at[c], gtg.at[c], g_m)

    def coarse_row(t, way):
        return ptsg[per * t, X2 + way:X2 + way + 1, :] + ptsg[per * t + 1, X2 + 2 + way:X2 + 3 + way, :]

    for t in range(NT2):
        for way in range(2):
            cc2[2 * t + way] = jnp.broadcast_to(coarse_row(t, way), (8, TILE))
    res_pass(1)

    def build_e2t(k):
        for t in range(NT2):
            e2t[pl.ds(pl.multiple_of(k * TILE, TILE), TILE), t * TILE:(t + 1) * TILE] = phi_tile(
                cm[k, 0], cm[k, 1], cc2[2 * t, 0:1], cc2[2 * t + 1, 0:1], coarse_inv)
    each(0, NT1, build_e2t)
    res_pass(nc // 2 - 1)
    row_wait(offag.at[pl.ds(0, nr - 1)], oa_m)
    own_tile = c * B1 + (r * Q1) // TILE
    own_half = pl.ds(pl.multiple_of(lax.rem(r * Q1, TILE), Q1), Q1)
    ox, oy = cm[own_tile, 0, own_half, :], cm[own_tile, 1, own_half, :]

    def build_a1t(k):
        rx = ptsg[k // T1, pl.ds(X1 + lax.rem(k, T1), 1), :]
        ry = ptsg[k // T1, pl.ds(Y1 + lax.rem(k, T1), 1), :]
        off = offag[k // T1, pl.ds(lax.rem(k, T1) * B1 + (r * Q1) // TILE, 1), :]
        a1t[:, pl.ds(pl.multiple_of(k * TILE, TILE), TILE)] = phi_tile(ox, oy, rx + off, ry, mid_inv)
    each(0, NT1, build_a1t)
    own_mids = pl.ds(pl.multiple_of(c * C1 + r * Q1, Q1), Q1)
    turned_w = g["scale_e2"] * (e2t[own_mids, :].astype(jnp.float32)
                                - (0.5 * g["scale_a1"]) * dot(a1t[...], e2t[...]))
    w_high, w_low = halves(turned_w)
    w_pair = jnp.concatenate([w_high.astype(jnp.float32), w_low.astype(jnp.float32)], axis=0).T.astype(jnp.bfloat16)
    wcat[:, :TILE] = w_pair
    wcat[:, TILE:] = w_pair
    for k in range(2, nc // 2 - 1):
        res_pass(k)

    def build_e1own(k):
        rx = ptsg[k // T1, pl.ds(X1 + lax.rem(k, T1), 1), :]
        ry = ptsg[k // T1, pl.ds(Y1 + lax.rem(k, T1), 1), :]
        for i in range(I0):
            off = offg[k // B1, pl.ds(I0 * B0 + i * B1 + lax.rem(k, B1), 1), :]
            e1own[i * TILE:(i + 1) * TILE, pl.ds(pl.multiple_of(k * TILE, TILE), TILE)] = phi_tile(
                cf[2 * i], cf[2 * i + 1], rx + off, ry, mid_inv)
    each(0, NT1, build_e1own)

    rc(resg.at[pl.ds(0, (nc // 2) * S0)], resg.at[pl.ds(0, (nc // 2) * S0)], re_s.at[0], rex_r.at[0], r, xp).wait_recv()
    held = resg[...].astype(jnp.float32)
    square = jnp.sum((held * held).reshape(R0 // 8, 8, -1), axis=0)
    part_buf[...] = dot(e1t[...], resg[...]).reshape(nr, Q1, -1)
    row_send(lambda q: part_buf.at[q], rsin.at[r], rs_m)
    rsin[r] = part_buf[r]
    rc(gtg.at[pl.ds(0, nc - 1)], gtg.at[pl.ds(0, nc - 1)], g_m.at[0], g_m.at[1], r, xp).wait()
    gt = gtg[...].reshape(N2, N2)
    gg_high, gg_low = halves(dot(gt.astype(jnp.float32).T.astype(jnp.bfloat16), gt))
    zcat[2 * C1:, :N2] = gg_high
    zcat[2 * C1:, N2:] = gg_low
    h_high, h_low = halves((g["scale_e1"] * g["scale_e2"]) * dot(e1own[...], e2t[...]))
    steps = (dot(h_high, gg_high) + dot(h_low, gg_high) + dot(h_high, gg_low),)
    own_rows = pl.ds(pl.multiple_of(c * C1, C1), C1)
    rows_c = e2t[own_rows, :]
    steps += (g["scale_e2"] * (dot(rows_c, gg_high) + dot(rows_c, gg_low)),)
    for k, step in enumerate(steps):
        high, low = halves(step)
        zcat[k * C1:(k + 1) * C1, :N2] = high
        zcat[k * C1:(k + 1) * C1, N2:] = low

    row_wait(rsin.at[pl.ds(0, nr - 1)], rs_m)
    quarter = rsin[0]
    for k in range(1, nr):
        quarter = quarter + rsin[k]
    quarter = g["scale_e1"] * quarter
    q_high, q_low = halves(quarter)
    part = dot(wcat[...], jnp.concatenate([q_high, q_high, q_low, q_low], axis=0))
    csend[...] = part.reshape(D, CR, -1).astype(jnp.bfloat16)

    def all_send(src_of, dst, m):
        def go(k):
            q = lax.rem(c + k, nc)
            for j in range(nr):
                p = lax.rem(r + j, nr)
                rc(src_of(p * nc + q), dst, m.at[0], m.at[1], p, q).start()
        each(1, nc, go)
        for j in range(1, nr):
            p = lax.rem(r + j, nr)
            rc(src_of(p * nc + c), dst, m.at[0], m.at[1], p, c).start()

    def all_wait(ref, m):
        rc(ref.at[pl.ds(0, D - 1)], ref.at[pl.ds(0, D - 1)], m.at[0], m.at[1], mate, c).wait()

    all_send(lambda q: csend.at[q], crecv.at[d], cr_m)
    midc[r] = jnp.concatenate([quarter, square], axis=0)
    mida[r, c] = q_high
    col_send(lambda q: mida.at[r, c], mida.at[r, c], mq_m)
    row_send(lambda q: midc.at[r], midc.at[r], mc_m)
    crecv[d] = csend[d]
    rc(mida.at[r, pl.ds(0, nc - 1)], mida.at[r, pl.ds(0, nc - 1)], mq_m.at[0], mq_m.at[1], r, xp).wait()
    all_wait(crecv, cr_m)
    cg[d] = jnp.sum(crecv[...].astype(jnp.float32), axis=0).astype(jnp.bfloat16)
    all_send(lambda q: cg.at[d], cg.at[d], ca_m)
    rc(mida.at[r], mida.at[r], mf_s.at[0], mf_r.at[0], yp, c).start()
    rc(mida.at[r], mida.at[r], mf_s.at[0], mf_r.at[1], mate, c).start()
    row_wait(midc.at[pl.ds(0, nr - 1)], mc_m)
    norm_o[...] = jnp.broadcast_to(jnp.sum(jnp.sum(midc[:, Q1:], axis=0), keepdims=True) * g["norm_scale"], norm_o.shape)
    rc(mida.at[yp], mida.at[yp], mf_s.at[0], mf_r.at[0], yp, c).wait_recv()
    rc(mida.at[yp], mida.at[yp], mf_s.at[0], mf_r.at[2], mate, c).start()
    all_wait(cg, ca_m)
    cd = cg[...].astype(jnp.float32).reshape(N2, -1).astype(jnp.bfloat16)
    both = jnp.concatenate([cd, cd], axis=0)
    mid_o[...] = 0.5 * midc[:, :Q1].reshape(C1, -1) + dot(zcat[C1:2 * C1, :], both)
    coarse_o[...] = dot(zcat[pl.ds(pl.multiple_of(2 * C1 + r * R2, R2), R2), :], both)
    rc(mida.at[mate], mida.at[mate], mf_s.at[0], mf_r.at[1], mate, c).wait_recv()
    rc(mida.at[diag], mida.at[diag], mf_s.at[0], mf_r.at[2], mate, c).wait_recv()
    for q in range(nc):
        for k in range(nr):
            mcb[q * C1 + k * Q1:q * C1 + (k + 1) * Q1] = mida[k, q]
    fine_o[...] = (0.5 * own_vals + (0.5 * g["scale_e1"]) * dot(e1own[...], mcb[...])
                   + dot(zcat[:C1, :], both))
    rc(mida.at[pl.ds(0, nr - 1)], mida.at[pl.ds(0, nr - 1)], mf_s.at[0], mf_r.at[0], mate, c).wait_send()
    rc(vall.at[pl.ds(0, nr - 1)], vall.at[pl.ds(0, nr - 1)], v_s.at[0], vp_r.at[0], mate, c).wait_send()
    rc(resg.at[pl.ds(0, (nc - 1) * S0)], resg.at[pl.ds(0, (nc - 1) * S0)], re_s.at[0], rex_r.at[0], r, xp).wait_send()


def finish_kernel(fine, mid, coarse, norm, fine_o, mid_o, coarse_o, norm_o):
    fine_o[...] = fine[...]
    mid_o[...] = mid[...]
    coarse_o[...] = coarse[...]
    norm_o[...] = norm[0:1, 0:1]


def fits(nr, nc, R0, R1, R2):
    if nr != 4 or nc % nr or (nc // nr) % 2:
        return False
    if 4 * (R1 // nc) != 2 * TILE or R0 != R1 * nr or R0 % (nc * TILE) or (R1 * nr) % (nc * TILE) or R1 % TILE or 2 * R2 != TILE:
        return False
    if (nr * R2) % (nr * nc * 8) or (nr * R2) % TILE or (nc * TILE) % (nr * R2):
        return False
    return 2 * (R0 // nc) * R0 * nr <= 8 << 20


def fused(values, points0, points1, points2, tiles_a0, tiles_e1, tiles_a1, factor):
    nr, nc = lax.axis_size("row"), lax.axis_size("col")
    R0, R1, R2 = points0.shape[1], points1.shape[1], points2.shape[1]
    F = values.shape[-1]
    if not fits(nr, nc, R0, R1, R2) or F != TILE:
        return per_device(values, points0, points1, points2, tiles_a0, tiles_e1, tiles_a1, factor)
    D, N2 = nr * nc, nr * R2
    T0, T1 = R0 // TILE, R1 // TILE
    B0, B1 = R0 * nr // nc // TILE, R1 * nr // nc // TILE
    S0 = R0 // nc
    I0 = S0 // TILE
    C1, CR, Q1 = B1 * TILE, N2 // D, R1 * nr // nc // nr
    used = 2 * T0 + 2 * T1 + 4
    NP = -(-used // 8) * 8
    NO = I0 * (B0 + B1)
    NOP = -(-NO // 8) * 8
    g = dict(nr=nr, nc=nc, R0=R0, R1=R1, R2=R2, N2=N2,
             scale_a0=(R0 / (nc * tiles_a0.shape[-1] * TILE * TILE)) ** 0.5,
             scale_e1=(R0 / (nc * tiles_e1.shape[-1] * TILE * TILE)) ** 0.5,
             scale_a1=(R1 / (nc * tiles_a1.shape[-1] * TILE * TILE)) ** 0.5,
             scale_e2=(1.0 / (R1 * nr)) ** 0.5,
             norm_scale=1.0 / (R0 * nr * F))
    f32, bf16, i32 = jnp.float32, jnp.bfloat16, jnp.int32
    V = pltpu.VMEM
    dma = pltpu.SemaphoreType.DMA
    wide = N2 // nc
    scratch = [
        V(points0.shape, bf16), V(points1.shape, bf16), V(points2.shape, bf16),
        V(tiles_a0.shape, i32), V(tiles_e1.shape, i32), V(tiles_a1.shape, i32), V((wide, R2), bf16),
        V((NP, TILE), f32), V((nc, NOP, TILE), f32), V((wide, TILE), bf16), V((B1 * T0, TILE), f32), V((T1 * B1, TILE), f32),
        V((nr, NP, TILE), f32), V((nc, NOP, TILE), f32), V((nr, wide, TILE), bf16), V((nr, T1 * B1, TILE), f32),
        V((nc, wide, N2), bf16),
        V((nr, R0, F), bf16), V((nr, S0, R0), bf16), V((S0, nr * R1), bf16), V((C1, R0), bf16),
        V((nr * R1, N2), bf16), V((Q1, nr * R1), bf16),
        V((2 * I0, TILE, TILE), f32), V((nr * T1, 2, TILE, TILE), f32), V((2 * N2 // TILE, 8, TILE), f32),
        V((R0, F), bf16), V((nr, Q1, F), f32), V((nr, Q1, F), f32), V((nr, Q1 + 8, F), f32),
        V((nr, nc, Q1, F), bf16), V((D, CR, F), bf16), V((D, CR, F), bf16), V((D, CR, F), bf16),
        V((N2, 4 * Q1), bf16), V((2 * C1 + N2, 2 * N2), bf16), V((nr * R1, F), bf16),
    ]
    for n in (8, 2, 2, 2, 2, 2, 1, CHUNKS, CHUNKS, 1, 1, 1, nc // 2, 1, 2, 2, 2, 1, 3, 2, 2):
        scratch += [dma((n,))]
    vm = pl.BlockSpec(memory_space=pltpu.VMEM)
    shapes = ((S0, F), (C1, F), (R2, F))
    parts = pl.pallas_call(
        functools.partial(cycle_kernel, g),
        out_shape=tuple(jax.ShapeDtypeStruct(s, f32) for s in shapes + ((8, TILE),)),
        in_specs=[pl.BlockSpec(memory_space=pltpu.HBM)] * 8,
        out_specs=[vm] * 4,
        scratch_shapes=scratch,
        compiler_params=pltpu.CompilerParams(collective_id=0, has_side_effects=True, vmem_limit_bytes=48 << 20),
    )(values, points0, points1, points2, tiles_a0, tiles_e1, tiles_a1, factor.T)
    fine, mid, coarse, norm = pl.pallas_call(
        finish_kernel,
        grid=(1,),
        out_shape=tuple(jax.ShapeDtypeStruct(s, f32) for s in shapes + ((1, 1),)),
        in_specs=[vm] * 4,
        out_specs=[pl.BlockSpec(s, lambda i: (0, 0)) for s in shapes + ((1, 1),)],
    )(*parts)
    return (fine, mid, coarse, norm.reshape(1))


def solution(mesh):
    return jax.shard_map(
        fused,
        mesh=mesh,
        in_specs=(
            P("row", None),
            P(None, "row"),
            P(None, "row"),
            P(None, "row"),
            P("row", "col", None, None),
            P("row", "col", None, None),
            P("row", "col", None, None),
            P("row", "col"),
        ),
        out_specs=(P(("row", "col"), None), P("col", None), P("row", None), P()),
        check_vma=False,
    )
```

```python
import functools
import math

import jax
import jax.numpy as jnp
from jax import lax
from jax.experimental import pallas as pl
from jax.experimental.pallas import tpu as pltpu
from jax.sharding import PartitionSpec as P

TILE = 128


support_fine = 0.35
support_mid = 0.55
support_coarse = 0.8


def spread(x, axis, root):
    mine = lax.axis_index(axis) == root
    return lax.psum(jnp.where(mine, x, jnp.zeros_like(x)), axis)


def wendland(left_pts, right_pts, support):
    left = left_pts.astype(jnp.float32)
    right = right_pts.astype(jnp.float32)
    across = left[0][..., :, None] - right[0][..., None, :]
    upward = left[1][..., :, None] - right[1][..., None, :]
    ratio_t = jnp.sqrt(across * across + upward * upward) / support
    margin = jnp.maximum(1.0 - ratio_t, 0.0)
    squared = margin * margin
    return (squared * squared * (4.0 * ratio_t + 1.0)).astype(jnp.bfloat16)


def listed_terms(row_pts, col_pts, listing, vector, support, flipped):
    row_tiles = row_pts.reshape(2, -1, TILE)
    col_tiles = col_pts.reshape(2, -1, TILE)
    listed = listing.shape[-1]
    group = math.gcd(listed, 32)
    order = listing.reshape(2, listed // group, group)
    fields = vector.shape[-1]
    inputs = vector.reshape(-1, TILE, fields)
    target = col_tiles.shape[1] if flipped else row_tiles.shape[1]
    total = jnp.zeros((target, TILE, fields), jnp.float32)

    def add_group(total, pair):
        tile_rows, tile_cols = pair
        kernel = wendland(row_tiles[:, tile_rows], col_tiles[:, tile_cols], support)
        if flipped:
            contrib = jnp.einsum(
                "gij,gir->gjr", kernel, inputs[tile_rows], preferred_element_type=jnp.float32
            )
            return (total.at[tile_cols].add(contrib), None)
        contrib = jnp.einsum(
            "gij,gjr->gir", kernel, inputs[tile_cols], preferred_element_type=jnp.float32
        )
        return (total.at[tile_rows].add(contrib), None)

    total, unused = lax.scan(add_group, total, (order[0], order[1]))
    return total.reshape(-1, fields)


def per_device(values, points0, points1, points2, tiles_a0, tiles_e1, tiles_a1, factor):
    row_count = lax.axis_size("row")
    col_count = lax.axis_size("col")
    col_id = lax.axis_index("col")
    col_per_row = col_count // row_count
    rows_fine, fields = values.shape
    rows_mid = points1.shape[1]
    share = rows_fine // col_count
    cols_fine = rows_fine // col_per_row
    cols_mid = rows_mid // col_per_row
    source = col_id // col_per_row
    part_index = col_id % col_per_row
    value_piece = lax.dynamic_slice_in_dim(values, part_index * cols_fine, cols_fine, 0)
    fine_piece = lax.dynamic_slice_in_dim(points0, part_index * cols_fine, cols_fine, 1)
    mid_piece = lax.dynamic_slice_in_dim(points1, part_index * cols_mid, cols_mid, 1)
    value_cols, fine_cols, mid_cols = (
        spread(value_piece, "row", source),
        spread(fine_piece, "row", source),
        spread(mid_piece, "row", source),
    )
    scale_a0 = (rows_fine / (col_count * tiles_a0.shape[-1] * TILE * TILE)) ** 0.5
    scale_e1 = (rows_fine / (col_count * tiles_e1.shape[-1] * TILE * TILE)) ** 0.5
    scale_a1 = (rows_mid / (col_count * tiles_a1.shape[-1] * TILE * TILE)) ** 0.5
    scale_e2 = (1.0 / (rows_mid * row_count)) ** 0.5
    fine_data = values.astype(jnp.float32)
    own_data = lax.dynamic_slice_in_dim(values, col_id * share, share, 0).astype(jnp.float32)
    product_part = listed_terms(points0, fine_cols, tiles_a0[0, 0], value_cols, support_fine, False)
    product_whole = lax.psum(product_part, "col")
    fine_residual = fine_data - 0.5 * (scale_a0 * product_whole)
    fine_square = jnp.sum(fine_residual * fine_residual)
    restrict_part = listed_terms(
        points0, mid_cols, tiles_e1[0, 0], fine_residual.astype(jnp.bfloat16), support_mid, True
    )
    restrict_sum = lax.psum(restrict_part, "row")
    mid_data = scale_e1 * restrict_sum
    mid_part = listed_terms(
        points1, mid_cols, tiles_a1[0, 0], mid_data.astype(jnp.bfloat16), support_mid, False
    )
    mid_whole = (scale_a1 * lax.psum(mid_part, "col")).astype(jnp.bfloat16)
    mid_slice = lax.dynamic_slice_in_dim(mid_whole, part_index * cols_mid, cols_mid, 0)
    mid_turned = spread(mid_slice, "row", source)
    mid_residual = mid_data - 0.5 * mid_turned.astype(jnp.float32)
    coarse_kernel = wendland(points2, mid_cols, support_coarse)
    coarse_part = jnp.dot(
        coarse_kernel, mid_residual.astype(jnp.bfloat16), preferred_element_type=jnp.float32
    )
    coarse_sum = lax.psum(coarse_part, "col")
    coarse_data = (scale_e2 * coarse_sum).astype(jnp.bfloat16)
    halfway_part = lax.dot_general(
        factor, coarse_data, (((0,), (0,)), ((), ())), preferred_element_type=jnp.float32
    )
    halfway = lax.psum(halfway_part, "row").astype(jnp.bfloat16)
    coarse_part_two = jnp.dot(factor, halfway, preferred_element_type=jnp.float32)
    coarse_coef = lax.psum(coarse_part_two, "col")
    prolong_part = lax.dot_general(
        coarse_kernel,
        coarse_coef.astype(jnp.bfloat16),
        (((0,), (0,)), ((), ())),
        preferred_element_type=jnp.float32,
    )
    mid_coef = 0.5 * mid_data + scale_e2 * lax.psum(prolong_part, "row")
    fine_part = listed_terms(
        points0, mid_cols, tiles_e1[0, 0], mid_coef.astype(jnp.bfloat16), support_mid, False
    )
    fine_coef = 0.5 * own_data + scale_e1 * lax.psum_scatter(
        fine_part, "col", scatter_dimension=0, tiled=True
    )
    fine_total = lax.psum(fine_square / col_count, ("row", "col"))
    fine_norm = fine_total / (rows_fine * row_count * fields)
    return (fine_coef, mid_coef, coarse_coef, jnp.stack([fine_norm]))


FAR = 1024.0
CHUNKS = 4
MESH = pl.DeviceIdType.MESH


def phi_tile(cx, cy, rx, ry, inv_square):
    across = cx - rx
    upward = cy - ry
    square = (across * across + upward * upward) * inv_square
    t = square * lax.rsqrt(jnp.maximum(square, 1e-30))
    margin = jnp.maximum(1.0 - t, 0.0)
    squared = margin * margin
    return (squared * squared * (4.0 * t + 1.0)).astype(jnp.bfloat16)


def dot(a, b):
    return jnp.dot(a, b, preferred_element_type=jnp.float32)


def far_rows(tiles, row_tiles, col_tiles, by_col):
    row, col = tiles[0, 0, 0:1, :], tiles[0, 0, 1:2, :]
    key = col * row_tiles + row if by_col else row * col_tiles + col
    count = row_tiles * col_tiles
    place = lax.broadcasted_iota(jnp.int32, (count, key.shape[1]), 0)
    near = jnp.max(jnp.where(place == key, 1.0, 0.0), axis=1, keepdims=True)
    return jnp.broadcast_to(FAR * (1.0 - near), (count, TILE))


def halves(x):
    high = x.astype(jnp.bfloat16)
    return high, (x - high.astype(jnp.float32)).astype(jnp.bfloat16)


def cycle_kernel(g, vals_h, points0_h, points1_h, points2_h, tiles_a0_h, tiles_e1_h, tiles_a1_h, factor_h,
                 fine_o, mid_o, coarse_o, norm_o,
                 points0, points1, points2, tiles_a0, tiles_e1, tiles_a1, factor,
                 pts, offs, fac, offe, offa, ptsg, offg, facg, offag, gtg, vall, a0, e1own, e1t, e2t, a1t, cf, cm, cc2,
                 resg, part_buf, rsin, midc, mida, csend, crecv, cg, wcat, zcat, mcb,
                 l_s, p_m, o_m, f_m, oa_m, g_m, v_s, vy_r, vx_r, vg_r, vp_r, re_s, rez_r, rex_r,
                 rs_m, mc_m, mq_m, mf_s, mf_r, cr_m, ca_m):
    nr, nc, R0, R1, R2 = g["nr"], g["nc"], g["R0"], g["R1"], g["R2"]
    D = nr * nc
    T0, T1 = R0 // TILE, R1 // TILE
    C0, C1 = R0 * nr // nc, R1 * nr // nc
    B0, B1 = C0 // TILE, C1 // TILE
    S0 = R0 // nc
    I0 = S0 // TILE
    Q1 = C1 // nr
    N2 = g["N2"]
    CR = N2 // D
    NT1 = nr * T1
    NT2 = N2 // TILE
    X1, Y1, X2 = 2 * T0, 2 * T0 + T1, 2 * T0 + 2 * T1
    fine_inv, mid_inv, coarse_inv = (1.0 / (s * s) for s in (support_fine, support_mid, support_coarse))
    r = lax.axis_index("row")
    c = lax.axis_index("col")
    d = r * nc + c
    mate = r + 1 - 2 * lax.rem(r, 2)
    yp = lax.rem(r + 2, nr)
    diag = lax.rem(mate + 2, nr)
    h = lax.rem(c, 2)
    xp = c + 1 - 2 * h

    def rc(src, dst, ssem, rsem, rr, cc):
        return pltpu.make_async_remote_copy(src_ref=src, dst_ref=dst, send_sem=ssem, recv_sem=rsem,
                                            device_id=(rr, cc), device_id_type=MESH)

    def each(lo, hi, f):
        def body(k, carry):
            f(k)
            return carry
        lax.fori_loop(lo, hi, body, 0)

    barrier = pltpu.get_barrier_semaphore()

    def greet(k):
        q = lax.rem(c + k, nc)
        for j in range(nr):
            pl.semaphore_signal(barrier, inc=1, device_id=(lax.rem(r + j, nr), q), device_id_type=MESH)

    each(1, nc, greet)
    for j in range(1, nr):
        pl.semaphore_signal(barrier, inc=1, device_id=(lax.rem(r + j, nr), c), device_id_type=MESH)
    loads = [pltpu.make_async_copy(s, t, l_s.at[k]) for k, (s, t) in enumerate((
        (points0_h, points0), (points1_h, points1), (points2_h, points2), (tiles_a0_h, tiles_a0),
        (tiles_e1_h, tiles_e1), (tiles_a1_h, tiles_a1), (factor_h, factor), (vals_h, vall.at[r])))]
    for load in loads:
        load.start()

    pts[...] = jnp.zeros_like(pts)
    offs[...] = jnp.zeros_like(offs)
    for load in loads[:-1]:
        load.wait()
    for way in range(2):
        for ref, at, count in ((points0, way * T0, T0), (points1, X1 + way * T1, T1)):
            line = ref[way:way + 1, :].astype(jnp.float32)
            for k in range(count):
                pts[at + k:at + k + 1, :] = line[:, k * TILE:(k + 1) * TILE]
        line = points2[way:way + 1, :].astype(jnp.float32)
        blank = jnp.zeros((1, TILE - R2), jnp.float32)
        pts[X2 + way:X2 + way + 1, :] = jnp.concatenate([line, blank], axis=1)
        pts[X2 + 2 + way:X2 + 3 + way, :] = jnp.concatenate([blank, line], axis=1)
    far_a0 = far_rows(tiles_a0, T0, B0, False)
    far_e1 = far_rows(tiles_e1, T0, B1, False)
    for q in range(nc):
        offs[q, :I0 * B0] = far_a0[q * I0 * B0:(q + 1) * I0 * B0]
        offs[q, I0 * B0:I0 * (B0 + B1)] = far_e1[q * I0 * B1:(q + 1) * I0 * B1]
    half_of = lax.rem(r, TILE // R2)
    raw = factor[...].astype(jnp.float32)
    fac[...] = jnp.concatenate([jnp.where(half_of == k, raw, 0.0) for k in range(TILE // R2)], axis=1).astype(jnp.bfloat16)
    offe[...] = far_rows(tiles_e1, T0, B1, True)
    offa[...] = far_rows(tiles_a1, T1, B1, False)
    loads[-1].wait()
    pl.semaphore_wait(barrier, D - 1)

    def row_send(src_of, dst, m):
        for k in range(1, nr):
            q = lax.rem(r + k, nr)
            rc(src_of(q), dst, m.at[0], m.at[1], q, c).start()

    def row_wait(slots, m):
        rc(slots, slots, m.at[0], m.at[1], mate, c).wait()

    def col_send(src_of, dst, m):
        def go(k):
            q = lax.rem(c + k, nc)
            rc(src_of(q), dst, m.at[0], m.at[1], r, q).start()
        each(1, nc, go)

    HALF = R0 // 2
    CH = HALF // CHUNKS

    def chunk(half, q):
        return pl.ds(pl.multiple_of(half * HALF + q * CH, CH), CH)

    def y_copy(q):
        return rc(vall.at[r, chunk(h, q)], vall.at[r, chunk(h, q)], v_s.at[0], vy_r.at[q], yp, c)

    def y_in(q):
        return rc(vall.at[yp, chunk(h, q)], vall.at[yp, chunk(h, q)], v_s.at[0], vy_r.at[q], yp, c)

    def x_copy(q):
        return rc(vall.at[yp, chunk(h, q)], vall.at[yp, chunk(h, q)], v_s.at[0], vx_r.at[q], r, xp)

    def x_in(q):
        return rc(vall.at[yp, chunk(1 - h, q)], vall.at[yp, chunk(1 - h, q)], v_s.at[0], vx_r.at[q], r, xp)

    def g_copy(half, q):
        return rc(vall.at[yp, chunk(half, q)], vall.at[yp, chunk(half, q)], v_s.at[0], vg_r.at[0], mate, c)

    row_send(lambda q: pts, ptsg.at[r], p_m)
    col_send(lambda q: offs.at[q], offg.at[c], o_m)
    for q in range(CHUNKS):
        y_copy(q).start()
    rc(vall.at[r], vall.at[r], v_s.at[0], vp_r.at[0], mate, c).start()
    row_send(lambda q: offa, offag.at[r], oa_m)
    row_send(lambda q: fac, facg.at[r], f_m)
    ptsg[r] = pts[...]
    offg[c] = offs[c]
    offag[r] = offa[...]
    facg[r] = fac[...]

    def turned(row):
        return jnp.broadcast_to(row, (TILE, TILE)).T

    for i in range(I0):
        for way in range(2):
            cf[2 * i + way] = turned(pts[pl.ds(way * T0 + c * I0 + i, 1), :])
    row_wait(ptsg.at[pl.ds(0, nr - 1)], p_m)

    def turn_mid(k):
        for way in range(2):
            cm[k, way] = turned(ptsg[k // T1, pl.ds(X1 + way * T1 + lax.rem(k, T1), 1), :])
    each(0, NT1, turn_mid)
    rc(offg.at[pl.ds(0, nc - 1)], offg.at[pl.ds(0, nc - 1)], o_m.at[0], o_m.at[1], r, xp).wait()

    blocks = (r, mate, yp, diag)
    for s, rb in enumerate(blocks):
        def build_a0(kk, s=s, rb=rb):
            rx = ptsg[rb, pl.ds(kk, 1), :]
            ry = ptsg[rb, pl.ds(T0 + kk, 1), :]
            cb = rb * (nc // nr) + kk // B0
            j = lax.rem(kk, B0)
            for i in range(I0):
                off = offg[cb, pl.ds(i * B0 + j, 1), :]
                a0[s, i * TILE:(i + 1) * TILE, pl.ds(pl.multiple_of(kk * TILE, TILE), TILE)] = phi_tile(
                    cf[2 * i], cf[2 * i + 1], rx + off, ry, fine_inv)
        each(0, T0, build_a0)
        if s < CHUNKS:
            y_in(s).wait_recv()
            x_copy(s).start()
            g_copy(h, s).start()
    acc = dot(a0[0], vall[r])
    for q in range(CHUNKS):
        x_in(q).wait_recv()
        g_copy(1 - h, q).start()
    rc(vall.at[mate], vall.at[mate], v_s.at[0], vp_r.at[0], mate, c).wait_recv()
    acc = acc + dot(a0[1], vall[mate])
    acc = acc + dot(a0[2], vall[yp])
    rc(vall.at[diag], vall.at[diag], v_s.at[0], vg_r.at[0], mate, c).wait_recv()
    acc = acc + dot(a0[3], vall[diag])
    own_vals = vall[r, pl.ds(pl.multiple_of(c * S0, S0), S0), :].astype(jnp.float32)
    res = own_vals - (0.5 * g["scale_a0"]) * acc

    def res_at(q):
        return resg.at[pl.ds(pl.multiple_of(q * S0, S0), S0)]

    resg[pl.ds(pl.multiple_of(c * S0, S0), S0), :] = res.astype(jnp.bfloat16)
    for k in range(1, nc // 2):
        q = lax.rem(c + 2 * k, nc)
        rc(res_at(c), res_at(c), re_s.at[0], rez_r.at[nc // 2 - k], r, q).start()
    rc(res_at(c), res_at(c), re_s.at[0], rex_r.at[0], r, xp).start()

    def res_pass(k):
        q = lax.rem(c + 2 * k, nc)
        rc(res_at(q), res_at(q), re_s.at[0], rez_r.at[k], r, q).wait_recv()
        rc(res_at(q), res_at(q), re_s.at[0], rex_r.at[0], r, xp).start()

    def build_e1t(i):
        rx, ry = pts[pl.ds(i, 1), :], pts[pl.ds(T0 + i, 1), :]
        for j in range(B1):
            off = offe[pl.ds(j * T0 + i, 1), :]
            e1t[j * TILE:(j + 1) * TILE, pl.ds(pl.multiple_of(i * TILE, TILE), TILE)] = phi_tile(
                cm[c * B1 + j, 0], cm[c * B1 + j, 1], rx + off, ry, mid_inv)
    each(0, T0, build_e1t)
    row_wait(facg.at[pl.ds(0, nr - 1)], f_m)
    strips = []
    per = TILE // R2
    for lane in range(N2 // TILE):
        total = facg[lane * per].astype(jnp.float32)
        for k in range(1, per):
            total = total + facg[lane * per + k].astype(jnp.float32)
        strips.append(total)
    gtg[c] = jnp.concatenate(strips, axis=1).astype(jnp.bfloat16)
    col_send(lambda q: gtg.at[c], gtg.at[c], g_m)

    def coarse_row(t, way):
        return ptsg[per * t, X2 + way:X2 + way + 1, :] + ptsg[per * t + 1, X2 + 2 + way:X2 + 3 + way, :]

    for t in range(NT2):
        for way in range(2):
            cc2[2 * t + way] = jnp.broadcast_to(coarse_row(t, way), (8, TILE))
    res_pass(1)

    def build_e2t(k):
        for t in range(NT2):
            e2t[pl.ds(pl.multiple_of(k * TILE, TILE), TILE), t * TILE:(t + 1) * TILE] = phi_tile(
                cm[k, 0], cm[k, 1], cc2[2 * t, 0:1], cc2[2 * t + 1, 0:1], coarse_inv)
    each(0, NT1, build_e2t)
    res_pass(nc // 2 - 1)
    row_wait(offag.at[pl.ds(0, nr - 1)], oa_m)
    own_tile = c * B1 + (r * Q1) // TILE
    own_half = pl.ds(pl.multiple_of(lax.rem(r * Q1, TILE), Q1), Q1)
    ox, oy = cm[own_tile, 0, own_half, :], cm[own_tile, 1, own_half, :]

    def build_a1t(k):
        rx = ptsg[k // T1, pl.ds(X1 + lax.rem(k, T1), 1), :]
        ry = ptsg[k // T1, pl.ds(Y1 + lax.rem(k, T1), 1), :]
        off = offag[k // T1, pl.ds(lax.rem(k, T1) * B1 + (r * Q1) // TILE, 1), :]
        a1t[:, pl.ds(pl.multiple_of(k * TILE, TILE), TILE)] = phi_tile(ox, oy, rx + off, ry, mid_inv)
    each(0, NT1, build_a1t)
    own_mids = pl.ds(pl.multiple_of(c * C1 + r * Q1, Q1), Q1)
    turned_w = g["scale_e2"] * (e2t[own_mids, :].astype(jnp.float32)
                                - (0.5 * g["scale_a1"]) * dot(a1t[...], e2t[...]))
    w_high, w_low = halves(turned_w)
    w_pair = jnp.concatenate([w_high.astype(jnp.float32), w_low.astype(jnp.float32)], axis=0).T.astype(jnp.bfloat16)
    wcat[:, :TILE] = w_pair
    wcat[:, TILE:] = w_pair
    for k in range(2, nc // 2 - 1):
        res_pass(k)

    def build_e1own(k):
        rx = ptsg[k // T1, pl.ds(X1 + lax.rem(k, T1), 1), :]
        ry = ptsg[k // T1, pl.ds(Y1 + lax.rem(k, T1), 1), :]
        for i in range(I0):
            off = offg[k // B1, pl.ds(I0 * B0 + i * B1 + lax.rem(k, B1), 1), :]
            e1own[i * TILE:(i + 1) * TILE, pl.ds(pl.multiple_of(k * TILE, TILE), TILE)] = phi_tile(
                cf[2 * i], cf[2 * i + 1], rx + off, ry, mid_inv)
    each(0, NT1, build_e1own)

    rc(resg.at[pl.ds(0, (nc // 2) * S0)], resg.at[pl.ds(0, (nc // 2) * S0)], re_s.at[0], rex_r.at[0], r, xp).wait_recv()
    held = resg[...].astype(jnp.float32)
    square = jnp.sum((held * held).reshape(R0 // 8, 8, -1), axis=0)
    part_buf[...] = dot(e1t[...], resg[...]).reshape(nr, Q1, -1)
    row_send(lambda q: part_buf.at[q], rsin.at[r], rs_m)
    rsin[r] = part_buf[r]
    rc(gtg.at[pl.ds(0, nc - 1)], gtg.at[pl.ds(0, nc - 1)], g_m.at[0], g_m.at[1], r, xp).wait()
    gt = gtg[...].reshape(N2, N2)
    gg_high, gg_low = halves(dot(gt.astype(jnp.float32).T.astype(jnp.bfloat16), gt))
    zcat[2 * C1:, :N2] = gg_high
    zcat[2 * C1:, N2:] = gg_low
    h_high, h_low = halves((g["scale_e1"] * g["scale_e2"]) * dot(e1own[...], e2t[...]))
    steps = (dot(h_high, gg_high) + dot(h_low, gg_high) + dot(h_high, gg_low),)
    own_rows = pl.ds(pl.multiple_of(c * C1, C1), C1)
    rows_c = e2t[own_rows, :]
    steps += (g["scale_e2"] * (dot(rows_c, gg_high) + dot(rows_c, gg_low)),)
    for k, step in enumerate(steps):
        high, low = halves(step)
        zcat[k * C1:(k + 1) * C1, :N2] = high
        zcat[k * C1:(k + 1) * C1, N2:] = low

    row_wait(rsin.at[pl.ds(0, nr - 1)], rs_m)
    quarter = rsin[0]
    for k in range(1, nr):
        quarter = quarter + rsin[k]
    quarter = g["scale_e1"] * quarter
    q_high, q_low = halves(quarter)
    part = dot(wcat[...], jnp.concatenate([q_high, q_high, q_low, q_low], axis=0))
    csend[...] = part.reshape(D, CR, -1).astype(jnp.bfloat16)

    def all_send(src_of, dst, m):
        def go(k):
            q = lax.rem(c + k, nc)
            for j in range(nr):
                p = lax.rem(r + j, nr)
                rc(src_of(p * nc + q), dst, m.at[0], m.at[1], p, q).start()
        each(1, nc, go)
        for j in range(1, nr):
            p = lax.rem(r + j, nr)
            rc(src_of(p * nc + c), dst, m.at[0], m.at[1], p, c).start()

    def all_wait(ref, m):
        rc(ref.at[pl.ds(0, D - 1)], ref.at[pl.ds(0, D - 1)], m.at[0], m.at[1], mate, c).wait()

    all_send(lambda q: csend.at[q], crecv.at[d], cr_m)
    midc[r] = jnp.concatenate([quarter, square], axis=0)
    mida[r, c] = q_high
    col_send(lambda q: mida.at[r, c], mida.at[r, c], mq_m)
    row_send(lambda q: midc.at[r], midc.at[r], mc_m)
    crecv[d] = csend[d]
    rc(mida.at[r, pl.ds(0, nc - 1)], mida.at[r, pl.ds(0, nc - 1)], mq_m.at[0], mq_m.at[1], r, xp).wait()
    all_wait(crecv, cr_m)
    cg[d] = jnp.sum(crecv[...].astype(jnp.float32), axis=0).astype(jnp.bfloat16)
    all_send(lambda q: cg.at[d], cg.at[d], ca_m)
    rc(mida.at[r], mida.at[r], mf_s.at[0], mf_r.at[0], yp, c).start()
    rc(mida.at[r], mida.at[r], mf_s.at[0], mf_r.at[1], mate, c).start()
    row_wait(midc.at[pl.ds(0, nr - 1)], mc_m)
    norm_o[...] = jnp.broadcast_to(jnp.sum(jnp.sum(midc[:, Q1:], axis=0), keepdims=True) * g["norm_scale"], norm_o.shape)
    rc(mida.at[yp], mida.at[yp], mf_s.at[0], mf_r.at[0], yp, c).wait_recv()
    rc(mida.at[yp], mida.at[yp], mf_s.at[0], mf_r.at[2], mate, c).start()
    all_wait(cg, ca_m)
    cd = cg[...].astype(jnp.float32).reshape(N2, -1).astype(jnp.bfloat16)
    both = jnp.concatenate([cd, cd], axis=0)
    mid_o[...] = 0.5 * midc[:, :Q1].reshape(C1, -1) + dot(zcat[C1:2 * C1, :], both)
    coarse_o[...] = dot(zcat[pl.ds(pl.multiple_of(2 * C1 + r * R2, R2), R2), :], both)
    rc(mida.at[mate], mida.at[mate], mf_s.at[0], mf_r.at[1], mate, c).wait_recv()
    rc(mida.at[diag], mida.at[diag], mf_s.at[0], mf_r.at[2], mate, c).wait_recv()
    for q in range(nc):
        for k in range(nr):
            mcb[q * C1 + k * Q1:q * C1 + (k + 1) * Q1] = mida[k, q]
    fine_o[...] = (0.5 * own_vals + (0.5 * g["scale_e1"]) * dot(e1own[...], mcb[...])
                   + dot(zcat[:C1, :], both))
    rc(mida.at[pl.ds(0, nr - 1)], mida.at[pl.ds(0, nr - 1)], mf_s.at[0], mf_r.at[0], mate, c).wait_send()
    rc(vall.at[pl.ds(0, nr - 1)], vall.at[pl.ds(0, nr - 1)], v_s.at[0], vp_r.at[0], mate, c).wait_send()
    rc(resg.at[pl.ds(0, (nc - 1) * S0)], resg.at[pl.ds(0, (nc - 1) * S0)], re_s.at[0], rex_r.at[0], r, xp).wait_send()


def finish_kernel(fine, mid, coarse, norm, fine_o, mid_o, coarse_o, norm_o):
    fine_o[...] = fine[...]
    mid_o[...] = mid[...]
    coarse_o[...] = coarse[...]
    norm_o[...] = norm[0:1, 0:1]


def fits(nr, nc, R0, R1, R2):
    if nr != 4 or nc % nr or (nc // nr) % 2:
        return False
    if 4 * (R1 // nc) != 2 * TILE or R0 != R1 * nr or R0 % (nc * TILE) or (R1 * nr) % (nc * TILE) or R1 % TILE or 2 * R2 != TILE:
        return False
    if (nr * R2) % (nr * nc * 8) or (nr * R2) % TILE or (nc * TILE) % (nr * R2):
        return False
    return 2 * (R0 // nc) * R0 * nr <= 8 << 20


def fused(values, points0, points1, points2, tiles_a0, tiles_e1, tiles_a1, factor):
    nr, nc = lax.axis_size("row"), lax.axis_size("col")
    R0, R1, R2 = points0.shape[1], points1.shape[1], points2.shape[1]
    F = values.shape[-1]
    if not fits(nr, nc, R0, R1, R2) or F != TILE:
        return per_device(values, points0, points1, points2, tiles_a0, tiles_e1, tiles_a1, factor)
    D, N2 = nr * nc, nr * R2
    T0, T1 = R0 // TILE, R1 // TILE
    B0, B1 = R0 * nr // nc // TILE, R1 * nr // nc // TILE
    S0 = R0 // nc
    I0 = S0 // TILE
    C1, CR, Q1 = B1 * TILE, N2 // D, R1 * nr // nc // nr
    used = 2 * T0 + 2 * T1 + 4
    NP = -(-used // 8) * 8
    NO = I0 * (B0 + B1)
    NOP = -(-NO // 8) * 8
    g = dict(nr=nr, nc=nc, R0=R0, R1=R1, R2=R2, N2=N2,
             scale_a0=(R0 / (nc * tiles_a0.shape[-1] * TILE * TILE)) ** 0.5,
             scale_e1=(R0 / (nc * tiles_e1.shape[-1] * TILE * TILE)) ** 0.5,
             scale_a1=(R1 / (nc * tiles_a1.shape[-1] * TILE * TILE)) ** 0.5,
             scale_e2=(1.0 / (R1 * nr)) ** 0.5,
             norm_scale=1.0 / (R0 * nr * F))
    f32, bf16, i32 = jnp.float32, jnp.bfloat16, jnp.int32
    V = pltpu.VMEM
    dma = pltpu.SemaphoreType.DMA
    wide = N2 // nc
    scratch = [
        V(points0.shape, bf16), V(points1.shape, bf16), V(points2.shape, bf16),
        V(tiles_a0.shape, i32), V(tiles_e1.shape, i32), V(tiles_a1.shape, i32), V((wide, R2), bf16),
        V((NP, TILE), f32), V((nc, NOP, TILE), f32), V((wide, TILE), bf16), V((B1 * T0, TILE), f32), V((T1 * B1, TILE), f32),
        V((nr, NP, TILE), f32), V((nc, NOP, TILE), f32), V((nr, wide, TILE), bf16), V((nr, T1 * B1, TILE), f32),
        V((nc, wide, N2), bf16),
        V((nr, R0, F), bf16), V((nr, S0, R0), bf16), V((S0, nr * R1), bf16), V((C1, R0), bf16),
        V((nr * R1, N2), bf16), V((Q1, nr * R1), bf16),
        V((2 * I0, TILE, TILE), f32), V((nr * T1, 2, TILE, TILE), f32), V((2 * N2 // TILE, 8, TILE), f32),
        V((R0, F), bf16), V((nr, Q1, F), f32), V((nr, Q1, F), f32), V((nr, Q1 + 8, F), f32),
        V((nr, nc, Q1, F), bf16), V((D, CR, F), bf16), V((D, CR, F), bf16), V((D, CR, F), bf16),
        V((N2, 4 * Q1), bf16), V((2 * C1 + N2, 2 * N2), bf16), V((nr * R1, F), bf16),
    ]
    for n in (8, 2, 2, 2, 2, 2, 1, CHUNKS, CHUNKS, 1, 1, 1, nc // 2, 1, 2, 2, 2, 1, 3, 2, 2):
        scratch += [dma((n,))]
    vm = pl.BlockSpec(memory_space=pltpu.VMEM)
    shapes = ((S0, F), (C1, F), (R2, F))
    parts = pl.pallas_call(
        functools.partial(cycle_kernel, g),
        out_shape=tuple(jax.ShapeDtypeStruct(s, f32) for s in shapes + ((8, TILE),)),
        in_specs=[pl.BlockSpec(memory_space=pltpu.HBM)] * 8,
        out_specs=[vm] * 4,
        scratch_shapes=scratch,
        compiler_params=pltpu.CompilerParams(collective_id=0, has_side_effects=True, vmem_limit_bytes=48 << 20),
    )(*[pltpu.with_memory_space_constraint(x, pltpu.HBM) for x in (
        values, points0, points1, points2, tiles_a0, tiles_e1, tiles_a1, factor.T)])
    fine, mid, coarse, norm = pl.pallas_call(
        finish_kernel,
        grid=(1,),
        out_shape=tuple(jax.ShapeDtypeStruct(s, f32) for s in shapes + ((1, 1),)),
        in_specs=[vm] * 4,
        out_specs=[pl.BlockSpec(s, lambda i: (0, 0)) for s in shapes + ((1, 1),)],
        compiler_params=pltpu.CompilerParams(vmem_limit_bytes=4 << 20),
    )(*parts)
    return (fine, mid, coarse, norm.reshape(1))


def solution(mesh):
    return jax.shard_map(
        fused,
        mesh=mesh,
        in_specs=(
            P("row", None),
            P(None, "row"),
            P(None, "row"),
            P(None, "row"),
            P("row", "col", None, None),
            P("row", "col", None, None),
            P("row", "col", None, None),
            P("row", "col"),
        ),
        out_specs=(P(("row", "col"), None), P("col", None), P("row", None), P()),
        check_vma=False,
    )
```

```python
import functools
import math

import jax
import jax.numpy as jnp
from jax import lax
from jax.experimental import pallas as pl
from jax.experimental.pallas import tpu as pltpu
from jax.sharding import PartitionSpec as P

TILE = 128


support_fine = 0.35
support_mid = 0.55
support_coarse = 0.8


def spread(x, axis, root):
    mine = lax.axis_index(axis) == root
    return lax.psum(jnp.where(mine, x, jnp.zeros_like(x)), axis)


def wendland(left_pts, right_pts, support):
    left = left_pts.astype(jnp.float32)
    right = right_pts.astype(jnp.float32)
    across = left[0][..., :, None] - right[0][..., None, :]
    upward = left[1][..., :, None] - right[1][..., None, :]
    ratio_t = jnp.sqrt(across * across + upward * upward) / support
    margin = jnp.maximum(1.0 - ratio_t, 0.0)
    squared = margin * margin
    return (squared * squared * (4.0 * ratio_t + 1.0)).astype(jnp.bfloat16)


def listed_terms(row_pts, col_pts, listing, vector, support, flipped):
    row_tiles = row_pts.reshape(2, -1, TILE)
    col_tiles = col_pts.reshape(2, -1, TILE)
    listed = listing.shape[-1]
    group = math.gcd(listed, 32)
    order = listing.reshape(2, listed // group, group)
    fields = vector.shape[-1]
    inputs = vector.reshape(-1, TILE, fields)
    target = col_tiles.shape[1] if flipped else row_tiles.shape[1]
    total = jnp.zeros((target, TILE, fields), jnp.float32)

    def add_group(total, pair):
        tile_rows, tile_cols = pair
        kernel = wendland(row_tiles[:, tile_rows], col_tiles[:, tile_cols], support)
        if flipped:
            contrib = jnp.einsum(
                "gij,gir->gjr", kernel, inputs[tile_rows], preferred_element_type=jnp.float32
            )
            return (total.at[tile_cols].add(contrib), None)
        contrib = jnp.einsum(
            "gij,gjr->gir", kernel, inputs[tile_cols], preferred_element_type=jnp.float32
        )
        return (total.at[tile_rows].add(contrib), None)

    total, unused = lax.scan(add_group, total, (order[0], order[1]))
    return total.reshape(-1, fields)


def per_device(values, points0, points1, points2, tiles_a0, tiles_e1, tiles_a1, factor):
    row_count = lax.axis_size("row")
    col_count = lax.axis_size("col")
    col_id = lax.axis_index("col")
    col_per_row = col_count // row_count
    rows_fine, fields = values.shape
    rows_mid = points1.shape[1]
    share = rows_fine // col_count
    cols_fine = rows_fine // col_per_row
    cols_mid = rows_mid // col_per_row
    source = col_id // col_per_row
    part_index = col_id % col_per_row
    value_piece = lax.dynamic_slice_in_dim(values, part_index * cols_fine, cols_fine, 0)
    fine_piece = lax.dynamic_slice_in_dim(points0, part_index * cols_fine, cols_fine, 1)
    mid_piece = lax.dynamic_slice_in_dim(points1, part_index * cols_mid, cols_mid, 1)
    value_cols, fine_cols, mid_cols = (
        spread(value_piece, "row", source),
        spread(fine_piece, "row", source),
        spread(mid_piece, "row", source),
    )
    scale_a0 = (rows_fine / (col_count * tiles_a0.shape[-1] * TILE * TILE)) ** 0.5
    scale_e1 = (rows_fine / (col_count * tiles_e1.shape[-1] * TILE * TILE)) ** 0.5
    scale_a1 = (rows_mid / (col_count * tiles_a1.shape[-1] * TILE * TILE)) ** 0.5
    scale_e2 = (1.0 / (rows_mid * row_count)) ** 0.5
    fine_data = values.astype(jnp.float32)
    own_data = lax.dynamic_slice_in_dim(values, col_id * share, share, 0).astype(jnp.float32)
    product_part = listed_terms(points0, fine_cols, tiles_a0[0, 0], value_cols, support_fine, False)
    product_whole = lax.psum(product_part, "col")
    fine_residual = fine_data - 0.5 * (scale_a0 * product_whole)
    fine_square = jnp.sum(fine_residual * fine_residual)
    restrict_part = listed_terms(
        points0, mid_cols, tiles_e1[0, 0], fine_residual.astype(jnp.bfloat16), support_mid, True
    )
    restrict_sum = lax.psum(restrict_part, "row")
    mid_data = scale_e1 * restrict_sum
    mid_part = listed_terms(
        points1, mid_cols, tiles_a1[0, 0], mid_data.astype(jnp.bfloat16), support_mid, False
    )
    mid_whole = (scale_a1 * lax.psum(mid_part, "col")).astype(jnp.bfloat16)
    mid_slice = lax.dynamic_slice_in_dim(mid_whole, part_index * cols_mid, cols_mid, 0)
    mid_turned = spread(mid_slice, "row", source)
    mid_residual = mid_data - 0.5 * mid_turned.astype(jnp.float32)
    coarse_kernel = wendland(points2, mid_cols, support_coarse)
    coarse_part = jnp.dot(
        coarse_kernel, mid_residual.astype(jnp.bfloat16), preferred_element_type=jnp.float32
    )
    coarse_sum = lax.psum(coarse_part, "col")
    coarse_data = (scale_e2 * coarse_sum).astype(jnp.bfloat16)
    halfway_part = lax.dot_general(
        factor, coarse_data, (((0,), (0,)), ((), ())), preferred_element_type=jnp.float32
    )
    halfway = lax.psum(halfway_part, "row").astype(jnp.bfloat16)
    coarse_part_two = jnp.dot(factor, halfway, preferred_element_type=jnp.float32)
    coarse_coef = lax.psum(coarse_part_two, "col")
    prolong_part = lax.dot_general(
        coarse_kernel,
        coarse_coef.astype(jnp.bfloat16),
        (((0,), (0,)), ((), ())),
        preferred_element_type=jnp.float32,
    )
    mid_coef = 0.5 * mid_data + scale_e2 * lax.psum(prolong_part, "row")
    fine_part = listed_terms(
        points0, mid_cols, tiles_e1[0, 0], mid_coef.astype(jnp.bfloat16), support_mid, False
    )
    fine_coef = 0.5 * own_data + scale_e1 * lax.psum_scatter(
        fine_part, "col", scatter_dimension=0, tiled=True
    )
    fine_total = lax.psum(fine_square / col_count, ("row", "col"))
    fine_norm = fine_total / (rows_fine * row_count * fields)
    return (fine_coef, mid_coef, coarse_coef, jnp.stack([fine_norm]))


FAR = 64.0
MESH = pl.DeviceIdType.MESH


def phi_of(square, support):
    square = jnp.maximum(square, 1e-20)
    distance = square * lax.rsqrt(square)
    margin = jnp.maximum(support - distance, 0.0)
    squared = margin * margin
    return (squared * squared * (1.25 * support - margin)).astype(jnp.bfloat16)


def gain(support):
    return 4.0 / support ** 5


def dot(a, b):
    return jnp.dot(a, b, preferred_element_type=jnp.float32)


def far_rows(tiles, row_tiles, col_tiles, by_col):
    row, col = tiles[0, 0, 0:1, :], tiles[0, 0, 1:2, :]
    key = col * row_tiles + row if by_col else row * col_tiles + col
    count = row_tiles * col_tiles
    place = lax.broadcasted_iota(jnp.int32, (count, key.shape[1]), 0)
    near = jnp.max(jnp.where(place == key, 1.0, 0.0), axis=1, keepdims=True)
    return jnp.broadcast_to(FAR * (1.0 - near), (count, TILE))


def halves(x):
    high = x.astype(jnp.bfloat16)
    return high, (x - high.astype(jnp.float32)).astype(jnp.bfloat16)


def describe(ref, lanes, x, y):
    norm = x * x + y * y
    first = norm.astype(jnp.bfloat16).astype(jnp.float32)
    second = (norm - first).astype(jnp.bfloat16).astype(jnp.float32)
    for k, line in enumerate((-2.0 * x, -2.0 * y, first, second, norm - first - second)):
        ref[k:k + 1, lanes] = line


def flipped_side(sides):
    return jnp.concatenate([-0.5 * sides[0:2], sides[5:8], sides[2:5]], axis=0)


def cycle_kernel(g, vals_h, points0_h, points1_h, points2_h, tiles_a0_h, tiles_e1_h, tiles_a1_h, factor_h,
                 fine_o, mid_o, coarse_o, norm_o,
                 tiles_a0, tiles_e1, tiles_a1, factor, points2,
                 v2, p0g, p1g, pcg, maskg, emask, tmask, masks_s, emask_s, tmask_s, fac, facg, gtg,
                 gall, gmid, gcoarse, gfine, gplane, gmids, gcs, fbuf, side_a, side_e, side_t, side_o, side_m,
                 a0, e1own, e1t, e2t, a1t, other_s, other_r, resg, part_buf, rsin, mida, csend, crecv, cg, wcat, zcat,
                 l_s, a_m, p0_m, p1_m, pc_m, v_m, em_m, tm_m, f_m, g_m, ot_m, re_m, rs_m, mz_m, ma_m, cr_m, ca_m):
    nr, nc, R0, R1, R2 = g["nr"], g["nc"], g["R0"], g["R1"], g["R2"]
    D = nr * nc
    T0, T1 = R0 // TILE, R1 // TILE
    C0, C1 = R0 * nr // nc, R1 * nr // nc
    B0, B1 = C0 // TILE, C1 // TILE
    S0 = R0 // nc
    I0 = S0 // TILE
    Q1 = C1 // nr
    N1, N2 = nr * R1, g["N2"]
    CR = N2 // D
    NT1 = nr * T1
    NT2 = N2 // TILE
    f32, bf16 = jnp.float32, jnp.bfloat16
    r = lax.axis_index("row")
    c = lax.axis_index("col")
    d = r * nc + c
    y, k_core = r // 2, lax.rem(r, 2)
    z, h = c // 2, lax.rem(c, 2)
    mate = r + 1 - 2 * k_core
    yp = lax.rem(r + 2, nr)
    diag = lax.rem(mate + 2, nr)
    xp = c + 1 - 2 * h
    own_b = 2 * r + h

    def rc(src, dst, ssem, rsem, rr, cc):
        return pltpu.make_async_remote_copy(src_ref=src, dst_ref=dst, send_sem=ssem, recv_sem=rsem,
                                            device_id=(rr, cc), device_id_type=MESH)

    def each(lo, hi, f):
        def body(k, carry):
            f(k)
            return carry
        lax.fori_loop(lo, hi, body, 0)

    barrier = pltpu.get_barrier_semaphore()

    def greet(k):
        q = lax.rem(c + k, nc)
        for j in range(nr):
            pl.semaphore_signal(barrier, inc=1, device_id=(lax.rem(r + j, nr), q), device_id_type=MESH)

    each(1, nc, greet)
    for j in range(1, nr):
        pl.semaphore_signal(barrier, inc=1, device_id=(lax.rem(r + j, nr), c), device_id_type=MESH)
    loads = [pltpu.make_async_copy(s, t, l_s.at[k]) for k, (s, t) in enumerate((
        (points0_h, p0g.at[r]), (points1_h, p1g.at[r]), (points2_h, points2), (tiles_a0_h, tiles_a0),
        (tiles_e1_h, tiles_e1), (tiles_a1_h, tiles_a1), (factor_h, factor), (vals_h, v2.at[k_core])))]
    for load in loads:
        load.start()

    def one_hot(ref, rows, columns):
        ref[16:16 + rows] = jnp.where(lax.broadcasted_iota(jnp.int32, (rows, columns), 1) // TILE
                                      == lax.broadcasted_iota(jnp.int32, (rows, columns), 0), 1.0, 0.0).astype(bf16)

    one_hot(gfine, 2 * T0, 2 * R0)
    one_hot(gplane, T0, R0)
    one_hot(gmids, NT1, N1)
    fbuf[...] = jnp.zeros_like(fbuf)
    emask_s[...] = jnp.zeros_like(emask_s)
    tmask_s[...] = jnp.zeros_like(tmask_s)
    for ref in (gall, gmid, gcoarse):
        ref[...] = jnp.ones_like(ref)
    for load in loads[:-1]:
        load.wait()
    far_a0 = far_rows(tiles_a0, T0, B0, False)
    far_e1 = far_rows(tiles_e1, T0, B1, False)
    for q in range(nc):
        masks_s[q] = far_a0[q * I0 * B0:(q + 1) * I0 * B0].astype(bf16)
        emask_s[q, :I0 * B1] = far_e1[q * I0 * B1:(q + 1) * I0 * B1]
    far_e1 = far_rows(tiles_e1, T0, B1, True)
    far_a1 = far_rows(tiles_a1, T1, B1, True)
    planes = nc // 2
    PT = T0 // planes
    for q in range(planes):
        for j in range(B1):
            tmask_s[q, j * PT:(j + 1) * PT] = far_e1[j * T0 + q * PT:j * T0 + (q + 1) * PT]
        j = q * Q1 // TILE
        tmask_s[q, B1 * PT:B1 * PT + T1] = far_a1[j * T1:(j + 1) * T1]
    half_of = lax.rem(r, TILE // R2)
    raw = factor[...].astype(f32)
    fac[...] = jnp.concatenate([jnp.where(half_of == k, raw, 0.0) for k in range(TILE // R2)], axis=1).astype(bf16)
    line = points2[...].astype(f32)
    pcg[r] = jnp.zeros((8, TILE), f32)
    pcg[r, 0:2] = jnp.concatenate([jnp.where(half_of == k, line, 0.0) for k in range(TILE // R2)], axis=1)
    loads[-1].wait()
    pl.semaphore_wait(barrier, D - 1)

    def row_send(src, dst, m):
        for k in range(1, nr):
            rc(src, dst, m.at[0], m.at[1], lax.rem(r + k, nr), c).start()

    def row_wait(ref, m):
        slots = ref.at[pl.ds(0, nr - 1)]
        rc(slots, slots, m.at[0], m.at[1], mate, c).wait()

    def col_send(src_of, dst, m):
        def go(k):
            q = lax.rem(c + k, nc)
            rc(src_of(q), dst, m.at[0], m.at[1], r, q).start()
        each(1, nc, go)

    y_of = c // planes
    mask_row = 2 * y_of + k_core
    mask_slot = jnp.where(y_of == y, 0, 1) * planes + lax.rem(c, planes)
    mask_self = y_of == y

    def mask_go(k):
        q = lax.rem(c + k, nc)
        rc(masks_s.at[q], maskg.at[mask_slot], a_m.at[0], a_m.at[1], mask_row, q).start()

    each(1, nc, mask_go)

    @pl.when(jnp.logical_not(mask_self))
    def _():
        mask_go(0)

    @pl.when(mask_self)
    def _():
        maskg[mask_slot] = masks_s[c]

    row_send(p0g.at[r], p0g.at[r], p0_m)
    rc(v2.at[k_core], v2.at[k_core], v_m.at[0], v_m.at[1], mate, c).start()
    row_send(p1g.at[r], p1g.at[r], p1_m)
    row_send(pcg.at[r], pcg.at[r], pc_m)
    tmask_self = c // 2 == r

    def tmask_go(q):
        rc(tmask_s.at[q], tmask.at[r], tm_m.at[0], tm_m.at[1], c // 2, 2 * q + h).start()

    for k in range(1, planes):
        tmask_go(lax.rem(z + k, planes))

    @pl.when(jnp.logical_not(tmask_self))
    def _():
        tmask_go(z)

    @pl.when(tmask_self)
    def _():
        tmask[r] = tmask_s[z]

    col_send(lambda q: emask_s.at[q], emask.at[c], em_m)
    row_send(fac, facg.at[r], f_m)
    emask[c] = emask_s[c]
    facg[r] = fac[...]

    def describe_fine(rb):
        describe(gall.at[rb], slice(None), p0g[rb, 0:1, :].astype(f32), p0g[rb, 1:2, :].astype(f32))

    describe_fine(r)
    row_wait(p0g, p0_m)
    for rb in (mate, yp, diag):
        describe_fine(rb)
    for k in range(2):
        gfine[:16, k * R0:(k + 1) * R0] = jnp.concatenate(
            [gall[2 * y + k], jnp.zeros((8, R0), f32)], axis=0).astype(bf16)
    row_wait(p1g, p1_m)
    for q in range(nr):
        describe(gmid, slice(q * R1, (q + 1) * R1), p1g[q, 0:1, :].astype(f32), p1g[q, 1:2, :].astype(f32))
    gmids[:16] = jnp.concatenate([gmid[...], jnp.zeros((8, N1), f32)], axis=0).astype(bf16)
    strip = pl.ds(pl.multiple_of(c * S0, S0), S0)
    for s, rb in enumerate((r, yp)):
        fbuf[0:8, s * S0:(s + 1) * S0] = flipped_side(gall[rb, :, strip])

    def wait_slots(ref, n, m):
        slots = ref.at[pl.ds(0, n)]
        rc(slots, slots, m.at[0], m.at[1], mate, c).wait()

    @pl.when(mask_self)
    def _():
        wait_slots(maskg, nc - 1, a_m)

    @pl.when(jnp.logical_not(mask_self))
    def _():
        wait_slots(maskg, nc, a_m)

    for s in range(2):
        for q in range(planes):
            rows = maskg[s * planes + q].astype(f32)
            for i in range(I0):
                fbuf[16 + q * B0:16 + (q + 1) * B0, (s * I0 + i) * TILE:(s * I0 + i + 1) * TILE] = rows[i * B0:(i + 1) * B0]
    side_a[...] = fbuf[...].T.astype(bf16)

    def build(put, side, sides, depth, support, columns, step):
        def go(k):
            lanes = pl.ds(pl.multiple_of(k * step, step), step)
            put(lanes, phi_of(dot(side[:, :depth], sides[:depth, lanes]), support))
        each(0, columns // step, go)

    def put_a0(s):
        def put(lanes, value):
            a0[s, :, lanes] = value
        return put

    KA = 16 + 2 * T0
    build(put_a0(1), side_a.at[pl.ds(S0, S0)], gfine, KA, support_fine, 2 * R0, 512)
    rc(v2.at[1 - k_core], v2.at[1 - k_core], v_m.at[0], v_m.at[1], mate, c).wait()
    other_s[...] = (dot(a0[1, :, :R0], v2[0]) + dot(a0[1, :, R0:], v2[1])).astype(bf16)
    rc(other_s, other_r, ot_m.at[0], ot_m.at[1], yp, c).start()
    build(put_a0(0), side_a.at[pl.ds(0, S0)], gfine, KA, support_fine, 2 * R0, 512)
    acc = dot(a0[0, :, :R0], v2[0]) + dot(a0[0, :, R0:], v2[1])
    own_vals = v2[k_core, strip, :].astype(f32)
    rc(other_s, other_r, ot_m.at[0], ot_m.at[1], yp, c).wait()
    res = own_vals - (0.5 * g["scale_a0"] * gain(support_fine)) * (acc + other_r[...].astype(f32))
    resg[own_b] = res.astype(bf16).reshape(2, S0 // 2, -1)

    def plane_gather(ref, m, depth):
        first, second = pl.ds(0, depth // 2), pl.ds(depth // 2, depth // 2)
        x_slot, y_slot, d_slot = 2 * r + 1 - h, 2 * yp + h, 2 * yp + 1 - h

        def send(part, sem, rr, cc):
            rc(part, part, m.at[0], m.at[sem], rr, cc).start()

        def take(part, sem):
            rc(part, part, m.at[0], m.at[sem], mate, c).wait_recv()

        def start():
            send(ref.at[own_b], 1, r, xp)
            send(ref.at[own_b], 2, yp, c)
            send(ref.at[own_b], 5, mate, c)

        def pass_x():
            take(ref.at[x_slot], 1)
            send(ref.at[x_slot, first], 3, yp, c)
            send(ref.at[x_slot], 5, mate, c)

        def pass_y():
            take(ref.at[y_slot], 2)
            send(ref.at[y_slot, second], 4, r, xp)
            send(ref.at[y_slot], 5, mate, c)

        def pass_d():
            take(ref.at[d_slot, first], 3)
            send(ref.at[d_slot, first], 5, mate, c)
            take(ref.at[d_slot, second], 4)
            send(ref.at[d_slot, second], 5, mate, c)

        def end():
            take(ref.at[pl.ds(0, 4)], 5)

        def drain():
            part = ref.at[pl.ds(0, 7)]
            rc(part, part, m.at[0], m.at[5], mate, c).wait_send()
        return start, pass_x, pass_y, pass_d, end, drain

    res_start, res_x, res_y, res_d, res_end, res_drain = plane_gather(resg, re_m, 2)
    res_start()
    for q in range(nr):
        gplane[:16, q * PT * TILE:(q + 1) * PT * TILE] = jnp.concatenate(
            [gall[q, :, pl.ds(pl.multiple_of(z * PT * TILE, PT * TILE), PT * TILE)],
             jnp.zeros((8, PT * TILE), f32)], axis=0).astype(bf16)

    @pl.when(tmask_self)
    def _():
        wait_slots(tmask, nr - 1, tm_m)

    @pl.when(jnp.logical_not(tmask_self))
    def _():
        wait_slots(tmask, nr, tm_m)

    block = pl.ds(pl.multiple_of(own_b * C1, C1), C1)
    fbuf[0:8, :C1] = flipped_side(gmid[:, block])
    for q in range(nr):
        for j in range(B1):
            fbuf[16 + q * PT:16 + (q + 1) * PT, j * TILE:(j + 1) * TILE] = tmask[q, j * PT:(j + 1) * PT, :]
    own_tile = pl.ds(pl.multiple_of(own_b * C1 + (z * Q1) // TILE * TILE, TILE), TILE)
    fbuf[0:8, C1:C1 + TILE] = flipped_side(gmid[:, own_tile])
    for q in range(nr):
        fbuf[16 + q * T1:16 + (q + 1) * T1, C1:C1 + TILE] = tmask[q, B1 * PT:B1 * PT + T1, :]
    side_t[...] = fbuf[...].T.astype(bf16)

    def put_e1t(lanes, value):
        e1t[:, lanes] = value

    build(put_e1t, side_t.at[pl.ds(0, C1)], gplane, 16 + T0, support_mid, R0, 512)
    row_wait(pcg, pc_m)
    row_wait(facg, f_m)
    res_x()
    res_y()
    strips = []
    per = TILE // R2
    for lane in range(NT2):
        total = facg[lane * per].astype(f32)
        for k in range(1, per):
            total = total + facg[lane * per + k].astype(f32)
        strips.append(total)
    gtg[c] = jnp.concatenate(strips, axis=1).astype(bf16)
    col_send(lambda q: gtg.at[c], gtg.at[c], g_m)
    for t in range(NT2):
        line = pcg[per * t] + pcg[per * t + 1]
        describe(gcoarse, slice(t * TILE, (t + 1) * TILE), line[0:1], line[1:2])
    gcs[...] = jnp.concatenate([gcoarse[...], jnp.zeros((8, N2), f32)], axis=0).astype(bf16)
    wide = fbuf.shape[1]
    for q in range(N1 // wide):
        fbuf[0:8] = flipped_side(gmid[:, q * wide:(q + 1) * wide])
        side_m[...] = fbuf[...].T.astype(bf16)
        e2t[q * wide:(q + 1) * wide] = phi_of(dot(side_m[:, :16], gcs[...]), support_coarse)
    res_d()

    def put_a1t(lanes, value):
        a1t[:, lanes] = value

    own_half = pl.ds(pl.multiple_of(C1 + lax.rem(z * Q1, TILE), Q1), Q1)
    build(put_a1t, side_t.at[own_half], gmids, 16 + NT1, support_mid, N1, 1024)
    own_mids = pl.ds(pl.multiple_of(own_b * C1 + z * Q1, Q1), Q1)
    coarse_gain = g["scale_e2"] * gain(support_coarse)
    turned_w = coarse_gain * (e2t[own_mids, :].astype(f32)
                              - (0.5 * g["scale_a1"] * gain(support_mid)) * dot(a1t[...], e2t[...]))
    w_high, w_low = halves(turned_w)
    w_pair = jnp.concatenate([w_high.astype(f32), w_low.astype(f32)], axis=0).T.astype(bf16)
    wcat[:, :TILE] = w_pair
    wcat[:, TILE:] = w_pair
    res_end()
    plane = resg[...].reshape(R0, -1)
    restricted = dot(e1t[...], plane)
    held = plane.astype(f32)
    square = jnp.sum((held * held).reshape(R0 // 16, 16, -1), axis=0)
    for q in range(planes):
        part_buf[q] = jnp.concatenate([restricted[q * Q1:(q + 1) * Q1], square], axis=0).astype(bf16)

    def z_send(src_of, dst, m):
        for k in range(1, planes):
            q = lax.rem(z + k, planes)
            rc(src_of(q), dst, m.at[0], m.at[1], r, 2 * q + h).start()

    z_send(lambda q: part_buf.at[q], rsin.at[z], rs_m)
    rsin[z] = part_buf[z]
    wait_slots(emask, nc - 1, em_m)
    fbuf[0:8, :S0] = flipped_side(gall[r, :, strip])
    for q in range(nc):
        for i in range(I0):
            fbuf[16 + q * B1:16 + (q + 1) * B1, i * TILE:(i + 1) * TILE] = emask[q, i * B1:(i + 1) * B1, :]
    side_e[...] = fbuf[:, :S0].T.astype(bf16)

    def put_e1own(lanes, value):
        e1own[:, lanes] = value

    build(put_e1own, side_e, gmids, 16 + NT1, support_mid, N1, 512)
    wait_slots(gtg, nc - 1, g_m)
    gt = gtg[...].reshape(N2, N2)
    gg_high, gg_low = halves(dot(gt.astype(f32).T.astype(bf16), gt))
    zcat[S0 + C1:, :N2] = gg_high
    zcat[S0 + C1:, N2:] = gg_low
    fine_gain = g["scale_e1"] * gain(support_mid)
    h_high, h_low = halves((fine_gain * coarse_gain) * dot(e1own[...], e2t[...]))
    steps = (dot(h_high, gg_high) + dot(h_low, gg_high) + dot(h_high, gg_low),)
    rows_c = e2t[pl.ds(pl.multiple_of(c * C1, C1), C1), :]
    steps += (coarse_gain * (dot(rows_c, gg_high) + dot(rows_c, gg_low)),)
    for k, step in enumerate(steps):
        high, low = halves(step)
        zcat[k * C1:(k + 1) * C1, :N2] = high
        zcat[k * C1:(k + 1) * C1, N2:] = low

    wait_slots(rsin, planes - 1, rs_m)
    total = rsin[0].astype(f32)
    for q in range(1, planes):
        total = total + rsin[q].astype(f32)
    q_high, q_low = halves(fine_gain * total[:Q1])
    part = dot(wcat[...], jnp.concatenate([q_high, q_high, q_low, q_low], axis=0))
    csend[...] = part.reshape(D, CR, -1).astype(bf16)

    def all_send(src_of, dst, m):
        def go(k):
            q = lax.rem(c + k, nc)
            for j in range(nr):
                p = lax.rem(r + j, nr)
                rc(src_of(p * nc + q), dst, m.at[0], m.at[1], p, q).start()
        each(1, nc, go)
        for j in range(1, nr):
            p = lax.rem(r + j, nr)
            rc(src_of(p * nc + c), dst, m.at[0], m.at[1], p, c).start()

    all_send(lambda q: csend.at[q], crecv.at[d], cr_m)
    mida[own_b, z] = q_high
    z_send(lambda q: mida.at[own_b, z], mida.at[own_b, z], mz_m)
    crecv[d] = csend[d]
    norm_o[...] = jnp.broadcast_to(jnp.sum(total[Q1:], keepdims=True) * g["norm_scale"], norm_o.shape)
    wait_slots(crecv, D - 1, cr_m)
    cg[d] = jnp.sum(crecv[...].astype(f32), axis=0).astype(bf16)
    all_send(lambda q: cg.at[d], cg.at[d], ca_m)
    mid_start, mid_x, mid_y, mid_d, mid_end, mid_drain = plane_gather(mida, ma_m, planes)
    arrived = mida.at[own_b, pl.ds(0, planes - 1)]
    rc(arrived, arrived, mz_m.at[0], mz_m.at[1], mate, c).wait()
    mid_start()
    mid_x()
    mid_y()
    wait_slots(cg, D - 1, ca_m)
    cd = cg[...].astype(f32).reshape(N2, -1).astype(bf16)
    both = jnp.concatenate([cd, cd], axis=0)
    coarse_o[...] = dot(zcat[pl.ds(pl.multiple_of(S0 + C1 + r * R2, R2), R2), :], both)
    mid_d()
    mid_end()
    mid_o[...] = 0.5 * mida[c].astype(f32).reshape(C1, -1) + dot(zcat[S0:S0 + C1, :], both)
    fine_o[...] = (0.5 * own_vals + (0.5 * fine_gain) * dot(e1own[...], mida[...].reshape(N1, -1))
                   + dot(zcat[:S0, :], both))
    res_drain()
    mid_drain()


def finish_kernel(fine, mid, coarse, norm, fine_o, mid_o, coarse_o, norm_o):
    fine_o[...] = fine[...]
    mid_o[...] = mid[...]
    coarse_o[...] = coarse[...]
    norm_o[...] = norm[0:1, 0:1]


def fits(nr, nc, R0, R1, R2):
    if nr != 4 or nc != 8:
        return False
    if R0 != R1 * nr or R0 != 2 * nc * TILE or 2 * R2 != TILE:
        return False
    return True


def fused(values, points0, points1, points2, tiles_a0, tiles_e1, tiles_a1, factor):
    nr, nc = lax.axis_size("row"), lax.axis_size("col")
    R0, R1, R2 = points0.shape[1], points1.shape[1], points2.shape[1]
    F = values.shape[-1]
    if not fits(nr, nc, R0, R1, R2) or F != TILE:
        return per_device(values, points0, points1, points2, tiles_a0, tiles_e1, tiles_a1, factor)
    D, N2 = nr * nc, nr * R2
    T0, T1 = R0 // TILE, R1 // TILE
    B0, B1 = R0 * nr // nc // TILE, R1 * nr // nc // TILE
    S0 = R0 // nc
    I0 = S0 // TILE
    C1, CR, Q1 = B1 * TILE, N2 // D, R1 * nr // nc // nr
    g = dict(nr=nr, nc=nc, R0=R0, R1=R1, R2=R2, N2=N2,
             scale_a0=(R0 / (nc * tiles_a0.shape[-1] * TILE * TILE)) ** 0.5,
             scale_e1=(R0 / (nc * tiles_e1.shape[-1] * TILE * TILE)) ** 0.5,
             scale_a1=(R1 / (nc * tiles_a1.shape[-1] * TILE * TILE)) ** 0.5,
             scale_e2=(1.0 / (R1 * nr)) ** 0.5,
             norm_scale=1.0 / (R0 * nr * F))
    f32, bf16, i32 = jnp.float32, jnp.bfloat16, jnp.int32
    V = pltpu.VMEM
    dma = pltpu.SemaphoreType.DMA
    wide = N2 // nc
    N1 = nr * R1
    planes = nc // 2
    scratch = [
        V(tiles_a0.shape, i32), V(tiles_e1.shape, i32), V(tiles_a1.shape, i32), V((wide, R2), bf16), V(points2.shape, bf16),
        V((2, R0, F), bf16), V((nr,) + points0.shape, bf16), V((nr,) + points1.shape, bf16), V((nr, 8, TILE), f32),
        V((nc, I0 * B0, TILE), bf16), V((nc, 8, TILE), f32), V((nr, 16, TILE), f32),
        V((nc, I0 * B0, TILE), bf16), V((nc, 8, TILE), f32), V((planes, 16, TILE), f32),
        V((wide, TILE), bf16), V((nr, wide, TILE), bf16), V((nc, wide, N2), bf16),
        V((nr, 8, R0), f32), V((8, N1), f32), V((8, N2), f32),
        V((16 + 2 * T0, 2 * R0), bf16), V((16 + T0, R0), bf16), V((16 + nr * T1, N1), bf16), V((16, N2), bf16),
        V((TILE, 2 * S0), f32), V((2 * S0, TILE), bf16), V((S0, TILE), bf16), V((2 * S0, TILE), bf16),
        V((8, TILE), bf16), V((2 * S0, TILE), bf16),
        V((2, S0, 2 * R0), bf16), V((S0, N1), bf16), V((C1, R0), bf16), V((N1, N2), bf16), V((Q1, N1), bf16),
        V((S0, F), bf16), V((S0, F), bf16), V((nc, 2, S0 // 2, F), bf16),
        V((planes, Q1 + 16, F), bf16), V((planes, Q1 + 16, F), bf16), V((nc, planes, Q1, F), bf16),
        V((D, CR, F), bf16), V((D, CR, F), bf16), V((D, CR, F), bf16), V((N2, 4 * Q1), bf16),
        V((S0 + C1 + N2, 2 * N2), bf16),
    ]
    for n in (8, 2, 2, 2, 2, 2, 2, 2, 2, 2, 2, 6, 2, 2, 6, 2, 2):
        scratch += [dma((n,))]
    vm = pl.BlockSpec(memory_space=pltpu.VMEM)
    shapes = ((S0, F), (C1, F), (R2, F))
    parts = pl.pallas_call(
        functools.partial(cycle_kernel, g),
        out_shape=tuple(jax.ShapeDtypeStruct(s, f32) for s in shapes + ((8, TILE),)),
        in_specs=[pl.BlockSpec(memory_space=pltpu.HBM)] * 8,
        out_specs=[vm] * 4,
        scratch_shapes=scratch,
        compiler_params=pltpu.CompilerParams(collective_id=0, has_side_effects=True, vmem_limit_bytes=48 << 20),
    )(*[pltpu.with_memory_space_constraint(x, pltpu.HBM) for x in (
        values, points0, points1, points2, tiles_a0, tiles_e1, tiles_a1, factor.T)])
    fine, mid, coarse, norm = pl.pallas_call(
        finish_kernel,
        grid=(1,),
        out_shape=tuple(jax.ShapeDtypeStruct(s, f32) for s in shapes + ((1, 1),)),
        in_specs=[vm] * 4,
        out_specs=[pl.BlockSpec(s, lambda i: (0, 0)) for s in shapes + ((1, 1),)],
        compiler_params=pltpu.CompilerParams(vmem_limit_bytes=4 << 20),
    )(*parts)
    return (fine, mid, coarse, norm.reshape(1))


def solution(mesh):
    return jax.shard_map(
        fused,
        mesh=mesh,
        in_specs=(
            P("row", None),
            P(None, "row"),
            P(None, "row"),
            P(None, "row"),
            P("row", "col", None, None),
            P("row", "col", None, None),
            P("row", "col", None, None),
            P("row", "col"),
        ),
        out_specs=(P(("row", "col"), None), P("col", None), P("row", None), P()),
        check_vma=False,
    )
```

```python
import functools
import math

import jax
import jax.numpy as jnp
from jax import lax
from jax.experimental import pallas as pl
from jax.experimental.pallas import tpu as pltpu
from jax.sharding import PartitionSpec as P

TILE = 128


support_fine = 0.35
support_mid = 0.55
support_coarse = 0.8


def spread(x, axis, root):
    mine = lax.axis_index(axis) == root
    return lax.psum(jnp.where(mine, x, jnp.zeros_like(x)), axis)


def wendland(left_pts, right_pts, support):
    left = left_pts.astype(jnp.float32)
    right = right_pts.astype(jnp.float32)
    across = left[0][..., :, None] - right[0][..., None, :]
    upward = left[1][..., :, None] - right[1][..., None, :]
    ratio_t = jnp.sqrt(across * across + upward * upward) / support
    margin = jnp.maximum(1.0 - ratio_t, 0.0)
    squared = margin * margin
    return (squared * squared * (4.0 * ratio_t + 1.0)).astype(jnp.bfloat16)


def listed_terms(row_pts, col_pts, listing, vector, support, flipped):
    row_tiles = row_pts.reshape(2, -1, TILE)
    col_tiles = col_pts.reshape(2, -1, TILE)
    listed = listing.shape[-1]
    group = math.gcd(listed, 32)
    order = listing.reshape(2, listed // group, group)
    fields = vector.shape[-1]
    inputs = vector.reshape(-1, TILE, fields)
    target = col_tiles.shape[1] if flipped else row_tiles.shape[1]
    total = jnp.zeros((target, TILE, fields), jnp.float32)

    def add_group(total, pair):
        tile_rows, tile_cols = pair
        kernel = wendland(row_tiles[:, tile_rows], col_tiles[:, tile_cols], support)
        if flipped:
            contrib = jnp.einsum(
                "gij,gir->gjr", kernel, inputs[tile_rows], preferred_element_type=jnp.float32
            )
            return (total.at[tile_cols].add(contrib), None)
        contrib = jnp.einsum(
            "gij,gjr->gir", kernel, inputs[tile_cols], preferred_element_type=jnp.float32
        )
        return (total.at[tile_rows].add(contrib), None)

    total, unused = lax.scan(add_group, total, (order[0], order[1]))
    return total.reshape(-1, fields)


def per_device(values, points0, points1, points2, tiles_a0, tiles_e1, tiles_a1, factor):
    row_count = lax.axis_size("row")
    col_count = lax.axis_size("col")
    col_id = lax.axis_index("col")
    col_per_row = col_count // row_count
    rows_fine, fields = values.shape
    rows_mid = points1.shape[1]
    share = rows_fine // col_count
    cols_fine = rows_fine // col_per_row
    cols_mid = rows_mid // col_per_row
    source = col_id // col_per_row
    part_index = col_id % col_per_row
    value_piece = lax.dynamic_slice_in_dim(values, part_index * cols_fine, cols_fine, 0)
    fine_piece = lax.dynamic_slice_in_dim(points0, part_index * cols_fine, cols_fine, 1)
    mid_piece = lax.dynamic_slice_in_dim(points1, part_index * cols_mid, cols_mid, 1)
    value_cols, fine_cols, mid_cols = (
        spread(value_piece, "row", source),
        spread(fine_piece, "row", source),
        spread(mid_piece, "row", source),
    )
    scale_a0 = (rows_fine / (col_count * tiles_a0.shape[-1] * TILE * TILE)) ** 0.5
    scale_e1 = (rows_fine / (col_count * tiles_e1.shape[-1] * TILE * TILE)) ** 0.5
    scale_a1 = (rows_mid / (col_count * tiles_a1.shape[-1] * TILE * TILE)) ** 0.5
    scale_e2 = (1.0 / (rows_mid * row_count)) ** 0.5
    fine_data = values.astype(jnp.float32)
    own_data = lax.dynamic_slice_in_dim(values, col_id * share, share, 0).astype(jnp.float32)
    product_part = listed_terms(points0, fine_cols, tiles_a0[0, 0], value_cols, support_fine, False)
    product_whole = lax.psum(product_part, "col")
    fine_residual = fine_data - 0.5 * (scale_a0 * product_whole)
    fine_square = jnp.sum(fine_residual * fine_residual)
    restrict_part = listed_terms(
        points0, mid_cols, tiles_e1[0, 0], fine_residual.astype(jnp.bfloat16), support_mid, True
    )
    restrict_sum = lax.psum(restrict_part, "row")
    mid_data = scale_e1 * restrict_sum
    mid_part = listed_terms(
        points1, mid_cols, tiles_a1[0, 0], mid_data.astype(jnp.bfloat16), support_mid, False
    )
    mid_whole = (scale_a1 * lax.psum(mid_part, "col")).astype(jnp.bfloat16)
    mid_slice = lax.dynamic_slice_in_dim(mid_whole, part_index * cols_mid, cols_mid, 0)
    mid_turned = spread(mid_slice, "row", source)
    mid_residual = mid_data - 0.5 * mid_turned.astype(jnp.float32)
    coarse_kernel = wendland(points2, mid_cols, support_coarse)
    coarse_part = jnp.dot(
        coarse_kernel, mid_residual.astype(jnp.bfloat16), preferred_element_type=jnp.float32
    )
    coarse_sum = lax.psum(coarse_part, "col")
    coarse_data = (scale_e2 * coarse_sum).astype(jnp.bfloat16)
    halfway_part = lax.dot_general(
        factor, coarse_data, (((0,), (0,)), ((), ())), preferred_element_type=jnp.float32
    )
    halfway = lax.psum(halfway_part, "row").astype(jnp.bfloat16)
    coarse_part_two = jnp.dot(factor, halfway, preferred_element_type=jnp.float32)
    coarse_coef = lax.psum(coarse_part_two, "col")
    prolong_part = lax.dot_general(
        coarse_kernel,
        coarse_coef.astype(jnp.bfloat16),
        (((0,), (0,)), ((), ())),
        preferred_element_type=jnp.float32,
    )
    mid_coef = 0.5 * mid_data + scale_e2 * lax.psum(prolong_part, "row")
    fine_part = listed_terms(
        points0, mid_cols, tiles_e1[0, 0], mid_coef.astype(jnp.bfloat16), support_mid, False
    )
    fine_coef = 0.5 * own_data + scale_e1 * lax.psum_scatter(
        fine_part, "col", scatter_dimension=0, tiled=True
    )
    fine_total = lax.psum(fine_square / col_count, ("row", "col"))
    fine_norm = fine_total / (rows_fine * row_count * fields)
    return (fine_coef, mid_coef, coarse_coef, jnp.stack([fine_norm]))


FAR = 64.0
MESH = pl.DeviceIdType.MESH


EDGE = 4.0 ** 0.2


def phi_of(square):
    square = jnp.maximum(square, 1e-20)
    margin = jnp.maximum(EDGE - square * lax.rsqrt(square), 0.0)
    squared = margin * margin
    return (squared * squared * (1.25 * EDGE - margin)).astype(jnp.bfloat16)


def dot(a, b):
    return jnp.dot(a, b, preferred_element_type=jnp.float32)


def far_rows(tiles, row_tiles, col_tiles, by_col):
    row, col = tiles[0, 0, 0:1, :], tiles[0, 0, 1:2, :]
    key = col * row_tiles + row if by_col else row * col_tiles + col
    count = row_tiles * col_tiles
    place = lax.broadcasted_iota(jnp.int32, (count, key.shape[1]), 0)
    near = jnp.max(jnp.where(place == key, 1.0, 0.0), axis=1, keepdims=True)
    return jnp.broadcast_to(FAR * (1.0 - near), (count, TILE))


def halves(x):
    high = x.astype(jnp.bfloat16)
    return high, (x - high.astype(jnp.float32)).astype(jnp.bfloat16)


def pieces(x):
    first = x.astype(jnp.bfloat16).astype(jnp.float32)
    second = (x - first).astype(jnp.bfloat16).astype(jnp.float32)
    return first, second, x - first - second


def describe(ref, lanes, x, y, support):
    square = (EDGE / support) ** 2
    lines = pieces(-2.0 * square * x) + pieces(-2.0 * square * y) + pieces(square * (x * x + y * y))
    for k, line in enumerate(lines):
        ref[k:k + 1, lanes] = line
    ref[12:13, lanes] = x
    ref[13:14, lanes] = y


def flipped_side(sides):
    x, y = sides[12:13], sides[13:14]
    one = jnp.ones_like(x)
    return jnp.concatenate([x, x, x, y, y, y, one, one, one, sides[6:9], jnp.zeros((4, x.shape[1]), jnp.float32)], axis=0)


def cycle_kernel(g, vals_h, points0_h, points1_h, points2_h, tiles_a0_h, tiles_e1_h, tiles_a1_h, factor_h,
                 fine_o, mid_o, coarse_o, norm_o,
                 tiles_a0, tiles_e1, tiles_a1, factor, points2,
                 v2, p0g, p1g, pcg, maskg, emask, tmask, masks_s, emask_s, tmask_s, fac, facg, gtg,
                 gall, gstrip, gpl, gmid, gmid2, gcoarse, gfine, gplane, gmids, gcs, fbuf, side_a, side_e, side_t, side_o, side_m,
                 a0, e1own, e1t, e2t, a1t, other_s, other_r, resg, part_buf, rsin, mida, csend, crecv, cg, wcat, zcat,
                 l_s, a_m, p0_m, p1_m, pc_m, v_m, em_m, tm_m, f_m, g_m, ot_m, re_m, rs_m, mz_m, ma_m, cr_m, ca_m):
    nr, nc, R0, R1, R2 = g["nr"], g["nc"], g["R0"], g["R1"], g["R2"]
    D = nr * nc
    T0, T1 = R0 // TILE, R1 // TILE
    C0, C1 = R0 * nr // nc, R1 * nr // nc
    B0, B1 = C0 // TILE, C1 // TILE
    S0 = R0 // nc
    I0 = S0 // TILE
    Q1 = C1 // nr
    N1, N2 = nr * R1, g["N2"]
    CR = N2 // D
    NT1 = nr * T1
    NT2 = N2 // TILE
    f32, bf16 = jnp.float32, jnp.bfloat16
    r = lax.axis_index("row")
    c = lax.axis_index("col")
    d = r * nc + c
    y, k_core = r // 2, lax.rem(r, 2)
    z, h = c // 2, lax.rem(c, 2)
    mate = r + 1 - 2 * k_core
    yp = lax.rem(r + 2, nr)
    diag = lax.rem(mate + 2, nr)
    xp = c + 1 - 2 * h
    own_b = 2 * r + h

    def rc(src, dst, ssem, rsem, rr, cc):
        return pltpu.make_async_remote_copy(src_ref=src, dst_ref=dst, send_sem=ssem, recv_sem=rsem,
                                            device_id=(rr, cc), device_id_type=MESH)

    def each(lo, hi, f):
        def body(k, carry):
            f(k)
            return carry
        lax.fori_loop(lo, hi, body, 0)

    barrier = pltpu.get_barrier_semaphore()

    def greet(k):
        q = lax.rem(c + k, nc)
        for j in range(nr):
            pl.semaphore_signal(barrier, inc=1, device_id=(lax.rem(r + j, nr), q), device_id_type=MESH)

    each(1, nc, greet)
    for j in range(1, nr):
        pl.semaphore_signal(barrier, inc=1, device_id=(lax.rem(r + j, nr), c), device_id_type=MESH)
    loads = [pltpu.make_async_copy(s, t, l_s.at[k]) for k, (s, t) in enumerate((
        (points0_h, p0g.at[r]), (points1_h, p1g.at[r]), (points2_h, points2), (tiles_a0_h, tiles_a0),
        (tiles_e1_h, tiles_e1), (tiles_a1_h, tiles_a1), (factor_h, factor), (vals_h, v2.at[k_core])))]
    for load in loads:
        load.start()

    def one_hot(ref, rows, columns):
        ref[16:16 + rows] = jnp.where(lax.broadcasted_iota(jnp.int32, (rows, columns), 1) // TILE
                                      == lax.broadcasted_iota(jnp.int32, (rows, columns), 0), 1.0, 0.0).astype(bf16)

    one_hot(gfine, 2 * T0, 2 * R0)
    one_hot(gplane, T0, R0)
    one_hot(gmids, NT1, N1)
    fbuf[...] = jnp.zeros_like(fbuf)
    emask_s[...] = jnp.zeros_like(emask_s)
    tmask_s[...] = jnp.zeros_like(tmask_s)
    for ref in (gall, gstrip, gpl, gmid, gmid2, gcoarse):
        ref[...] = jnp.ones_like(ref)
    for load in loads[:-1]:
        load.wait()
    far_a0 = far_rows(tiles_a0, T0, B0, False)
    far_e1 = far_rows(tiles_e1, T0, B1, False)
    for q in range(nc):
        masks_s[q] = far_a0[q * I0 * B0:(q + 1) * I0 * B0].astype(bf16)
        emask_s[q, :I0 * B1] = far_e1[q * I0 * B1:(q + 1) * I0 * B1]
    far_e1 = far_rows(tiles_e1, T0, B1, True)
    far_a1 = far_rows(tiles_a1, T1, B1, True)
    planes = nc // 2
    PT = T0 // planes
    for q in range(planes):
        for j in range(B1):
            tmask_s[q, j * PT:(j + 1) * PT] = far_e1[j * T0 + q * PT:j * T0 + (q + 1) * PT]
        tmask_s[q, B1 * PT:B1 * PT + B1 * T1] = far_a1
    half_of = lax.rem(r, TILE // R2)
    raw = factor[...].astype(f32)
    fac[...] = jnp.concatenate([jnp.where(half_of == k, raw, 0.0) for k in range(TILE // R2)], axis=1).astype(bf16)
    line = points2[...].astype(f32)
    pcg[r] = jnp.zeros((8, TILE), f32)
    pcg[r, 0:2] = jnp.concatenate([jnp.where(half_of == k, line, 0.0) for k in range(TILE // R2)], axis=1)
    loads[-1].wait()
    pl.semaphore_wait(barrier, D - 1)

    def row_send(src, dst, m):
        for k in range(1, nr):
            rc(src, dst, m.at[0], m.at[1], lax.rem(r + k, nr), c).start()

    def row_wait(ref, m):
        slots = ref.at[pl.ds(0, nr - 1)]
        rc(slots, slots, m.at[0], m.at[1], mate, c).wait()

    def col_send(src_of, dst, m):
        def go(k):
            q = lax.rem(c + k, nc)
            rc(src_of(q), dst, m.at[0], m.at[1], r, q).start()
        each(1, nc, go)

    y_of = c // planes
    mask_row = 2 * y_of + k_core
    mask_slot = jnp.where(y_of == y, 0, 1) * planes + lax.rem(c, planes)
    mask_self = y_of == y

    def mask_go(k):
        q = lax.rem(c + k, nc)
        rc(masks_s.at[q], maskg.at[mask_slot], a_m.at[0], a_m.at[1], mask_row, q).start()

    each(1, nc, mask_go)

    @pl.when(jnp.logical_not(mask_self))
    def _():
        mask_go(0)

    @pl.when(mask_self)
    def _():
        maskg[mask_slot] = masks_s[c]

    row_send(p0g.at[r], p0g.at[r], p0_m)
    rc(v2.at[k_core], v2.at[k_core], v_m.at[0], v_m.at[1], mate, c).start()
    row_send(p1g.at[r], p1g.at[r], p1_m)
    row_send(pcg.at[r], pcg.at[r], pc_m)
    tmask_self = c // 2 == r

    def tmask_go(q):
        rc(tmask_s.at[q], tmask.at[r], tm_m.at[0], tm_m.at[1], c // 2, 2 * q + h).start()

    for k in range(1, planes):
        tmask_go(lax.rem(z + k, planes))

    @pl.when(jnp.logical_not(tmask_self))
    def _():
        tmask_go(z)

    @pl.when(tmask_self)
    def _():
        tmask[r] = tmask_s[z]

    col_send(lambda q: emask_s.at[q], emask.at[c], em_m)
    row_send(fac, facg.at[r], f_m)
    emask[c] = emask_s[c]
    facg[r] = fac[...]

    def line_of(ref, q, way, lanes=slice(None)):
        return ref[q, way:way + 1, lanes].astype(f32)

    def describe_own(rb, slot):
        describe(gall.at[slot], slice(None), line_of(p0g, rb, 0), line_of(p0g, rb, 1), support_fine)
        gfine[:16, pl.ds(pl.multiple_of(slot * R0, R0), R0)] = gall[slot].astype(bf16)

    strip = pl.ds(pl.multiple_of(c * S0, S0), S0)
    describe_own(r, k_core)
    row_wait(p0g, p0_m)
    describe_own(mate, 1 - k_core)
    describe(gstrip, slice(None), line_of(p0g, yp, 0, strip), line_of(p0g, yp, 1, strip), support_fine)
    fbuf[0:16, :S0] = flipped_side(gall[k_core, :, strip])
    fbuf[0:16, S0:] = flipped_side(gstrip[...])

    def wait_slots(ref, n, m):
        slots = ref.at[pl.ds(0, n)]
        rc(slots, slots, m.at[0], m.at[1], mate, c).wait()

    @pl.when(mask_self)
    def _():
        wait_slots(maskg, nc - 1, a_m)

    @pl.when(jnp.logical_not(mask_self))
    def _():
        wait_slots(maskg, nc, a_m)

    for s in range(2):
        for q in range(planes):
            rows = maskg[s * planes + q].astype(f32)
            for i in range(I0):
                fbuf[16 + q * B0:16 + (q + 1) * B0, (s * I0 + i) * TILE:(s * I0 + i + 1) * TILE] = rows[i * B0:(i + 1) * B0]
    side_a[...] = fbuf[...].T.astype(bf16)

    def build(put, side, sides, depth, columns, step):
        def go(k):
            lanes = pl.ds(pl.multiple_of(k * step, step), step)
            put(lanes, phi_of(dot(side[:, :depth], sides[:depth, lanes])))
        each(0, columns // step, go)

    def put_a0(s):
        def put(lanes, value):
            a0[s, :, lanes] = value
        return put

    KA = 16 + 2 * T0
    build(put_a0(1), side_a.at[pl.ds(S0, S0)], gfine, KA, 2 * R0, 2048)
    rc(v2.at[1 - k_core], v2.at[1 - k_core], v_m.at[0], v_m.at[1], mate, c).wait()
    other_s[...] = (dot(a0[1, :, :R0], v2[0]) + dot(a0[1, :, R0:], v2[1])).astype(bf16)
    rc(other_s, other_r, ot_m.at[0], ot_m.at[1], yp, c).start()
    build(put_a0(0), side_a.at[pl.ds(0, S0)], gfine, KA, 2 * R0, 2048)
    acc = dot(a0[0, :, :R0], v2[0]) + dot(a0[0, :, R0:], v2[1])
    own_vals = v2[k_core, strip, :].astype(f32)
    rc(other_s, other_r, ot_m.at[0], ot_m.at[1], yp, c).wait()
    res = own_vals - (0.5 * g["scale_a0"]) * (acc + other_r[...].astype(f32))
    resg[own_b] = res.astype(bf16)

    x_slot, y_slot, d_slot = 2 * r + 1 - h, 2 * yp + h, 2 * diag + 1 - h

    def plane_gather(ref, m):
        def send(slot, sem, rr, cc):
            rc(ref.at[slot], ref.at[slot], m.at[0], m.at[sem], rr, cc).start()

        def start():
            send(own_b, 1, r, xp)
            send(own_b, 2, yp, c)
            send(own_b, 3, diag, xp)
            send(own_b, 4, mate, c)

        def relay(slot, sem):
            rc(ref.at[slot], ref.at[slot], m.at[0], m.at[sem], mate, c).wait_recv()
            send(slot, 4, mate, c)

        def end():
            part = ref.at[pl.ds(0, 4)]
            rc(part, part, m.at[0], m.at[4], mate, c).wait_recv()

        def drain():
            part = ref.at[pl.ds(0, 7)]
            rc(part, part, m.at[0], m.at[4], mate, c).wait_send()
        return (start, functools.partial(relay, x_slot, 1), functools.partial(relay, y_slot, 2),
                functools.partial(relay, d_slot, 3), end, drain)

    res_start, res_x, res_y, res_d, res_end, res_drain = plane_gather(resg, re_m)
    res_start()
    PL = PT * TILE
    plane_lanes = pl.ds(pl.multiple_of(z * PL, PL), PL)
    row_wait(p1g, p1_m)
    for q in range(nr):
        describe(gpl, slice(q * PL, (q + 1) * PL), line_of(p0g, q, 0, plane_lanes), line_of(p0g, q, 1, plane_lanes), support_mid)
        lanes = slice(q * R1, (q + 1) * R1)
        describe(gmid, lanes, line_of(p1g, q, 0), line_of(p1g, q, 1), support_mid)
    gplane[:16] = gpl[...].astype(bf16)
    gmids[:16] = gmid[...].astype(bf16)

    @pl.when(tmask_self)
    def _():
        wait_slots(tmask, nr - 1, tm_m)

    @pl.when(jnp.logical_not(tmask_self))
    def _():
        wait_slots(tmask, nr, tm_m)

    block = pl.ds(pl.multiple_of(own_b * C1, C1), C1)
    fbuf[0:16, :C1] = flipped_side(gmid[:, block])
    fbuf[0:16, C1:] = fbuf[0:16, :C1]
    for q in range(nr):
        for j in range(B1):
            fbuf[16 + q * PT:16 + (q + 1) * PT, j * TILE:(j + 1) * TILE] = tmask[q, j * PT:(j + 1) * PT, :]
            at = B1 * PT + j * T1
            fbuf[16 + q * T1:16 + (q + 1) * T1, C1 + j * TILE:C1 + (j + 1) * TILE] = tmask[q, at:at + T1, :]
    side_t[...] = fbuf[...].T.astype(bf16)

    def put_e1t(lanes, value):
        e1t[:, lanes] = value

    build(put_e1t, side_t.at[pl.ds(0, C1)], gplane, 16 + T0, R0, 2048)
    row_wait(pcg, pc_m)
    row_wait(facg, f_m)
    res_x()
    res_y()
    strips = []
    per = TILE // R2
    for lane in range(NT2):
        total = facg[lane * per].astype(f32)
        for k in range(1, per):
            total = total + facg[lane * per + k].astype(f32)
        strips.append(total)
    gtg[c] = jnp.concatenate(strips, axis=1).astype(bf16)
    col_send(lambda q: gtg.at[c], gtg.at[c], g_m)
    for t in range(NT2):
        line = pcg[per * t] + pcg[per * t + 1]
        describe(gcoarse, slice(t * TILE, (t + 1) * TILE), line[0:1], line[1:2], support_coarse)
    gcs[...] = gcoarse[...].astype(bf16)
    for q in range(nr):
        describe(gmid2, slice(q * R1, (q + 1) * R1), line_of(p1g, q, 0), line_of(p1g, q, 1), support_coarse)
    wide = fbuf.shape[1]
    for q in range(N1 // wide):
        fbuf[0:16] = flipped_side(gmid2[:, q * wide:(q + 1) * wide])
        side_m[...] = fbuf[...].T.astype(bf16)
        e2t[q * wide:(q + 1) * wide] = phi_of(dot(side_m[:, :16], gcs[...]))
    res_d()

    restricted = jnp.zeros((C1, resg.shape[-1]), f32)
    square = jnp.zeros((16, resg.shape[-1]), f32)

    def restrict(slot):
        strip_data = resg[slot]
        held = strip_data.astype(f32)
        return (dot(e1t[:, pl.ds(pl.multiple_of(slot * S0, S0), S0)], strip_data),
                jnp.sum((held * held).reshape(S0 // 16, 16, -1), axis=0))

    for slot in (own_b, x_slot, y_slot, d_slot):
        term = restrict(slot)
        restricted, square = restricted + term[0], square + term[1]
    res_end()
    for slot in (2 * mate + h, 2 * mate + 1 - h, 2 * diag + h, 2 * yp + 1 - h):
        term = restrict(slot)
        restricted, square = restricted + term[0], square + term[1]
    restricted = g["scale_e1"] * restricted
    for q in range(planes):
        part_buf[q] = jnp.concatenate([restricted[q * Q1:(q + 1) * Q1], square], axis=0).astype(bf16)

    def z_send(src_of, dst, m):
        for k in range(1, planes):
            q = lax.rem(z + k, planes)
            rc(src_of(q), dst, m.at[0], m.at[1], r, 2 * q + h).start()

    z_send(lambda q: part_buf.at[q], rsin.at[z], rs_m)
    rsin[z] = part_buf[z]
    def put_a1t(lanes, value):
        a1t[:, lanes] = value

    build(put_a1t, side_t.at[pl.ds(C1, C1)], gmids, 16 + NT1, N1, 1024)
    turned_w = g["scale_e2"] * (e2t[block, :].astype(f32) - (0.5 * g["scale_a1"]) * dot(a1t[...], e2t[...]))
    w_high, w_low = halves(turned_w.T)
    for k, w in enumerate((w_high, w_low, w_high)):
        wcat[:, k * C1:(k + 1) * C1] = w
    def all_send(src_of, dst, m):
        def go(k):
            q = lax.rem(c + k, nc)
            for j in range(nr):
                p = lax.rem(r + j, nr)
                rc(src_of(p * nc + q), dst, m.at[0], m.at[1], p, q).start()
        each(1, nc, go)
        for j in range(1, nr):
            p = lax.rem(r + j, nr)
            rc(src_of(p * nc + c), dst, m.at[0], m.at[1], p, c).start()

    part_high, part_low = halves(restricted)
    part = dot(wcat[...], jnp.concatenate([part_high, part_high, part_low], axis=0))
    csend[...] = part.reshape(D, CR, -1).astype(bf16)
    all_send(lambda q: csend.at[q], crecv.at[d], cr_m)
    crecv[d] = csend[d]
    wait_slots(emask, nc - 1, em_m)
    describe(gstrip, slice(None), line_of(p0g, r, 0, strip), line_of(p0g, r, 1, strip), support_mid)
    fbuf[0:16, :S0] = flipped_side(gstrip[...])
    for q in range(nc):
        for i in range(I0):
            fbuf[16 + q * B1:16 + (q + 1) * B1, i * TILE:(i + 1) * TILE] = emask[q, i * B1:(i + 1) * B1, :]
    side_e[...] = fbuf[:, :S0].T.astype(bf16)

    def put_e1own(lanes, value):
        e1own[:, lanes] = value

    build(put_e1own, side_e, gmids, 16 + NT1, N1, 2048)
    fine_gain = g["scale_e1"]
    wait_slots(rsin, planes - 1, rs_m)
    total = rsin[0].astype(f32)
    for q in range(1, planes):
        total = total + rsin[q].astype(f32)
    q_high = total[:Q1].astype(bf16)
    mida[own_b, z] = q_high
    z_send(lambda q: mida.at[own_b, z], mida.at[own_b, z], mz_m)
    wait_slots(gtg, nc - 1, g_m)
    gt = gtg[...].reshape(N2, N2)
    gg_high, gg_low = halves(dot(gt.astype(f32).T.astype(bf16), gt))
    zcat[S0 + C1:, :N2] = gg_high
    zcat[S0 + C1:, N2:] = gg_low
    h_high, h_low = halves((fine_gain * g["scale_e2"]) * dot(e1own[...], e2t[...]))
    steps = (dot(h_high, gg_high) + dot(h_low, gg_high) + dot(h_high, gg_low),)
    rows_c = e2t[pl.ds(pl.multiple_of(c * C1, C1), C1), :]
    steps += (g["scale_e2"] * (dot(rows_c, gg_high) + dot(rows_c, gg_low)),)
    for k, step in enumerate(steps):
        high, low = halves(step)
        zcat[k * C1:(k + 1) * C1, :N2] = high
        zcat[k * C1:(k + 1) * C1, N2:] = low

    wait_slots(crecv, D - 1, cr_m)
    cg[d] = jnp.sum(crecv[...].astype(f32), axis=0).astype(bf16)
    all_send(lambda q: cg.at[d], cg.at[d], ca_m)
    mid_start, mid_x, mid_y, mid_d, mid_end, mid_drain = plane_gather(mida, ma_m)
    norm_o[...] = jnp.broadcast_to(jnp.sum(total[Q1:], keepdims=True) * g["norm_scale"], norm_o.shape)
    arrived = mida.at[own_b, pl.ds(0, planes - 1)]
    rc(arrived, arrived, mz_m.at[0], mz_m.at[1], mate, c).wait()
    mid_start()
    mid_x()
    mid_y()
    mid_d()
    wait_slots(cg, D - 1, ca_m)
    cd = cg[...].astype(f32).reshape(N2, -1).astype(bf16)
    both = jnp.concatenate([cd, cd], axis=0)
    coarse_o[...] = dot(zcat[pl.ds(pl.multiple_of(S0 + C1 + r * R2, R2), R2), :], both)
    step = dot(zcat[:S0 + C1, :], both)
    mid_end()
    mid_o[...] = 0.5 * mida[c].astype(f32).reshape(C1, -1) + step[S0:]
    fine_o[...] = 0.5 * own_vals + (0.5 * fine_gain) * dot(e1own[...], mida[...].reshape(N1, -1)) + step[:S0]
    res_drain()
    mid_drain()


def finish_kernel(fine, mid, coarse, norm, fine_o, mid_o, coarse_o, norm_o):
    fine_o[...] = fine[...]
    mid_o[...] = mid[...]
    coarse_o[...] = coarse[...]
    norm_o[...] = norm[0:1, 0:1]


def fits(nr, nc, R0, R1, R2):
    if nr != 4 or nc != 8:
        return False
    if R0 != R1 * nr or R0 != 2 * nc * TILE or 2 * R2 != TILE:
        return False
    return True


def fused(values, points0, points1, points2, tiles_a0, tiles_e1, tiles_a1, factor):
    nr, nc = lax.axis_size("row"), lax.axis_size("col")
    R0, R1, R2 = points0.shape[1], points1.shape[1], points2.shape[1]
    F = values.shape[-1]
    if not fits(nr, nc, R0, R1, R2) or F != TILE:
        return per_device(values, points0, points1, points2, tiles_a0, tiles_e1, tiles_a1, factor)
    D, N2 = nr * nc, nr * R2
    T0, T1 = R0 // TILE, R1 // TILE
    B0, B1 = R0 * nr // nc // TILE, R1 * nr // nc // TILE
    S0 = R0 // nc
    I0 = S0 // TILE
    C1, CR, Q1 = B1 * TILE, N2 // D, R1 * nr // nc // nr
    g = dict(nr=nr, nc=nc, R0=R0, R1=R1, R2=R2, N2=N2,
             scale_a0=(R0 / (nc * tiles_a0.shape[-1] * TILE * TILE)) ** 0.5,
             scale_e1=(R0 / (nc * tiles_e1.shape[-1] * TILE * TILE)) ** 0.5,
             scale_a1=(R1 / (nc * tiles_a1.shape[-1] * TILE * TILE)) ** 0.5,
             scale_e2=(1.0 / (R1 * nr)) ** 0.5,
             norm_scale=1.0 / (R0 * nr * F))
    f32, bf16, i32 = jnp.float32, jnp.bfloat16, jnp.int32
    V = pltpu.VMEM
    dma = pltpu.SemaphoreType.DMA
    wide = N2 // nc
    N1 = nr * R1
    planes = nc // 2
    scratch = [
        V(tiles_a0.shape, i32), V(tiles_e1.shape, i32), V(tiles_a1.shape, i32), V((wide, R2), bf16), V(points2.shape, bf16),
        V((2, R0, F), bf16), V((nr,) + points0.shape, bf16), V((nr,) + points1.shape, bf16), V((nr, 8, TILE), f32),
        V((nc, I0 * B0, TILE), bf16), V((nc, 8, TILE), f32), V((nr, 16, TILE), f32),
        V((nc, I0 * B0, TILE), bf16), V((nc, 8, TILE), f32), V((planes, 16, TILE), f32),
        V((wide, TILE), bf16), V((nr, wide, TILE), bf16), V((nc, wide, N2), bf16),
        V((2, 16, R0), f32), V((16, S0), f32), V((16, R0), f32), V((16, N1), f32), V((16, N1), f32), V((16, N2), f32),
        V((16 + 2 * T0, 2 * R0), bf16), V((16 + T0, R0), bf16), V((16 + nr * T1, N1), bf16), V((16, N2), bf16),
        V((TILE, 2 * S0), f32), V((2 * S0, TILE), bf16), V((S0, TILE), bf16), V((2 * S0, TILE), bf16),
        V((8, TILE), bf16), V((2 * S0, TILE), bf16),
        V((2, S0, 2 * R0), bf16), V((S0, N1), bf16), V((C1, R0), bf16), V((N1, N2), bf16), V((C1, N1), bf16),
        V((S0, F), bf16), V((S0, F), bf16), V((nc, S0, F), bf16),
        V((planes, Q1 + 16, F), bf16), V((planes, Q1 + 16, F), bf16), V((nc, planes, Q1, F), bf16),
        V((D, CR, F), bf16), V((D, CR, F), bf16), V((D, CR, F), bf16), V((N2, 3 * C1), bf16),
        V((S0 + C1 + N2, 2 * N2), bf16),
    ]
    for n in (8, 2, 2, 2, 2, 2, 2, 2, 2, 2, 2, 5, 2, 2, 5, 2, 2):
        scratch += [dma((n,))]
    vm = pl.BlockSpec(memory_space=pltpu.VMEM)
    shapes = ((S0, F), (C1, F), (R2, F))
    parts = pl.pallas_call(
        functools.partial(cycle_kernel, g),
        out_shape=tuple(jax.ShapeDtypeStruct(s, f32) for s in shapes + ((8, TILE),)),
        in_specs=[pl.BlockSpec(memory_space=pltpu.HBM)] * 8,
        out_specs=[vm] * 4,
        scratch_shapes=scratch,
        compiler_params=pltpu.CompilerParams(collective_id=0, has_side_effects=True, vmem_limit_bytes=48 << 20),
    )(*[pltpu.with_memory_space_constraint(x, pltpu.HBM) for x in (
        values, points0, points1, points2, tiles_a0, tiles_e1, tiles_a1, factor.T)])
    fine, mid, coarse, norm = pl.pallas_call(
        finish_kernel,
        grid=(1,),
        out_shape=tuple(jax.ShapeDtypeStruct(s, f32) for s in shapes + ((1, 1),)),
        in_specs=[vm] * 4,
        out_specs=[pl.BlockSpec(s, lambda i: (0, 0)) for s in shapes + ((1, 1),)],
        compiler_params=pltpu.CompilerParams(vmem_limit_bytes=4 << 20),
    )(*parts)
    return (fine, mid, coarse, norm.reshape(1))


def solution(mesh):
    return jax.shard_map(
        fused,
        mesh=mesh,
        in_specs=(
            P("row", None),
            P(None, "row"),
            P(None, "row"),
            P(None, "row"),
            P("row", "col", None, None),
            P("row", "col", None, None),
            P("row", "col", None, None),
            P("row", "col"),
        ),
        out_specs=(P(("row", "col"), None), P("col", None), P("row", None), P()),
        check_vma=False,
    )
```

```python
import functools
import math

import jax
import jax.numpy as jnp
from jax import lax
from jax.experimental import pallas as pl
from jax.experimental.pallas import tpu as pltpu
from jax.sharding import PartitionSpec as P

TILE = 128


support_fine = 0.35
support_mid = 0.55
support_coarse = 0.8


def spread(x, axis, root):
    mine = lax.axis_index(axis) == root
    return lax.psum(jnp.where(mine, x, jnp.zeros_like(x)), axis)


def wendland(left_pts, right_pts, support):
    left = left_pts.astype(jnp.float32)
    right = right_pts.astype(jnp.float32)
    across = left[0][..., :, None] - right[0][..., None, :]
    upward = left[1][..., :, None] - right[1][..., None, :]
    ratio_t = jnp.sqrt(across * across + upward * upward) / support
    margin = jnp.maximum(1.0 - ratio_t, 0.0)
    squared = margin * margin
    return (squared * squared * (4.0 * ratio_t + 1.0)).astype(jnp.bfloat16)


def listed_terms(row_pts, col_pts, listing, vector, support, flipped):
    row_tiles = row_pts.reshape(2, -1, TILE)
    col_tiles = col_pts.reshape(2, -1, TILE)
    listed = listing.shape[-1]
    group = math.gcd(listed, 32)
    order = listing.reshape(2, listed // group, group)
    fields = vector.shape[-1]
    inputs = vector.reshape(-1, TILE, fields)
    target = col_tiles.shape[1] if flipped else row_tiles.shape[1]
    total = jnp.zeros((target, TILE, fields), jnp.float32)

    def add_group(total, pair):
        tile_rows, tile_cols = pair
        kernel = wendland(row_tiles[:, tile_rows], col_tiles[:, tile_cols], support)
        if flipped:
            contrib = jnp.einsum(
                "gij,gir->gjr", kernel, inputs[tile_rows], preferred_element_type=jnp.float32
            )
            return (total.at[tile_cols].add(contrib), None)
        contrib = jnp.einsum(
            "gij,gjr->gir", kernel, inputs[tile_cols], preferred_element_type=jnp.float32
        )
        return (total.at[tile_rows].add(contrib), None)

    total, unused = lax.scan(add_group, total, (order[0], order[1]))
    return total.reshape(-1, fields)


def per_device(values, points0, points1, points2, tiles_a0, tiles_e1, tiles_a1, factor):
    row_count = lax.axis_size("row")
    col_count = lax.axis_size("col")
    col_id = lax.axis_index("col")
    col_per_row = col_count // row_count
    rows_fine, fields = values.shape
    rows_mid = points1.shape[1]
    share = rows_fine // col_count
    cols_fine = rows_fine // col_per_row
    cols_mid = rows_mid // col_per_row
    source = col_id // col_per_row
    part_index = col_id % col_per_row
    value_piece = lax.dynamic_slice_in_dim(values, part_index * cols_fine, cols_fine, 0)
    fine_piece = lax.dynamic_slice_in_dim(points0, part_index * cols_fine, cols_fine, 1)
    mid_piece = lax.dynamic_slice_in_dim(points1, part_index * cols_mid, cols_mid, 1)
    value_cols, fine_cols, mid_cols = (
        spread(value_piece, "row", source),
        spread(fine_piece, "row", source),
        spread(mid_piece, "row", source),
    )
    scale_a0 = (rows_fine / (col_count * tiles_a0.shape[-1] * TILE * TILE)) ** 0.5
    scale_e1 = (rows_fine / (col_count * tiles_e1.shape[-1] * TILE * TILE)) ** 0.5
    scale_a1 = (rows_mid / (col_count * tiles_a1.shape[-1] * TILE * TILE)) ** 0.5
    scale_e2 = (1.0 / (rows_mid * row_count)) ** 0.5
    fine_data = values.astype(jnp.float32)
    own_data = lax.dynamic_slice_in_dim(values, col_id * share, share, 0).astype(jnp.float32)
    product_part = listed_terms(points0, fine_cols, tiles_a0[0, 0], value_cols, support_fine, False)
    product_whole = lax.psum(product_part, "col")
    fine_residual = fine_data - 0.5 * (scale_a0 * product_whole)
    fine_square = jnp.sum(fine_residual * fine_residual)
    restrict_part = listed_terms(
        points0, mid_cols, tiles_e1[0, 0], fine_residual.astype(jnp.bfloat16), support_mid, True
    )
    restrict_sum = lax.psum(restrict_part, "row")
    mid_data = scale_e1 * restrict_sum
    mid_part = listed_terms(
        points1, mid_cols, tiles_a1[0, 0], mid_data.astype(jnp.bfloat16), support_mid, False
    )
    mid_whole = (scale_a1 * lax.psum(mid_part, "col")).astype(jnp.bfloat16)
    mid_slice = lax.dynamic_slice_in_dim(mid_whole, part_index * cols_mid, cols_mid, 0)
    mid_turned = spread(mid_slice, "row", source)
    mid_residual = mid_data - 0.5 * mid_turned.astype(jnp.float32)
    coarse_kernel = wendland(points2, mid_cols, support_coarse)
    coarse_part = jnp.dot(
        coarse_kernel, mid_residual.astype(jnp.bfloat16), preferred_element_type=jnp.float32
    )
    coarse_sum = lax.psum(coarse_part, "col")
    coarse_data = (scale_e2 * coarse_sum).astype(jnp.bfloat16)
    halfway_part = lax.dot_general(
        factor, coarse_data, (((0,), (0,)), ((), ())), preferred_element_type=jnp.float32
    )
    halfway = lax.psum(halfway_part, "row").astype(jnp.bfloat16)
    coarse_part_two = jnp.dot(factor, halfway, preferred_element_type=jnp.float32)
    coarse_coef = lax.psum(coarse_part_two, "col")
    prolong_part = lax.dot_general(
        coarse_kernel,
        coarse_coef.astype(jnp.bfloat16),
        (((0,), (0,)), ((), ())),
        preferred_element_type=jnp.float32,
    )
    mid_coef = 0.5 * mid_data + scale_e2 * lax.psum(prolong_part, "row")
    fine_part = listed_terms(
        points0, mid_cols, tiles_e1[0, 0], mid_coef.astype(jnp.bfloat16), support_mid, False
    )
    fine_coef = 0.5 * own_data + scale_e1 * lax.psum_scatter(
        fine_part, "col", scatter_dimension=0, tiled=True
    )
    fine_total = lax.psum(fine_square / col_count, ("row", "col"))
    fine_norm = fine_total / (rows_fine * row_count * fields)
    return (fine_coef, mid_coef, coarse_coef, jnp.stack([fine_norm]))


FAR = 64.0
MESH = pl.DeviceIdType.MESH


EDGE = 4.0 ** 0.2


def phi_of(square):
    square = jnp.maximum(square, 1e-20)
    margin = jnp.maximum(EDGE - square * lax.rsqrt(square), 0.0)
    squared = margin * margin
    return (squared * squared * (1.25 * EDGE - margin)).astype(jnp.bfloat16)


def dot(a, b):
    return jnp.dot(a, b, preferred_element_type=jnp.float32)


def far_rows(tiles, row_tiles, col_tiles, by_col):
    row, col = tiles[0, 0, 0:1, :], tiles[0, 0, 1:2, :]
    key = col * row_tiles + row if by_col else row * col_tiles + col
    count = row_tiles * col_tiles
    place = lax.broadcasted_iota(jnp.int32, (count, key.shape[1]), 0)
    near = jnp.max(jnp.where(place == key, 1.0, 0.0), axis=1, keepdims=True)
    return jnp.broadcast_to(FAR * (1.0 - near), (count, TILE))


def halves(x):
    high = x.astype(jnp.bfloat16)
    return high, (x - high.astype(jnp.float32)).astype(jnp.bfloat16)


def pieces(x):
    first = x.astype(jnp.bfloat16).astype(jnp.float32)
    second = (x - first).astype(jnp.bfloat16).astype(jnp.float32)
    return first, second, x - first - second


def describe(ref, lanes, x, y, support):
    square = (EDGE / support) ** 2
    lines = pieces(-2.0 * square * x) + pieces(-2.0 * square * y) + pieces(square * (x * x + y * y))
    for k, line in enumerate(lines):
        ref[k:k + 1, lanes] = line
    ref[12:13, lanes] = x
    ref[13:14, lanes] = y


def flipped_side(sides):
    x, y = sides[12:13], sides[13:14]
    one = jnp.ones_like(x)
    return jnp.concatenate([x, x, x, y, y, y, one, one, one, sides[6:9], jnp.zeros((4, x.shape[1]), jnp.float32)], axis=0)


def cycle_kernel(g, vals_h, points0_h, points1_h, points2_h, tiles_a0_h, tiles_e1_h, tiles_a1_h, factor_h,
                 fine_o, mid_o, coarse_o, norm_o,
                 tiles_a0, tiles_e1, tiles_a1, factor, points2,
                 v2, p0g, p1g, pcg, maskg, emask, tmask, masks_s, emask_s, tmask_s, fac, facg, gtg,
                 gall, gstrip, gpl, gmid, gmid2, gcoarse, gfine, gplane, gmids, gcs, fbuf, side_a, side_e, side_t, side_o, side_m,
                 a0, e1own, e1t, e2t, a1t, other_s, other_r, resg, part_buf, rsin, mida, csend, crecv, cg, wcat, zcat,
                 l_s, a_m, p0_m, p1_m, pc_m, v_m, em_m, tm_m, f_m, g_m, ot_m, re_m, rs_m, mz_m, ma_m, cr_m, ca_m):
    nr, nc, R0, R1, R2 = g["nr"], g["nc"], g["R0"], g["R1"], g["R2"]
    D = nr * nc
    T0, T1 = R0 // TILE, R1 // TILE
    C0, C1 = R0 * nr // nc, R1 * nr // nc
    B0, B1 = C0 // TILE, C1 // TILE
    S0 = R0 // nc
    I0 = S0 // TILE
    Q1 = C1 // nr
    N1, N2 = nr * R1, g["N2"]
    CR = N2 // D
    NT1 = nr * T1
    NT2 = N2 // TILE
    f32, bf16 = jnp.float32, jnp.bfloat16
    r = lax.axis_index("row")
    c = lax.axis_index("col")
    d = r * nc + c
    y, k_core = r // 2, lax.rem(r, 2)
    z, h = c // 2, lax.rem(c, 2)
    mate = r + 1 - 2 * k_core
    yp = lax.rem(r + 2, nr)
    diag = lax.rem(mate + 2, nr)
    xp = c + 1 - 2 * h
    own_b = 2 * r + h

    def rc(src, dst, ssem, rsem, rr, cc):
        return pltpu.make_async_remote_copy(src_ref=src, dst_ref=dst, send_sem=ssem, recv_sem=rsem,
                                            device_id=(rr, cc), device_id_type=MESH)

    def each(lo, hi, f):
        def body(k, carry):
            f(k)
            return carry
        lax.fori_loop(lo, hi, body, 0)

    barrier = pltpu.get_barrier_semaphore()

    def greet(k):
        q = lax.rem(c + k, nc)
        for j in range(nr):
            pl.semaphore_signal(barrier, inc=1, device_id=(lax.rem(r + j, nr), q), device_id_type=MESH)

    each(1, nc, greet)
    for j in range(1, nr):
        pl.semaphore_signal(barrier, inc=1, device_id=(lax.rem(r + j, nr), c), device_id_type=MESH)
    loads = [pltpu.make_async_copy(s, t, l_s.at[k]) for k, (s, t) in enumerate((
        (points0_h, p0g.at[r]), (points1_h, p1g.at[r]), (points2_h, points2), (tiles_a0_h, tiles_a0),
        (tiles_e1_h, tiles_e1), (tiles_a1_h, tiles_a1), (factor_h, factor), (vals_h, v2.at[k_core])))]
    for load in loads:
        load.start()

    def one_hot(ref, rows, columns):
        ref[16:16 + rows] = jnp.where(lax.broadcasted_iota(jnp.int32, (rows, columns), 1) // TILE
                                      == lax.broadcasted_iota(jnp.int32, (rows, columns), 0), 1.0, 0.0).astype(bf16)

    one_hot(gfine, 2 * T0, 2 * R0)
    one_hot(gplane, T0, R0)
    one_hot(gmids, NT1, N1)
    fbuf[...] = jnp.zeros_like(fbuf)
    emask_s[...] = jnp.zeros_like(emask_s)
    tmask_s[...] = jnp.zeros_like(tmask_s)
    for ref in (gall, gstrip, gpl, gmid, gmid2, gcoarse):
        ref[...] = jnp.ones_like(ref)
    for load in loads[:-1]:
        load.wait()
    far_a0 = far_rows(tiles_a0, T0, B0, False)
    far_e1 = far_rows(tiles_e1, T0, B1, False)
    for q in range(nc):
        masks_s[q] = far_a0[q * I0 * B0:(q + 1) * I0 * B0].astype(bf16)
        emask_s[q, :I0 * B1] = far_e1[q * I0 * B1:(q + 1) * I0 * B1]
    far_e1 = far_rows(tiles_e1, T0, B1, True)
    far_a1 = far_rows(tiles_a1, T1, B1, True)
    planes = nc // 2
    PT = T0 // planes
    for q in range(planes):
        for j in range(B1):
            tmask_s[q, j * PT:(j + 1) * PT] = far_e1[j * T0 + q * PT:j * T0 + (q + 1) * PT]
        tmask_s[q, B1 * PT:B1 * PT + B1 * T1] = far_a1
    half_of = lax.rem(r, TILE // R2)
    raw = factor[...].astype(f32)
    fac[...] = jnp.concatenate([jnp.where(half_of == k, raw, 0.0) for k in range(TILE // R2)], axis=1).astype(bf16)
    line = points2[...].astype(f32)
    pcg[r] = jnp.zeros((8, TILE), f32)
    pcg[r, 0:2] = jnp.concatenate([jnp.where(half_of == k, line, 0.0) for k in range(TILE // R2)], axis=1)
    loads[-1].wait()
    pl.semaphore_wait(barrier, D - 1)

    def row_send(src, dst, m):
        for k in range(1, nr):
            rc(src, dst, m.at[0], m.at[1], lax.rem(r + k, nr), c).start()

    def row_wait(ref, m):
        slots = ref.at[pl.ds(0, nr - 1)]
        rc(slots, slots, m.at[0], m.at[1], mate, c).wait()

    def col_send(src_of, dst, m):
        def go(k):
            q = lax.rem(c + k, nc)
            rc(src_of(q), dst, m.at[0], m.at[1], r, q).start()
        each(1, nc, go)

    y_of = c // planes
    mask_row = 2 * y_of + k_core
    mask_slot = jnp.where(y_of == y, 0, 1) * planes + lax.rem(c, planes)
    mask_self = y_of == y

    def mask_go(k):
        q = lax.rem(c + k, nc)
        rc(masks_s.at[q], maskg.at[mask_slot], a_m.at[0], a_m.at[1], mask_row, q).start()

    each(1, nc, mask_go)

    @pl.when(jnp.logical_not(mask_self))
    def _():
        mask_go(0)

    @pl.when(mask_self)
    def _():
        maskg[mask_slot] = masks_s[c]

    row_send(p0g.at[r], p0g.at[r], p0_m)
    rc(v2.at[k_core], v2.at[k_core], v_m.at[0], v_m.at[1], mate, c).start()
    row_send(p1g.at[r], p1g.at[r], p1_m)
    row_send(pcg.at[r], pcg.at[r], pc_m)
    tmask_self = c // 2 == r

    def tmask_go(q):
        rc(tmask_s.at[q], tmask.at[r], tm_m.at[0], tm_m.at[1], c // 2, 2 * q + h).start()

    for k in range(1, planes):
        tmask_go(lax.rem(z + k, planes))

    @pl.when(jnp.logical_not(tmask_self))
    def _():
        tmask_go(z)

    @pl.when(tmask_self)
    def _():
        tmask[r] = tmask_s[z]

    col_send(lambda q: emask_s.at[q], emask.at[c], em_m)
    row_send(fac, facg.at[r], f_m)
    emask[c] = emask_s[c]
    facg[r] = fac[...]

    def line_of(ref, q, way, lanes=slice(None)):
        return ref[q, way:way + 1, lanes].astype(f32)

    def describe_own(rb, slot):
        describe(gall.at[slot], slice(None), line_of(p0g, rb, 0), line_of(p0g, rb, 1), support_fine)
        gfine[:16, pl.ds(pl.multiple_of(slot * R0, R0), R0)] = gall[slot].astype(bf16)

    strip = pl.ds(pl.multiple_of(c * S0, S0), S0)
    describe_own(r, k_core)
    row_wait(p0g, p0_m)
    describe_own(mate, 1 - k_core)
    describe(gstrip, slice(None), line_of(p0g, yp, 0, strip), line_of(p0g, yp, 1, strip), support_fine)
    fbuf[0:16, :S0] = flipped_side(gall[k_core, :, strip])
    fbuf[0:16, S0:] = flipped_side(gstrip[...])

    def wait_slots(ref, n, m):
        slots = ref.at[pl.ds(0, n)]
        rc(slots, slots, m.at[0], m.at[1], mate, c).wait()

    @pl.when(mask_self)
    def _():
        wait_slots(maskg, nc - 1, a_m)

    @pl.when(jnp.logical_not(mask_self))
    def _():
        wait_slots(maskg, nc, a_m)

    for s in range(2):
        for q in range(planes):
            rows = maskg[s * planes + q].astype(f32)
            for i in range(I0):
                fbuf[16 + q * B0:16 + (q + 1) * B0, (s * I0 + i) * TILE:(s * I0 + i + 1) * TILE] = rows[i * B0:(i + 1) * B0]
    side_a[...] = fbuf[...].T.astype(bf16)

    def build(put, side, sides, depth, columns, step):
        def go(k):
            lanes = pl.ds(pl.multiple_of(k * step, step), step)
            put(lanes, phi_of(dot(side[:, :depth], sides[:depth, lanes])))
        each(0, columns // step, go)

    def put_a0(s):
        def put(lanes, value):
            a0[s, :, lanes] = value
        return put

    KA = 16 + 2 * T0
    def product(s, lo, hi):
        total = None
        for k in range(2):
            lanes = slice(k * R0, (k + 1) * R0)
            a0[s, lo:hi, lanes] = phi_of(dot(side_a[s * S0 + lo:s * S0 + hi, :KA], gfine[:KA, lanes]))
            if s == 1 and lo == 0 and k == 0:
                rc(v2.at[1 - k_core], v2.at[1 - k_core], v_m.at[0], v_m.at[1], mate, c).wait()
            term = dot(a0[s, lo:hi, lanes], v2[k])
            total = term if total is None else total + term
        return total

    def other_copy(i):
        rows = pl.ds(i * TILE, TILE)
        return rc(other_s.at[rows], other_r.at[rows], ot_m.at[0], ot_m.at[1 + i], yp, c)

    for i in range(I0):
        other_s[i * TILE:(i + 1) * TILE] = product(1, i * TILE, (i + 1) * TILE).astype(bf16)
        other_copy(i).start()
    acc = product(0, 0, S0)
    own_vals = v2[k_core, strip, :].astype(f32)
    x_slot, y_slot, d_slot = 2 * r + 1 - h, 2 * yp + h, 2 * diag + 1 - h

    def plane_gather(at, m, base, mate_sem):
        def send(slot, sem, rr, cc):
            rc(at(slot), at(slot), m.at[0], m.at[sem], rr, cc).start()

        def start():
            send(own_b, base, r, xp)
            send(own_b, base + 1, yp, c)
            send(own_b, base + 2, diag, xp)
            send(own_b, mate_sem, mate, c)

        def relay(slot, sem):
            rc(at(slot), at(slot), m.at[0], m.at[sem], mate, c).wait_recv()
            send(slot, mate_sem, mate, c)

        return (start, functools.partial(relay, x_slot, base), functools.partial(relay, y_slot, base + 1),
                functools.partial(relay, d_slot, base + 2))

    def plane_end(ref, m, mate_sem):
        part = ref.at[pl.ds(0, 4)]
        rc(part, part, m.at[0], m.at[mate_sem], mate, c).wait_recv()

    def plane_drain(ref, m, mate_sem):
        part = ref.at[pl.ds(0, 7)]
        rc(part, part, m.at[0], m.at[mate_sem], mate, c).wait_send()

    def all_send(src_of, dst, m):
        def go(k):
            q = lax.rem(c + k, nc)
            for j in range(nr):
                p = lax.rem(r + j, nr)
                rc(src_of(p * nc + q), dst, m.at[0], m.at[1], p, q).start()
        each(1, nc, go)
        for j in range(1, nr):
            p = lax.rem(r + j, nr)
            rc(src_of(p * nc + c), dst, m.at[0], m.at[1], p, c).start()

    def res_part(i):
        return plane_gather(lambda slot: resg.at[slot, pl.ds(i * TILE, TILE)], re_m, 1 + 3 * i, 7)

    res_parts = [res_part(i) for i in range(I0)]
    for i in range(I0):
        other_copy(i).wait_recv()
        rows = slice(i * TILE, (i + 1) * TILE)
        resg[own_b, rows] = (own_vals[rows] - (0.5 * g["scale_a0"]) * (acc[rows] + other_r[rows].astype(f32))).astype(bf16)
        res_parts[i][0]()
    PL = PT * TILE
    plane_lanes = pl.ds(pl.multiple_of(z * PL, PL), PL)
    row_wait(p1g, p1_m)
    for q in range(nr):
        describe(gpl, slice(q * PL, (q + 1) * PL), line_of(p0g, q, 0, plane_lanes), line_of(p0g, q, 1, plane_lanes), support_mid)
        lanes = slice(q * R1, (q + 1) * R1)
        describe(gmid, lanes, line_of(p1g, q, 0), line_of(p1g, q, 1), support_mid)
    gplane[:16] = gpl[...].astype(bf16)
    gmids[:16] = gmid[...].astype(bf16)

    @pl.when(tmask_self)
    def _():
        wait_slots(tmask, nr - 1, tm_m)

    @pl.when(jnp.logical_not(tmask_self))
    def _():
        wait_slots(tmask, nr, tm_m)

    block = pl.ds(pl.multiple_of(own_b * C1, C1), C1)
    fbuf[0:16, :C1] = flipped_side(gmid[:, block])
    fbuf[0:16, C1:] = fbuf[0:16, :C1]
    for q in range(nr):
        for j in range(B1):
            fbuf[16 + q * PT:16 + (q + 1) * PT, j * TILE:(j + 1) * TILE] = tmask[q, j * PT:(j + 1) * PT, :]
            at = B1 * PT + j * T1
            fbuf[16 + q * T1:16 + (q + 1) * T1, C1 + j * TILE:C1 + (j + 1) * TILE] = tmask[q, at:at + T1, :]
    side_t[...] = fbuf[...].T.astype(bf16)

    def put_e1t(lanes, value):
        e1t[:, lanes] = value

    build(put_e1t, side_t.at[pl.ds(0, C1)], gplane, 16 + T0, R0, 2048)
    row_wait(pcg, pc_m)
    row_wait(facg, f_m)
    def put_a1t(lanes, value):
        a1t[:, lanes] = value

    build(put_a1t, side_t.at[pl.ds(C1, C1)], gmids, 16 + NT1, N1, 1024)
    for k in range(1, 4):
        res_parts[0][k]()
    strips = []
    per = TILE // R2
    for lane in range(NT2):
        total = facg[lane * per].astype(f32)
        for k in range(1, per):
            total = total + facg[lane * per + k].astype(f32)
        strips.append(total)
    gtg[c] = jnp.concatenate(strips, axis=1).astype(bf16)
    col_send(lambda q: gtg.at[c], gtg.at[c], g_m)
    for t in range(NT2):
        line = pcg[per * t] + pcg[per * t + 1]
        describe(gcoarse, slice(t * TILE, (t + 1) * TILE), line[0:1], line[1:2], support_coarse)
    gcs[...] = gcoarse[...].astype(bf16)
    for q in range(nr):
        describe(gmid2, slice(q * R1, (q + 1) * R1), line_of(p1g, q, 0), line_of(p1g, q, 1), support_coarse)
    wide = fbuf.shape[1]
    for q in range(N1 // wide):
        fbuf[0:16] = flipped_side(gmid2[:, q * wide:(q + 1) * wide])
        side_m[...] = fbuf[...].T.astype(bf16)
        e2t[q * wide:(q + 1) * wide] = phi_of(dot(side_m[:, :16], gcs[...]))
    for k in range(1, 4):
        res_parts[1][k]()
    restricted = jnp.zeros((C1, resg.shape[-1]), f32)
    square = jnp.zeros((16, resg.shape[-1]), f32)

    def restrict(slot):
        strip_data = resg[slot]
        held = strip_data.astype(f32)
        return (dot(e1t[:, pl.ds(pl.multiple_of(slot * S0, S0), S0)], strip_data),
                jnp.sum((held * held).reshape(S0 // 16, 16, -1), axis=0))

    for slot in (own_b, x_slot, y_slot, d_slot):
        term = restrict(slot)
        restricted, square = restricted + term[0], square + term[1]
    plane_end(resg, re_m, 7)
    for slot in (2 * mate + h, 2 * mate + 1 - h, 2 * diag + h, 2 * yp + 1 - h):
        term = restrict(slot)
        restricted, square = restricted + term[0], square + term[1]
    restricted = g["scale_e1"] * restricted
    for q in range(planes):
        part_buf[q] = jnp.concatenate([restricted[q * Q1:(q + 1) * Q1], square], axis=0).astype(bf16)

    def z_send(src_of, dst, m):
        for k in range(1, planes):
            q = lax.rem(z + k, planes)
            rc(src_of(q), dst, m.at[0], m.at[1], r, 2 * q + h).start()

    z_send(lambda q: part_buf.at[q], rsin.at[z], rs_m)
    rsin[z] = part_buf[z]
    turned_w = g["scale_e2"] * (e2t[block, :].astype(f32) - (0.5 * g["scale_a1"]) * dot(a1t[...], e2t[...]))
    w_high, w_low = halves(turned_w.T)
    for k, w in enumerate((w_high, w_low, w_high)):
        wcat[:, k * C1:(k + 1) * C1] = w

    part_high, part_low = halves(restricted)
    part = dot(wcat[...], jnp.concatenate([part_high, part_high, part_low], axis=0))
    csend[...] = part.reshape(D, CR, -1).astype(bf16)
    all_send(lambda q: csend.at[q], crecv.at[d], cr_m)
    crecv[d] = csend[d]
    wait_slots(emask, nc - 1, em_m)
    describe(gstrip, slice(None), line_of(p0g, r, 0, strip), line_of(p0g, r, 1, strip), support_mid)
    fbuf[0:16, :S0] = flipped_side(gstrip[...])
    for q in range(nc):
        for i in range(I0):
            fbuf[16 + q * B1:16 + (q + 1) * B1, i * TILE:(i + 1) * TILE] = emask[q, i * B1:(i + 1) * B1, :]
    side_e[...] = fbuf[:, :S0].T.astype(bf16)

    def put_e1own(lanes, value):
        e1own[:, lanes] = value

    build(put_e1own, side_e, gmids, 16 + NT1, N1, 2048)
    fine_gain = g["scale_e1"]
    wait_slots(rsin, planes - 1, rs_m)
    total = rsin[0].astype(f32)
    for q in range(1, planes):
        total = total + rsin[q].astype(f32)
    q_high = total[:Q1].astype(bf16)
    mida[own_b, z] = q_high
    own_q = mida.at[own_b, z]
    near_z = z + 1 - 2 * lax.rem(z, 2)
    rc(own_q, own_q, mz_m.at[0], mz_m.at[1], r, 2 * near_z + h).start()
    rank = jnp.where((z == 0) | (z == planes - 1), 3, 2)
    for k in range(2):
        q = jnp.where(z < 2, 2 + k, k)
        rc(own_q, own_q, mz_m.at[0], mz_m.at[rank], r, 2 * q + h).start()
    order = (z, near_z, jnp.where(z < 2, 2, 1), jnp.where(z < 2, 3, 0))

    def batch(k):
        return plane_gather(lambda slot: mida.at[slot, order[k]], ma_m, 1 + 3 * k, 13)

    batches = [batch(k) for k in range(planes)]
    batches[0][0]()
    wait_slots(gtg, nc - 1, g_m)
    gt = gtg[...].reshape(N2, N2)
    gg_high, gg_low = halves(dot(gt.astype(f32).T.astype(bf16), gt))
    zcat[S0 + C1:, :N2] = gg_high
    zcat[S0 + C1:, N2:] = gg_low
    h_high, h_low = halves((fine_gain * g["scale_e2"]) * dot(e1own[...], e2t[...]))
    steps = (dot(h_high, gg_high) + dot(h_low, gg_high) + dot(h_high, gg_low),)
    rows_c = e2t[pl.ds(pl.multiple_of(c * C1, C1), C1), :]
    steps += (g["scale_e2"] * (dot(rows_c, gg_high) + dot(rows_c, gg_low)),)
    for k, step in enumerate(steps):
        high, low = halves(step)
        zcat[k * C1:(k + 1) * C1, :N2] = high
        zcat[k * C1:(k + 1) * C1, N2:] = low

    def z_take(k):
        piece = mida.at[own_b, order[k]]
        rc(piece, piece, mz_m.at[0], mz_m.at[k], mate, c).wait_recv()
        batches[k][0]()

    wait_slots(crecv, D - 1, cr_m)
    cg[d] = jnp.sum(crecv[...].astype(f32), axis=0).astype(bf16)
    all_send(lambda q: cg.at[d], cg.at[d], ca_m)
    for k in range(1, 4):
        batches[0][k]()
    z_take(1)
    z_take(2)
    z_take(3)
    norm_o[...] = jnp.broadcast_to(jnp.sum(total[Q1:], keepdims=True) * g["norm_scale"], norm_o.shape)
    for b in batches[1:]:
        for k in range(1, 4):
            b[k]()
    wait_slots(cg, D - 1, ca_m)
    cd = cg[...].astype(f32).reshape(N2, -1).astype(bf16)
    both = jnp.concatenate([cd, cd], axis=0)
    coarse_o[...] = dot(zcat[pl.ds(pl.multiple_of(S0 + C1 + r * R2, R2), R2), :], both)
    step = dot(zcat[:S0 + C1, :], both)
    plane_end(mida, ma_m, 13)
    mid_o[...] = 0.5 * mida[c].astype(f32).reshape(C1, -1) + step[S0:]
    fine_o[...] = 0.5 * own_vals + (0.5 * fine_gain) * dot(e1own[...], mida[...].reshape(N1, -1)) + step[:S0]
    rc(other_s, other_r, ot_m.at[0], ot_m.at[1], yp, c).wait_send()
    plane_drain(resg, re_m, 7)
    plane_drain(mida, ma_m, 13)
    held_z = mida.at[own_b, pl.ds(0, planes - 1)]
    rc(held_z, held_z, mz_m.at[0], mz_m.at[1], mate, c).wait_send()


def finish_kernel(fine, mid, coarse, norm, fine_o, mid_o, coarse_o, norm_o):
    fine_o[...] = fine[...]
    mid_o[...] = mid[...]
    coarse_o[...] = coarse[...]
    norm_o[...] = norm[0:1, 0:1]


def fits(nr, nc, R0, R1, R2):
    if nr != 4 or nc != 8:
        return False
    if R0 != R1 * nr or R0 != 2 * nc * TILE or 2 * R2 != TILE:
        return False
    return True


def fused(values, points0, points1, points2, tiles_a0, tiles_e1, tiles_a1, factor):
    nr, nc = lax.axis_size("row"), lax.axis_size("col")
    R0, R1, R2 = points0.shape[1], points1.shape[1], points2.shape[1]
    F = values.shape[-1]
    if not fits(nr, nc, R0, R1, R2) or F != TILE:
        return per_device(values, points0, points1, points2, tiles_a0, tiles_e1, tiles_a1, factor)
    D, N2 = nr * nc, nr * R2
    T0, T1 = R0 // TILE, R1 // TILE
    B0, B1 = R0 * nr // nc // TILE, R1 * nr // nc // TILE
    S0 = R0 // nc
    I0 = S0 // TILE
    C1, CR, Q1 = B1 * TILE, N2 // D, R1 * nr // nc // nr
    g = dict(nr=nr, nc=nc, R0=R0, R1=R1, R2=R2, N2=N2,
             scale_a0=(R0 / (nc * tiles_a0.shape[-1] * TILE * TILE)) ** 0.5,
             scale_e1=(R0 / (nc * tiles_e1.shape[-1] * TILE * TILE)) ** 0.5,
             scale_a1=(R1 / (nc * tiles_a1.shape[-1] * TILE * TILE)) ** 0.5,
             scale_e2=(1.0 / (R1 * nr)) ** 0.5,
             norm_scale=1.0 / (R0 * nr * F))
    f32, bf16, i32 = jnp.float32, jnp.bfloat16, jnp.int32
    V = pltpu.VMEM
    dma = pltpu.SemaphoreType.DMA
    wide = N2 // nc
    N1 = nr * R1
    planes = nc // 2
    scratch = [
        V(tiles_a0.shape, i32), V(tiles_e1.shape, i32), V(tiles_a1.shape, i32), V((wide, R2), bf16), V(points2.shape, bf16),
        V((2, R0, F), bf16), V((nr,) + points0.shape, bf16), V((nr,) + points1.shape, bf16), V((nr, 8, TILE), f32),
        V((nc, I0 * B0, TILE), bf16), V((nc, 8, TILE), f32), V((nr, 16, TILE), f32),
        V((nc, I0 * B0, TILE), bf16), V((nc, 8, TILE), f32), V((planes, 16, TILE), f32),
        V((wide, TILE), bf16), V((nr, wide, TILE), bf16), V((nc, wide, N2), bf16),
        V((2, 16, R0), f32), V((16, S0), f32), V((16, R0), f32), V((16, N1), f32), V((16, N1), f32), V((16, N2), f32),
        V((16 + 2 * T0, 2 * R0), bf16), V((16 + T0, R0), bf16), V((16 + nr * T1, N1), bf16), V((16, N2), bf16),
        V((TILE, 2 * S0), f32), V((2 * S0, TILE), bf16), V((S0, TILE), bf16), V((2 * S0, TILE), bf16),
        V((8, TILE), bf16), V((2 * S0, TILE), bf16),
        V((2, S0, 2 * R0), bf16), V((S0, N1), bf16), V((C1, R0), bf16), V((N1, N2), bf16), V((C1, N1), bf16),
        V((S0, F), bf16), V((S0, F), bf16), V((nc, S0, F), bf16),
        V((planes, Q1 + 16, F), bf16), V((planes, Q1 + 16, F), bf16), V((nc, planes, Q1, F), bf16),
        V((D, CR, F), bf16), V((D, CR, F), bf16), V((D, CR, F), bf16), V((N2, 3 * C1), bf16),
        V((S0 + C1 + N2, 2 * N2), bf16),
    ]
    for n in (8, 2, 2, 2, 2, 2, 2, 2, 2, 2, 1 + I0, 2 + 3 * I0, 2, 4, 14, 2, 2):
        scratch += [dma((n,))]
    vm = pl.BlockSpec(memory_space=pltpu.VMEM)
    shapes = ((S0, F), (C1, F), (R2, F))
    parts = pl.pallas_call(
        functools.partial(cycle_kernel, g),
        out_shape=tuple(jax.ShapeDtypeStruct(s, f32) for s in shapes + ((8, TILE),)),
        in_specs=[pl.BlockSpec(memory_space=pltpu.HBM)] * 8,
        out_specs=[vm] * 4,
        scratch_shapes=scratch,
        compiler_params=pltpu.CompilerParams(collective_id=0, has_side_effects=True, vmem_limit_bytes=48 << 20),
    )(*[pltpu.with_memory_space_constraint(x, pltpu.HBM) for x in (
        values, points0, points1, points2, tiles_a0, tiles_e1, tiles_a1, factor.T)])
    fine, mid, coarse, norm = pl.pallas_call(
        finish_kernel,
        grid=(1,),
        out_shape=tuple(jax.ShapeDtypeStruct(s, f32) for s in shapes + ((1, 1),)),
        in_specs=[vm] * 4,
        out_specs=[pl.BlockSpec(s, lambda i: (0, 0)) for s in shapes + ((1, 1),)],
        compiler_params=pltpu.CompilerParams(vmem_limit_bytes=4 << 20),
    )(*parts)
    return (fine, mid, coarse, norm.reshape(1))


def solution(mesh):
    return jax.shard_map(
        fused,
        mesh=mesh,
        in_specs=(
            P("row", None),
            P(None, "row"),
            P(None, "row"),
            P(None, "row"),
            P("row", "col", None, None),
            P("row", "col", None, None),
            P("row", "col", None, None),
            P("row", "col"),
        ),
        out_specs=(P(("row", "col"), None), P("col", None), P("row", None), P()),
        check_vma=False,
    )
```

```python
import functools
import math

import jax
import jax.numpy as jnp
from jax import lax
from jax.experimental import pallas as pl
from jax.experimental.pallas import tpu as pltpu
from jax.sharding import PartitionSpec as P

TILE = 128


support_fine = 0.35
support_mid = 0.55
support_coarse = 0.8


def spread(x, axis, root):
    mine = lax.axis_index(axis) == root
    return lax.psum(jnp.where(mine, x, jnp.zeros_like(x)), axis)


def wendland(left_pts, right_pts, support):
    left = left_pts.astype(jnp.float32)
    right = right_pts.astype(jnp.float32)
    across = left[0][..., :, None] - right[0][..., None, :]
    upward = left[1][..., :, None] - right[1][..., None, :]
    ratio_t = jnp.sqrt(across * across + upward * upward) / support
    margin = jnp.maximum(1.0 - ratio_t, 0.0)
    squared = margin * margin
    return (squared * squared * (4.0 * ratio_t + 1.0)).astype(jnp.bfloat16)


def listed_terms(row_pts, col_pts, listing, vector, support, flipped):
    row_tiles = row_pts.reshape(2, -1, TILE)
    col_tiles = col_pts.reshape(2, -1, TILE)
    listed = listing.shape[-1]
    group = math.gcd(listed, 32)
    order = listing.reshape(2, listed // group, group)
    fields = vector.shape[-1]
    inputs = vector.reshape(-1, TILE, fields)
    target = col_tiles.shape[1] if flipped else row_tiles.shape[1]
    total = jnp.zeros((target, TILE, fields), jnp.float32)

    def add_group(total, pair):
        tile_rows, tile_cols = pair
        kernel = wendland(row_tiles[:, tile_rows], col_tiles[:, tile_cols], support)
        if flipped:
            contrib = jnp.einsum(
                "gij,gir->gjr", kernel, inputs[tile_rows], preferred_element_type=jnp.float32
            )
            return (total.at[tile_cols].add(contrib), None)
        contrib = jnp.einsum(
            "gij,gjr->gir", kernel, inputs[tile_cols], preferred_element_type=jnp.float32
        )
        return (total.at[tile_rows].add(contrib), None)

    total, unused = lax.scan(add_group, total, (order[0], order[1]))
    return total.reshape(-1, fields)


def per_device(values, points0, points1, points2, tiles_a0, tiles_e1, tiles_a1, factor):
    row_count = lax.axis_size("row")
    col_count = lax.axis_size("col")
    col_id = lax.axis_index("col")
    col_per_row = col_count // row_count
    rows_fine, fields = values.shape
    rows_mid = points1.shape[1]
    share = rows_fine // col_count
    cols_fine = rows_fine // col_per_row
    cols_mid = rows_mid // col_per_row
    source = col_id // col_per_row
    part_index = col_id % col_per_row
    value_piece = lax.dynamic_slice_in_dim(values, part_index * cols_fine, cols_fine, 0)
    fine_piece = lax.dynamic_slice_in_dim(points0, part_index * cols_fine, cols_fine, 1)
    mid_piece = lax.dynamic_slice_in_dim(points1, part_index * cols_mid, cols_mid, 1)
    value_cols, fine_cols, mid_cols = (
        spread(value_piece, "row", source),
        spread(fine_piece, "row", source),
        spread(mid_piece, "row", source),
    )
    scale_a0 = (rows_fine / (col_count * tiles_a0.shape[-1] * TILE * TILE)) ** 0.5
    scale_e1 = (rows_fine / (col_count * tiles_e1.shape[-1] * TILE * TILE)) ** 0.5
    scale_a1 = (rows_mid / (col_count * tiles_a1.shape[-1] * TILE * TILE)) ** 0.5
    scale_e2 = (1.0 / (rows_mid * row_count)) ** 0.5
    fine_data = values.astype(jnp.float32)
    own_data = lax.dynamic_slice_in_dim(values, col_id * share, share, 0).astype(jnp.float32)
    product_part = listed_terms(points0, fine_cols, tiles_a0[0, 0], value_cols, support_fine, False)
    product_whole = lax.psum(product_part, "col")
    fine_residual = fine_data - 0.5 * (scale_a0 * product_whole)
    fine_square = jnp.sum(fine_residual * fine_residual)
    restrict_part = listed_terms(
        points0, mid_cols, tiles_e1[0, 0], fine_residual.astype(jnp.bfloat16), support_mid, True
    )
    restrict_sum = lax.psum(restrict_part, "row")
    mid_data = scale_e1 * restrict_sum
    mid_part = listed_terms(
        points1, mid_cols, tiles_a1[0, 0], mid_data.astype(jnp.bfloat16), support_mid, False
    )
    mid_whole = (scale_a1 * lax.psum(mid_part, "col")).astype(jnp.bfloat16)
    mid_slice = lax.dynamic_slice_in_dim(mid_whole, part_index * cols_mid, cols_mid, 0)
    mid_turned = spread(mid_slice, "row", source)
    mid_residual = mid_data - 0.5 * mid_turned.astype(jnp.float32)
    coarse_kernel = wendland(points2, mid_cols, support_coarse)
    coarse_part = jnp.dot(
        coarse_kernel, mid_residual.astype(jnp.bfloat16), preferred_element_type=jnp.float32
    )
    coarse_sum = lax.psum(coarse_part, "col")
    coarse_data = (scale_e2 * coarse_sum).astype(jnp.bfloat16)
    halfway_part = lax.dot_general(
        factor, coarse_data, (((0,), (0,)), ((), ())), preferred_element_type=jnp.float32
    )
    halfway = lax.psum(halfway_part, "row").astype(jnp.bfloat16)
    coarse_part_two = jnp.dot(factor, halfway, preferred_element_type=jnp.float32)
    coarse_coef = lax.psum(coarse_part_two, "col")
    prolong_part = lax.dot_general(
        coarse_kernel,
        coarse_coef.astype(jnp.bfloat16),
        (((0,), (0,)), ((), ())),
        preferred_element_type=jnp.float32,
    )
    mid_coef = 0.5 * mid_data + scale_e2 * lax.psum(prolong_part, "row")
    fine_part = listed_terms(
        points0, mid_cols, tiles_e1[0, 0], mid_coef.astype(jnp.bfloat16), support_mid, False
    )
    fine_coef = 0.5 * own_data + scale_e1 * lax.psum_scatter(
        fine_part, "col", scatter_dimension=0, tiled=True
    )
    fine_total = lax.psum(fine_square / col_count, ("row", "col"))
    fine_norm = fine_total / (rows_fine * row_count * fields)
    return (fine_coef, mid_coef, coarse_coef, jnp.stack([fine_norm]))


FAR = 64.0
MESH = pl.DeviceIdType.MESH


EDGE = 4.0 ** 0.2


def phi_of(square):
    square = jnp.maximum(square, 1e-20)
    margin = jnp.maximum(EDGE - square * lax.rsqrt(square), 0.0)
    squared = margin * margin
    return (squared * squared * (1.25 * EDGE - margin)).astype(jnp.bfloat16)


def dot(a, b):
    return jnp.dot(a, b, preferred_element_type=jnp.float32)


def far_rows(tiles, row_tiles, col_tiles, by_col):
    row, col = tiles[0, 0, 0:1, :], tiles[0, 0, 1:2, :]
    key = col * row_tiles + row if by_col else row * col_tiles + col
    count = row_tiles * col_tiles
    place = lax.broadcasted_iota(jnp.int32, (count, key.shape[1]), 0)
    near = jnp.max(jnp.where(place == key, 1.0, 0.0), axis=1, keepdims=True)
    return jnp.broadcast_to(FAR * (1.0 - near), (count, TILE))


def halves(x):
    high = x.astype(jnp.bfloat16)
    return high, (x - high.astype(jnp.float32)).astype(jnp.bfloat16)


def pieces(x):
    first = x.astype(jnp.bfloat16).astype(jnp.float32)
    second = (x - first).astype(jnp.bfloat16).astype(jnp.float32)
    return first, second, x - first - second


def describe(ref, lanes, x, y, support):
    square = (EDGE / support) ** 2
    lines = pieces(-2.0 * square * x) + pieces(-2.0 * square * y) + pieces(square * (x * x + y * y))
    for k, line in enumerate(lines):
        ref[k:k + 1, lanes] = line
    ref[12:13, lanes] = x
    ref[13:14, lanes] = y


def flipped_side(sides):
    x, y = sides[12:13], sides[13:14]
    one = jnp.ones_like(x)
    return jnp.concatenate([x, x, x, y, y, y, one, one, one, sides[6:9], jnp.zeros((4, x.shape[1]), jnp.float32)], axis=0)


def cycle_kernel(g, vals_h, points0_h, points1_h, points2_h, tiles_a0_h, tiles_e1_h, tiles_a1_h, factor_h,
                 fine_o, mid_o, coarse_o, norm_o,
                 tiles_a0, tiles_e1, tiles_a1, factor, points2,
                 v2, p0g, p1g, pcg, maskg, emask, tmask, masks_s, emask_s, tmask_s, fac, facg, gtg,
                 gall, gstrip, gpl, gmid, gmid2, gcoarse, gfine, gplane, gmids, gcs, fbuf, side_a, side_e, side_t, side_o, side_m,
                 a0, e1own, e1t, e2t, a1t, other_s, other_r, resg, part_buf, rsin, square_g, mida, csend, crecv, cg, wcat, zcat,
                 l_s, a_m, p0_m, p1_m, pc_m, v_m, em_m, tm_m, f_m, g_m, ot_m, re_m, rs_m, sq_m, mz_m, ma_m, cr_m, ca_m):
    nr, nc, R0, R1, R2 = g["nr"], g["nc"], g["R0"], g["R1"], g["R2"]
    D = nr * nc
    T0, T1 = R0 // TILE, R1 // TILE
    C0, C1 = R0 * nr // nc, R1 * nr // nc
    B0, B1 = C0 // TILE, C1 // TILE
    S0 = R0 // nc
    I0 = S0 // TILE
    Q1 = C1 // nr
    N1, N2 = nr * R1, g["N2"]
    CR = N2 // D
    NT1 = nr * T1
    NT2 = N2 // TILE
    f32, bf16 = jnp.float32, jnp.bfloat16
    r = lax.axis_index("row")
    c = lax.axis_index("col")
    d = r * nc + c
    y, k_core = r // 2, lax.rem(r, 2)
    z, h = c // 2, lax.rem(c, 2)
    mate = r + 1 - 2 * k_core
    yp = lax.rem(r + 2, nr)
    diag = lax.rem(mate + 2, nr)
    xp = c + 1 - 2 * h
    own_b = 2 * r + h

    def rc(src, dst, ssem, rsem, rr, cc):
        return pltpu.make_async_remote_copy(src_ref=src, dst_ref=dst, send_sem=ssem, recv_sem=rsem,
                                            device_id=(rr, cc), device_id_type=MESH)

    def each(lo, hi, f):
        def body(k, carry):
            f(k)
            return carry
        lax.fori_loop(lo, hi, body, 0)

    barrier = pltpu.get_barrier_semaphore()

    def greet(k):
        q = lax.rem(c + k, nc)
        for j in range(nr):
            pl.semaphore_signal(barrier, inc=1, device_id=(lax.rem(r + j, nr), q), device_id_type=MESH)

    each(1, nc, greet)
    for j in range(1, nr):
        pl.semaphore_signal(barrier, inc=1, device_id=(lax.rem(r + j, nr), c), device_id_type=MESH)
    loads = [pltpu.make_async_copy(s, t, l_s.at[k]) for k, (s, t) in enumerate((
        (points0_h, p0g.at[r]), (points1_h, p1g.at[r]), (points2_h, points2), (tiles_a0_h, tiles_a0),
        (tiles_e1_h, tiles_e1), (tiles_a1_h, tiles_a1), (factor_h, factor), (vals_h, v2.at[k_core])))]
    for load in loads:
        load.start()

    def one_hot(ref, rows, columns):
        ref[16:16 + rows] = jnp.where(lax.broadcasted_iota(jnp.int32, (rows, columns), 1) // TILE
                                      == lax.broadcasted_iota(jnp.int32, (rows, columns), 0), 1.0, 0.0).astype(bf16)

    one_hot(gfine, 2 * T0, 2 * R0)
    one_hot(gplane, T0, R0)
    one_hot(gmids, NT1, N1)
    fbuf[...] = jnp.zeros_like(fbuf)
    emask_s[...] = jnp.zeros_like(emask_s)
    tmask_s[...] = jnp.zeros_like(tmask_s)
    for ref in (gall, gstrip, gpl, gmid, gmid2, gcoarse):
        ref[...] = jnp.ones_like(ref)
    for load in loads[:-1]:
        load.wait()
    far_a0 = far_rows(tiles_a0, T0, B0, False)
    far_e1 = far_rows(tiles_e1, T0, B1, False)
    for q in range(nc):
        masks_s[q] = far_a0[q * I0 * B0:(q + 1) * I0 * B0].astype(bf16)
        emask_s[q, :I0 * B1] = far_e1[q * I0 * B1:(q + 1) * I0 * B1]
    far_e1 = far_rows(tiles_e1, T0, B1, True)
    far_a1 = far_rows(tiles_a1, T1, B1, True)
    planes = nc // 2
    PT = T0 // planes
    for q in range(planes):
        for j in range(B1):
            tmask_s[q, j * PT:(j + 1) * PT] = far_e1[j * T0 + q * PT:j * T0 + (q + 1) * PT]
        tmask_s[q, B1 * PT:B1 * PT + B1 * T1] = far_a1
    half_of = lax.rem(r, TILE // R2)
    raw = factor[...].astype(f32)
    fac[...] = jnp.concatenate([jnp.where(half_of == k, raw, 0.0) for k in range(TILE // R2)], axis=1).astype(bf16)
    line = points2[...].astype(f32)
    pcg[r] = jnp.zeros((8, TILE), f32)
    pcg[r, 0:2] = jnp.concatenate([jnp.where(half_of == k, line, 0.0) for k in range(TILE // R2)], axis=1)
    loads[-1].wait()
    pl.semaphore_wait(barrier, D - 1)

    def row_send(src, dst, m):
        for k in range(1, nr):
            rc(src, dst, m.at[0], m.at[1], lax.rem(r + k, nr), c).start()

    def row_wait(ref, m):
        slots = ref.at[pl.ds(0, nr - 1)]
        rc(slots, slots, m.at[0], m.at[1], mate, c).wait()

    def col_send(src_of, dst, m):
        def go(k):
            q = lax.rem(c + k, nc)
            rc(src_of(q), dst, m.at[0], m.at[1], r, q).start()
        each(1, nc, go)

    y_of = c // planes
    mask_row = 2 * y_of + k_core
    mask_slot = jnp.where(y_of == y, 0, 1) * planes + lax.rem(c, planes)
    mask_self = y_of == y

    def mask_go(k):
        q = lax.rem(c + k, nc)
        rc(masks_s.at[q], maskg.at[mask_slot], a_m.at[0], a_m.at[1], mask_row, q).start()

    each(1, nc, mask_go)

    @pl.when(jnp.logical_not(mask_self))
    def _():
        mask_go(0)

    @pl.when(mask_self)
    def _():
        maskg[mask_slot] = masks_s[c]

    row_send(p0g.at[r], p0g.at[r], p0_m)
    rc(v2.at[k_core], v2.at[k_core], v_m.at[0], v_m.at[1], mate, c).start()
    row_send(p1g.at[r], p1g.at[r], p1_m)
    row_send(pcg.at[r], pcg.at[r], pc_m)
    tmask_self = c // 2 == r

    def tmask_go(q):
        rc(tmask_s.at[q], tmask.at[r], tm_m.at[0], tm_m.at[1], c // 2, 2 * q + h).start()

    for k in range(1, planes):
        tmask_go(lax.rem(z + k, planes))

    @pl.when(jnp.logical_not(tmask_self))
    def _():
        tmask_go(z)

    @pl.when(tmask_self)
    def _():
        tmask[r] = tmask_s[z]

    col_send(lambda q: emask_s.at[q], emask.at[c], em_m)
    row_send(fac, facg.at[r], f_m)
    emask[c] = emask_s[c]
    facg[r] = fac[...]

    def line_of(ref, q, way, lanes=slice(None)):
        return ref[q, way:way + 1, lanes].astype(f32)

    def describe_own(rb, slot):
        describe(gall.at[slot], slice(None), line_of(p0g, rb, 0), line_of(p0g, rb, 1), support_fine)
        gfine[:16, pl.ds(pl.multiple_of(slot * R0, R0), R0)] = gall[slot].astype(bf16)

    strip = pl.ds(pl.multiple_of(c * S0, S0), S0)
    describe_own(r, k_core)
    row_wait(p0g, p0_m)
    describe_own(mate, 1 - k_core)
    describe(gstrip, slice(None), line_of(p0g, yp, 0, strip), line_of(p0g, yp, 1, strip), support_fine)
    fbuf[0:16, :S0] = flipped_side(gall[k_core, :, strip])
    fbuf[0:16, S0:] = flipped_side(gstrip[...])

    def wait_slots(ref, n, m):
        slots = ref.at[pl.ds(0, n)]
        rc(slots, slots, m.at[0], m.at[1], mate, c).wait()

    @pl.when(mask_self)
    def _():
        wait_slots(maskg, nc - 1, a_m)

    @pl.when(jnp.logical_not(mask_self))
    def _():
        wait_slots(maskg, nc, a_m)

    for s in range(2):
        for q in range(planes):
            rows = maskg[s * planes + q].astype(f32)
            for i in range(I0):
                fbuf[16 + q * B0:16 + (q + 1) * B0, (s * I0 + i) * TILE:(s * I0 + i + 1) * TILE] = rows[i * B0:(i + 1) * B0]
    side_a[...] = fbuf[...].T.astype(bf16)

    def build(put, side, sides, depth, columns, step):
        def go(k):
            lanes = pl.ds(pl.multiple_of(k * step, step), step)
            put(lanes, phi_of(dot(side[:, :depth], sides[:depth, lanes])))
        each(0, columns // step, go)

    def put_a0(s):
        def put(lanes, value):
            a0[s, :, lanes] = value
        return put

    KA = 16 + 2 * T0
    def product(s, lo, hi):
        total = None
        for k in range(2):
            lanes = slice(k * R0, (k + 1) * R0)
            a0[s, lo:hi, lanes] = phi_of(dot(side_a[s * S0 + lo:s * S0 + hi, :KA], gfine[:KA, lanes]))
            if s == 1 and lo == 0 and k == 0:
                rc(v2.at[1 - k_core], v2.at[1 - k_core], v_m.at[0], v_m.at[1], mate, c).wait()
            term = dot(a0[s, lo:hi, lanes], v2[k])
            total = term if total is None else total + term
        return total

    def other_copy(i):
        rows = pl.ds(i * TILE, TILE)
        return rc(other_s.at[rows], other_r.at[rows], ot_m.at[0], ot_m.at[1 + i], yp, c)

    for i in range(I0):
        other_s[i * TILE:(i + 1) * TILE] = product(1, i * TILE, (i + 1) * TILE).astype(bf16)
        other_copy(i).start()
    acc = product(0, 0, S0)
    own_vals = v2[k_core, strip, :].astype(f32)
    x_slot, y_slot, d_slot = 2 * r + 1 - h, 2 * yp + h, 2 * diag + 1 - h

    def plane_gather(at, m, base, mate_sem):
        def send(slot, sem, rr, cc):
            rc(at(slot), at(slot), m.at[0], m.at[sem], rr, cc).start()

        def start():
            send(own_b, base + 2, diag, xp)
            send(own_b, base + 1, yp, c)
            send(own_b, base, r, xp)
            send(own_b, mate_sem, mate, c)

        def relay(slot, sem):
            rc(at(slot), at(slot), m.at[0], m.at[sem], mate, c).wait_recv()
            send(slot, mate_sem, mate, c)

        return (start, functools.partial(relay, x_slot, base), functools.partial(relay, y_slot, base + 1),
                functools.partial(relay, d_slot, base + 2))

    def plane_end(ref, m, mate_sem):
        part = ref.at[pl.ds(0, 4)]
        rc(part, part, m.at[0], m.at[mate_sem], mate, c).wait_recv()

    def plane_drain(ref, m, mate_sem):
        part = ref.at[pl.ds(0, 7)]
        rc(part, part, m.at[0], m.at[mate_sem], mate, c).wait_send()

    def all_send(src_of, dst, m):
        def go(k):
            q = lax.rem(c + k, nc)
            for j in range(nr):
                p = lax.rem(r + j, nr)
                rc(src_of(p * nc + q), dst, m.at[0], m.at[1], p, q).start()
        each(1, nc, go)
        for j in range(1, nr):
            p = lax.rem(r + j, nr)
            rc(src_of(p * nc + c), dst, m.at[0], m.at[1], p, c).start()

    def res_part(i):
        return plane_gather(lambda slot: resg.at[slot, pl.ds(i * TILE, TILE)], re_m, 1 + 3 * i, 7)

    res_parts = [res_part(i) for i in range(I0)]
    for i in range(I0):
        other_copy(i).wait_recv()
        rows = slice(i * TILE, (i + 1) * TILE)
        resg[own_b, rows] = (own_vals[rows] - (0.5 * g["scale_a0"]) * (acc[rows] + other_r[rows].astype(f32))).astype(bf16)
        res_parts[i][0]()
    PL = PT * TILE
    plane_lanes = pl.ds(pl.multiple_of(z * PL, PL), PL)
    row_wait(p1g, p1_m)
    for q in range(nr):
        describe(gpl, slice(q * PL, (q + 1) * PL), line_of(p0g, q, 0, plane_lanes), line_of(p0g, q, 1, plane_lanes), support_mid)
        lanes = slice(q * R1, (q + 1) * R1)
        describe(gmid, lanes, line_of(p1g, q, 0), line_of(p1g, q, 1), support_mid)
    gplane[:16] = gpl[...].astype(bf16)
    gmids[:16] = gmid[...].astype(bf16)

    @pl.when(tmask_self)
    def _():
        wait_slots(tmask, nr - 1, tm_m)

    @pl.when(jnp.logical_not(tmask_self))
    def _():
        wait_slots(tmask, nr, tm_m)

    block = pl.ds(pl.multiple_of(own_b * C1, C1), C1)
    fbuf[0:16, :C1] = flipped_side(gmid[:, block])
    fbuf[0:16, C1:] = fbuf[0:16, :C1]
    for q in range(nr):
        for j in range(B1):
            fbuf[16 + q * PT:16 + (q + 1) * PT, j * TILE:(j + 1) * TILE] = tmask[q, j * PT:(j + 1) * PT, :]
            at = B1 * PT + j * T1
            fbuf[16 + q * T1:16 + (q + 1) * T1, C1 + j * TILE:C1 + (j + 1) * TILE] = tmask[q, at:at + T1, :]
    side_t[...] = fbuf[...].T.astype(bf16)

    def put_e1t(lanes, value):
        e1t[:, lanes] = value

    build(put_e1t, side_t.at[pl.ds(0, C1)], gplane, 16 + T0, R0, 2048)
    row_wait(pcg, pc_m)
    row_wait(facg, f_m)
    def put_a1t(lanes, value):
        a1t[:, lanes] = value

    build(put_a1t, side_t.at[pl.ds(C1, C1)], gmids, 16 + NT1, N1, 1024)
    for k in range(1, 4):
        res_parts[0][k]()
    strips = []
    per = TILE // R2
    for lane in range(NT2):
        total = facg[lane * per].astype(f32)
        for k in range(1, per):
            total = total + facg[lane * per + k].astype(f32)
        strips.append(total)
    gtg[c] = jnp.concatenate(strips, axis=1).astype(bf16)
    col_send(lambda q: gtg.at[c], gtg.at[c], g_m)
    for t in range(NT2):
        line = pcg[per * t] + pcg[per * t + 1]
        describe(gcoarse, slice(t * TILE, (t + 1) * TILE), line[0:1], line[1:2], support_coarse)
    gcs[...] = gcoarse[...].astype(bf16)
    for q in range(nr):
        describe(gmid2, slice(q * R1, (q + 1) * R1), line_of(p1g, q, 0), line_of(p1g, q, 1), support_coarse)
    wide = fbuf.shape[1]
    for q in range(N1 // wide):
        fbuf[0:16] = flipped_side(gmid2[:, q * wide:(q + 1) * wide])
        side_m[...] = fbuf[...].T.astype(bf16)
        e2t[q * wide:(q + 1) * wide] = phi_of(dot(side_m[:, :16], gcs[...]))
    for k in range(1, 4):
        res_parts[1][k]()
    restricted = jnp.zeros((C1, resg.shape[-1]), f32)
    square = jnp.zeros((16, resg.shape[-1]), f32)

    def restrict(slot):
        strip_data = resg[slot]
        held = strip_data.astype(f32)
        return (dot(e1t[:, pl.ds(pl.multiple_of(slot * S0, S0), S0)], strip_data),
                jnp.sum((held * held).reshape(S0 // 16, 16, -1), axis=0))

    for slot in (own_b, x_slot, y_slot, d_slot):
        term = restrict(slot)
        restricted, square = restricted + term[0], square + term[1]
    plane_end(resg, re_m, 7)
    for slot in (2 * mate + h, 2 * mate + 1 - h, 2 * diag + h, 2 * yp + 1 - h):
        term = restrict(slot)
        restricted, square = restricted + term[0], square + term[1]
    restricted = g["scale_e1"] * restricted
    for q in range(planes):
        part_buf[q] = restricted[q * Q1:(q + 1) * Q1].astype(bf16)

    near_z = z + 1 - 2 * lax.rem(z, 2)
    far_first = (jnp.where(z < 2, 3, 0), jnp.where(z < 2, 2, 1), near_z)

    def z_send(src_of, dst, m):
        for q in far_first:
            rc(src_of(q), dst, m.at[0], m.at[1], r, 2 * q + h).start()

    z_send(lambda q: part_buf.at[q], rsin.at[z], rs_m)
    rsin[z] = part_buf[z]
    square_g[z] = square.astype(bf16)
    turned_w = g["scale_e2"] * (e2t[block, :].astype(f32) - (0.5 * g["scale_a1"]) * dot(a1t[...], e2t[...]))
    w_high, w_low = halves(turned_w.T)
    for k, w in enumerate((w_high, w_low, w_high)):
        wcat[:, k * C1:(k + 1) * C1] = w

    part_high, part_low = halves(restricted)
    part = dot(wcat[...], jnp.concatenate([part_high, part_high, part_low], axis=0))
    csend[...] = part.reshape(D, CR, -1).astype(bf16)
    all_send(lambda q: csend.at[q], crecv.at[d], cr_m)
    crecv[d] = csend[d]
    wait_slots(emask, nc - 1, em_m)
    describe(gstrip, slice(None), line_of(p0g, r, 0, strip), line_of(p0g, r, 1, strip), support_mid)
    fbuf[0:16, :S0] = flipped_side(gstrip[...])
    for q in range(nc):
        for i in range(I0):
            fbuf[16 + q * B1:16 + (q + 1) * B1, i * TILE:(i + 1) * TILE] = emask[q, i * B1:(i + 1) * B1, :]
    side_e[...] = fbuf[:, :S0].T.astype(bf16)

    def put_e1own(lanes, value):
        e1own[:, lanes] = value

    build(put_e1own, side_e, gmids, 16 + NT1, N1, 2048)
    fine_gain = g["scale_e1"]
    wait_slots(rsin, planes - 1, rs_m)
    total = rsin[0].astype(f32)
    for q in range(1, planes):
        total = total + rsin[q].astype(f32)
    q_high = total.astype(bf16)
    mida[own_b, z] = q_high
    own_q = mida.at[own_b, z]
    rank = jnp.where((z == 0) | (z == planes - 1), 3, 2)
    for q, sem in ((far_first[0], rank), (far_first[1], rank), (near_z, 1)):
        rc(own_q, own_q, mz_m.at[0], mz_m.at[sem], r, 2 * q + h).start()
    order = (z,) + far_first[::-1]

    def batch(k):
        return plane_gather(lambda slot: mida.at[slot, order[k]], ma_m, 1 + 3 * k, 13)

    batches = [batch(k) for k in range(planes)]
    batches[0][0]()
    z_send(lambda q: square_g.at[z], square_g.at[z], sq_m)
    wait_slots(gtg, nc - 1, g_m)
    gt = gtg[...].reshape(N2, N2)
    gg_high, gg_low = halves(dot(gt.astype(f32).T.astype(bf16), gt))
    zcat[S0 + C1:, :N2] = gg_high
    zcat[S0 + C1:, N2:] = gg_low
    h_high, h_low = halves((fine_gain * g["scale_e2"]) * dot(e1own[...], e2t[...]))
    steps = (dot(h_high, gg_high) + dot(h_low, gg_high) + dot(h_high, gg_low),)
    rows_c = e2t[pl.ds(pl.multiple_of(c * C1, C1), C1), :]
    steps += (g["scale_e2"] * (dot(rows_c, gg_high) + dot(rows_c, gg_low)),)
    for k, step in enumerate(steps):
        high, low = halves(step)
        zcat[k * C1:(k + 1) * C1, :N2] = high
        zcat[k * C1:(k + 1) * C1, N2:] = low

    def z_take(k):
        piece = mida.at[own_b, order[k]]
        rc(piece, piece, mz_m.at[0], mz_m.at[k], mate, c).wait_recv()
        batches[k][0]()

    wait_slots(crecv, D - 1, cr_m)
    cg[d] = jnp.sum(crecv[...].astype(f32), axis=0).astype(bf16)
    all_send(lambda q: cg.at[d], cg.at[d], ca_m)
    for k in range(1, 4):
        batches[0][k]()
    z_take(1)
    z_take(2)
    z_take(3)
    wait_slots(square_g, planes - 1, sq_m)
    norm_o[...] = jnp.broadcast_to(jnp.sum(square_g[...].astype(f32), keepdims=True).reshape(1, 1) * g["norm_scale"], norm_o.shape)
    for b in batches[1:]:
        for k in range(1, 4):
            b[k]()
    wait_slots(cg, D - 1, ca_m)
    cd = cg[...].astype(f32).reshape(N2, -1).astype(bf16)
    both = jnp.concatenate([cd, cd], axis=0)
    coarse_o[...] = dot(zcat[pl.ds(pl.multiple_of(S0 + C1 + r * R2, R2), R2), :], both)
    step = dot(zcat[:S0 + C1, :], both)
    def prolong(slot):
        return dot(e1own[:, pl.ds(pl.multiple_of(slot * C1, C1), C1)], mida[slot].reshape(C1, -1))

    base = prolong(own_b) + prolong(x_slot) + prolong(y_slot) + prolong(d_slot)
    plane_end(mida, ma_m, 13)
    for slot in (2 * mate + h, 2 * mate + 1 - h, 2 * diag + h, 2 * yp + 1 - h):
        base = base + prolong(slot)
    mid_o[...] = 0.5 * mida[c].astype(f32).reshape(C1, -1) + step[S0:]
    fine_o[...] = 0.5 * own_vals + (0.5 * fine_gain) * base + step[:S0]
    rc(other_s, other_r, ot_m.at[0], ot_m.at[1], yp, c).wait_send()
    plane_drain(resg, re_m, 7)
    plane_drain(mida, ma_m, 13)
    held_z = mida.at[own_b, pl.ds(0, planes - 1)]
    rc(held_z, held_z, mz_m.at[0], mz_m.at[1], mate, c).wait_send()


def finish_kernel(fine, mid, coarse, norm, fine_o, mid_o, coarse_o, norm_o):
    fine_o[...] = fine[...]
    mid_o[...] = mid[...]
    coarse_o[...] = coarse[...]
    norm_o[...] = norm[0:1, 0:1]


def fits(nr, nc, R0, R1, R2):
    if nr != 4 or nc != 8:
        return False
    if R0 != R1 * nr or R0 != 2 * nc * TILE or 2 * R2 != TILE:
        return False
    return True


def fused(values, points0, points1, points2, tiles_a0, tiles_e1, tiles_a1, factor):
    nr, nc = lax.axis_size("row"), lax.axis_size("col")
    R0, R1, R2 = points0.shape[1], points1.shape[1], points2.shape[1]
    F = values.shape[-1]
    if not fits(nr, nc, R0, R1, R2) or F != TILE:
        return per_device(values, points0, points1, points2, tiles_a0, tiles_e1, tiles_a1, factor)
    D, N2 = nr * nc, nr * R2
    T0, T1 = R0 // TILE, R1 // TILE
    B0, B1 = R0 * nr // nc // TILE, R1 * nr // nc // TILE
    S0 = R0 // nc
    I0 = S0 // TILE
    C1, CR, Q1 = B1 * TILE, N2 // D, R1 * nr // nc // nr
    g = dict(nr=nr, nc=nc, R0=R0, R1=R1, R2=R2, N2=N2,
             scale_a0=(R0 / (nc * tiles_a0.shape[-1] * TILE * TILE)) ** 0.5,
             scale_e1=(R0 / (nc * tiles_e1.shape[-1] * TILE * TILE)) ** 0.5,
             scale_a1=(R1 / (nc * tiles_a1.shape[-1] * TILE * TILE)) ** 0.5,
             scale_e2=(1.0 / (R1 * nr)) ** 0.5,
             norm_scale=1.0 / (R0 * nr * F))
    f32, bf16, i32 = jnp.float32, jnp.bfloat16, jnp.int32
    V = pltpu.VMEM
    dma = pltpu.SemaphoreType.DMA
    wide = N2 // nc
    N1 = nr * R1
    planes = nc // 2
    scratch = [
        V(tiles_a0.shape, i32), V(tiles_e1.shape, i32), V(tiles_a1.shape, i32), V((wide, R2), bf16), V(points2.shape, bf16),
        V((2, R0, F), bf16), V((nr,) + points0.shape, bf16), V((nr,) + points1.shape, bf16), V((nr, 8, TILE), f32),
        V((nc, I0 * B0, TILE), bf16), V((nc, 8, TILE), f32), V((nr, 16, TILE), f32),
        V((nc, I0 * B0, TILE), bf16), V((nc, 8, TILE), f32), V((planes, 16, TILE), f32),
        V((wide, TILE), bf16), V((nr, wide, TILE), bf16), V((nc, wide, N2), bf16),
        V((2, 16, R0), f32), V((16, S0), f32), V((16, R0), f32), V((16, N1), f32), V((16, N1), f32), V((16, N2), f32),
        V((16 + 2 * T0, 2 * R0), bf16), V((16 + T0, R0), bf16), V((16 + nr * T1, N1), bf16), V((16, N2), bf16),
        V((TILE, 2 * S0), f32), V((2 * S0, TILE), bf16), V((S0, TILE), bf16), V((2 * S0, TILE), bf16),
        V((8, TILE), bf16), V((2 * S0, TILE), bf16),
        V((2, S0, 2 * R0), bf16), V((S0, N1), bf16), V((C1, R0), bf16), V((N1, N2), bf16), V((C1, N1), bf16),
        V((S0, F), bf16), V((S0, F), bf16), V((nc, S0, F), bf16),
        V((planes, Q1, F), bf16), V((planes, Q1, F), bf16), V((planes, 16, F), bf16), V((nc, planes, Q1, F), bf16),
        V((D, CR, F), bf16), V((D, CR, F), bf16), V((D, CR, F), bf16), V((N2, 3 * C1), bf16),
        V((S0 + C1 + N2, 2 * N2), bf16),
    ]
    for n in (8, 2, 2, 2, 2, 2, 2, 2, 2, 2, 1 + I0, 2 + 3 * I0, 2, 2, 4, 14, 2, 2):
        scratch += [dma((n,))]
    vm = pl.BlockSpec(memory_space=pltpu.VMEM)
    shapes = ((S0, F), (C1, F), (R2, F))
    parts = pl.pallas_call(
        functools.partial(cycle_kernel, g),
        out_shape=tuple(jax.ShapeDtypeStruct(s, f32) for s in shapes + ((8, TILE),)),
        in_specs=[pl.BlockSpec(memory_space=pltpu.HBM)] * 8,
        out_specs=[vm] * 4,
        scratch_shapes=scratch,
        compiler_params=pltpu.CompilerParams(collective_id=0, has_side_effects=True, vmem_limit_bytes=48 << 20),
    )(*[pltpu.with_memory_space_constraint(x, pltpu.HBM) for x in (
        values, points0, points1, points2, tiles_a0, tiles_e1, tiles_a1, factor.T)])
    fine, mid, coarse, norm = pl.pallas_call(
        finish_kernel,
        grid=(1,),
        out_shape=tuple(jax.ShapeDtypeStruct(s, f32) for s in shapes + ((1, 1),)),
        in_specs=[vm] * 4,
        out_specs=[pl.BlockSpec(s, lambda i: (0, 0)) for s in shapes + ((1, 1),)],
        compiler_params=pltpu.CompilerParams(vmem_limit_bytes=4 << 20),
    )(*parts)
    return (fine, mid, coarse, norm.reshape(1))


def solution(mesh):
    return jax.shard_map(
        fused,
        mesh=mesh,
        in_specs=(
            P("row", None),
            P(None, "row"),
            P(None, "row"),
            P(None, "row"),
            P("row", "col", None, None),
            P("row", "col", None, None),
            P("row", "col", None, None),
            P("row", "col"),
        ),
        out_specs=(P(("row", "col"), None), P("col", None), P("row", None), P()),
        check_vma=False,
    )
```

```python
import functools
import math

import jax
import jax.numpy as jnp
from jax import lax
from jax.experimental import pallas as pl
from jax.experimental.pallas import tpu as pltpu
from jax.sharding import PartitionSpec as P

TILE = 128


support_fine = 0.35
support_mid = 0.55
support_coarse = 0.8


def spread(x, axis, root):
    mine = lax.axis_index(axis) == root
    return lax.psum(jnp.where(mine, x, jnp.zeros_like(x)), axis)


def wendland(left_pts, right_pts, support):
    left = left_pts.astype(jnp.float32)
    right = right_pts.astype(jnp.float32)
    across = left[0][..., :, None] - right[0][..., None, :]
    upward = left[1][..., :, None] - right[1][..., None, :]
    ratio_t = jnp.sqrt(across * across + upward * upward) / support
    margin = jnp.maximum(1.0 - ratio_t, 0.0)
    squared = margin * margin
    return (squared * squared * (4.0 * ratio_t + 1.0)).astype(jnp.bfloat16)


def listed_terms(row_pts, col_pts, listing, vector, support, flipped):
    row_tiles = row_pts.reshape(2, -1, TILE)
    col_tiles = col_pts.reshape(2, -1, TILE)
    listed = listing.shape[-1]
    group = math.gcd(listed, 32)
    order = listing.reshape(2, listed // group, group)
    fields = vector.shape[-1]
    inputs = vector.reshape(-1, TILE, fields)
    target = col_tiles.shape[1] if flipped else row_tiles.shape[1]
    total = jnp.zeros((target, TILE, fields), jnp.float32)

    def add_group(total, pair):
        tile_rows, tile_cols = pair
        kernel = wendland(row_tiles[:, tile_rows], col_tiles[:, tile_cols], support)
        if flipped:
            contrib = jnp.einsum(
                "gij,gir->gjr", kernel, inputs[tile_rows], preferred_element_type=jnp.float32
            )
            return (total.at[tile_cols].add(contrib), None)
        contrib = jnp.einsum(
            "gij,gjr->gir", kernel, inputs[tile_cols], preferred_element_type=jnp.float32
        )
        return (total.at[tile_rows].add(contrib), None)

    total, unused = lax.scan(add_group, total, (order[0], order[1]))
    return total.reshape(-1, fields)


def per_device(values, points0, points1, points2, tiles_a0, tiles_e1, tiles_a1, factor):
    row_count = lax.axis_size("row")
    col_count = lax.axis_size("col")
    col_id = lax.axis_index("col")
    col_per_row = col_count // row_count
    rows_fine, fields = values.shape
    rows_mid = points1.shape[1]
    share = rows_fine // col_count
    cols_fine = rows_fine // col_per_row
    cols_mid = rows_mid // col_per_row
    source = col_id // col_per_row
    part_index = col_id % col_per_row
    value_piece = lax.dynamic_slice_in_dim(values, part_index * cols_fine, cols_fine, 0)
    fine_piece = lax.dynamic_slice_in_dim(points0, part_index * cols_fine, cols_fine, 1)
    mid_piece = lax.dynamic_slice_in_dim(points1, part_index * cols_mid, cols_mid, 1)
    value_cols, fine_cols, mid_cols = (
        spread(value_piece, "row", source),
        spread(fine_piece, "row", source),
        spread(mid_piece, "row", source),
    )
    scale_a0 = (rows_fine / (col_count * tiles_a0.shape[-1] * TILE * TILE)) ** 0.5
    scale_e1 = (rows_fine / (col_count * tiles_e1.shape[-1] * TILE * TILE)) ** 0.5
    scale_a1 = (rows_mid / (col_count * tiles_a1.shape[-1] * TILE * TILE)) ** 0.5
    scale_e2 = (1.0 / (rows_mid * row_count)) ** 0.5
    fine_data = values.astype(jnp.float32)
    own_data = lax.dynamic_slice_in_dim(values, col_id * share, share, 0).astype(jnp.float32)
    product_part = listed_terms(points0, fine_cols, tiles_a0[0, 0], value_cols, support_fine, False)
    product_whole = lax.psum(product_part, "col")
    fine_residual = fine_data - 0.5 * (scale_a0 * product_whole)
    fine_square = jnp.sum(fine_residual * fine_residual)
    restrict_part = listed_terms(
        points0, mid_cols, tiles_e1[0, 0], fine_residual.astype(jnp.bfloat16), support_mid, True
    )
    restrict_sum = lax.psum(restrict_part, "row")
    mid_data = scale_e1 * restrict_sum
    mid_part = listed_terms(
        points1, mid_cols, tiles_a1[0, 0], mid_data.astype(jnp.bfloat16), support_mid, False
    )
    mid_whole = (scale_a1 * lax.psum(mid_part, "col")).astype(jnp.bfloat16)
    mid_slice = lax.dynamic_slice_in_dim(mid_whole, part_index * cols_mid, cols_mid, 0)
    mid_turned = spread(mid_slice, "row", source)
    mid_residual = mid_data - 0.5 * mid_turned.astype(jnp.float32)
    coarse_kernel = wendland(points2, mid_cols, support_coarse)
    coarse_part = jnp.dot(
        coarse_kernel, mid_residual.astype(jnp.bfloat16), preferred_element_type=jnp.float32
    )
    coarse_sum = lax.psum(coarse_part, "col")
    coarse_data = (scale_e2 * coarse_sum).astype(jnp.bfloat16)
    halfway_part = lax.dot_general(
        factor, coarse_data, (((0,), (0,)), ((), ())), preferred_element_type=jnp.float32
    )
    halfway = lax.psum(halfway_part, "row").astype(jnp.bfloat16)
    coarse_part_two = jnp.dot(factor, halfway, preferred_element_type=jnp.float32)
    coarse_coef = lax.psum(coarse_part_two, "col")
    prolong_part = lax.dot_general(
        coarse_kernel,
        coarse_coef.astype(jnp.bfloat16),
        (((0,), (0,)), ((), ())),
        preferred_element_type=jnp.float32,
    )
    mid_coef = 0.5 * mid_data + scale_e2 * lax.psum(prolong_part, "row")
    fine_part = listed_terms(
        points0, mid_cols, tiles_e1[0, 0], mid_coef.astype(jnp.bfloat16), support_mid, False
    )
    fine_coef = 0.5 * own_data + scale_e1 * lax.psum_scatter(
        fine_part, "col", scatter_dimension=0, tiled=True
    )
    fine_total = lax.psum(fine_square / col_count, ("row", "col"))
    fine_norm = fine_total / (rows_fine * row_count * fields)
    return (fine_coef, mid_coef, coarse_coef, jnp.stack([fine_norm]))


FAR = 64.0
MESH = pl.DeviceIdType.MESH


EDGE = 4.0 ** 0.2


def phi_of(square):
    square = jnp.maximum(square, 1e-20)
    margin = jnp.maximum(EDGE - square * lax.rsqrt(square), 0.0)
    squared = margin * margin
    return (squared * squared * (1.25 * EDGE - margin)).astype(jnp.bfloat16)


def dot(a, b):
    return jnp.dot(a, b, preferred_element_type=jnp.float32)


def far_rows(tiles, row_tiles, col_tiles, by_col):
    row, col = tiles[0, 0, 0:1, :], tiles[0, 0, 1:2, :]
    key = col * row_tiles + row if by_col else row * col_tiles + col
    count = row_tiles * col_tiles
    place = lax.broadcasted_iota(jnp.int32, (count, key.shape[1]), 0)
    near = jnp.max(jnp.where(place == key, 1.0, 0.0), axis=1, keepdims=True)
    return jnp.broadcast_to(FAR * (1.0 - near), (count, TILE))


def halves(x):
    high = x.astype(jnp.bfloat16)
    return high, (x - high.astype(jnp.float32)).astype(jnp.bfloat16)


def pieces(x):
    first = x.astype(jnp.bfloat16).astype(jnp.float32)
    second = (x - first).astype(jnp.bfloat16).astype(jnp.float32)
    return first, second, x - first - second


def describe(ref, lanes, x, y, support):
    square = (EDGE / support) ** 2
    lines = pieces(-2.0 * square * x) + pieces(-2.0 * square * y) + pieces(square * (x * x + y * y))
    for k, line in enumerate(lines):
        ref[k:k + 1, lanes] = line
    ref[12:13, lanes] = x
    ref[13:14, lanes] = y


def flipped_side(sides):
    x, y = sides[12:13], sides[13:14]
    one = jnp.ones_like(x)
    return jnp.concatenate([x, x, x, y, y, y, one, one, one, sides[6:9], jnp.zeros((4, x.shape[1]), jnp.float32)], axis=0)


def cycle_kernel(g, vals_h, points0_h, points1_h, points2_h, tiles_a0_h, tiles_e1_h, tiles_a1_h, factor_h,
                 fine_o, mid_o, coarse_o, norm_o,
                 tiles_a0, tiles_e1, tiles_a1, factor, points2,
                 v2, p0g, p1g, pcg, maskg, emask, tmask, masks_s, emask_s, tmask_s, fac, facg, gtg,
                 gall, gstrip, gpl, gmid, gmid2, gcoarse, gfine, gplane, gmids, gcs, fbuf, side_a, side_e, side_t, side_o, side_m,
                 a0, e1own, e1t, e2t, a1t, other_s, other_r, resg, part_buf, rsin, square_g, mida, csend, crecv, cg, wcat, zcat,
                 l_s, a_m, p0_m, p1_m, pc_m, v_m, em_m, tm_m, f_m, g_m, ot_m, re_m, rs_m, sq_m, mz_m, ma_m, cr_m, ca_m):
    nr, nc, R0, R1, R2 = g["nr"], g["nc"], g["R0"], g["R1"], g["R2"]
    D = nr * nc
    T0, T1 = R0 // TILE, R1 // TILE
    C0, C1 = R0 * nr // nc, R1 * nr // nc
    B0, B1 = C0 // TILE, C1 // TILE
    S0 = R0 // nc
    I0 = S0 // TILE
    Q1 = C1 // nr
    N1, N2 = nr * R1, g["N2"]
    CR = N2 // D
    NT1 = nr * T1
    NT2 = N2 // TILE
    f32, bf16 = jnp.float32, jnp.bfloat16
    r = lax.axis_index("row")
    c = lax.axis_index("col")
    d = r * nc + c
    y, k_core = r // 2, lax.rem(r, 2)
    z, h = c // 2, lax.rem(c, 2)
    mate = r + 1 - 2 * k_core
    yp = lax.rem(r + 2, nr)
    diag = lax.rem(mate + 2, nr)
    xp = c + 1 - 2 * h
    own_b = 2 * r + h

    def rc(src, dst, ssem, rsem, rr, cc):
        return pltpu.make_async_remote_copy(src_ref=src, dst_ref=dst, send_sem=ssem, recv_sem=rsem,
                                            device_id=(rr, cc), device_id_type=MESH)

    def each(lo, hi, f):
        def body(k, carry):
            f(k)
            return carry
        lax.fori_loop(lo, hi, body, 0)

    barrier = pltpu.get_barrier_semaphore()

    def greet(k):
        q = lax.rem(c + k, nc)
        for j in range(nr):
            pl.semaphore_signal(barrier, inc=1, device_id=(lax.rem(r + j, nr), q), device_id_type=MESH)

    each(1, nc, greet)
    for j in range(1, nr):
        pl.semaphore_signal(barrier, inc=1, device_id=(lax.rem(r + j, nr), c), device_id_type=MESH)
    loads = [pltpu.make_async_copy(s, t, l_s.at[k]) for k, (s, t) in enumerate((
        (points0_h, p0g.at[r]), (points1_h, p1g.at[r]), (points2_h, points2), (tiles_a0_h, tiles_a0),
        (tiles_e1_h, tiles_e1), (tiles_a1_h, tiles_a1), (factor_h, factor), (vals_h, v2.at[k_core])))]
    for load in loads:
        load.start()

    def one_hot(ref, rows, columns):
        ref[16:16 + rows] = jnp.where(lax.broadcasted_iota(jnp.int32, (rows, columns), 1) // TILE
                                      == lax.broadcasted_iota(jnp.int32, (rows, columns), 0), 1.0, 0.0).astype(bf16)

    one_hot(gfine, 2 * T0, 2 * R0)
    one_hot(gplane, T0, R0)
    one_hot(gmids, NT1, N1)
    fbuf[...] = jnp.zeros_like(fbuf)
    emask_s[...] = jnp.zeros_like(emask_s)
    tmask_s[...] = jnp.zeros_like(tmask_s)
    for ref in (gall, gstrip, gpl, gmid, gmid2, gcoarse):
        ref[...] = jnp.ones_like(ref)
    for load in loads[:-1]:
        load.wait()
    far_a0 = far_rows(tiles_a0, T0, B0, False)
    far_e1 = far_rows(tiles_e1, T0, B1, False)
    for q in range(nc):
        masks_s[q] = far_a0[q * I0 * B0:(q + 1) * I0 * B0].astype(bf16)
        emask_s[q, :I0 * B1] = far_e1[q * I0 * B1:(q + 1) * I0 * B1]
    far_e1 = far_rows(tiles_e1, T0, B1, True)
    far_a1 = far_rows(tiles_a1, T1, B1, True)
    planes = nc // 2
    PT = T0 // planes
    for q in range(planes):
        for j in range(B1):
            tmask_s[q, j * PT:(j + 1) * PT] = far_e1[j * T0 + q * PT:j * T0 + (q + 1) * PT]
        tmask_s[q, B1 * PT:B1 * PT + B1 * T1] = far_a1
    half_of = lax.rem(r, TILE // R2)
    raw = factor[...].astype(f32)
    fac[...] = jnp.concatenate([jnp.where(half_of == k, raw, 0.0) for k in range(TILE // R2)], axis=1).astype(bf16)
    line = points2[...].astype(f32)
    pcg[r] = jnp.zeros((8, TILE), f32)
    pcg[r, 0:2] = jnp.concatenate([jnp.where(half_of == k, line, 0.0) for k in range(TILE // R2)], axis=1)
    loads[-1].wait()
    pl.semaphore_wait(barrier, D - 1)

    def row_send(src, dst, m):
        for k in range(1, nr):
            rc(src, dst, m.at[0], m.at[1], lax.rem(r + k, nr), c).start()

    def row_wait(ref, m):
        slots = ref.at[pl.ds(0, nr - 1)]
        rc(slots, slots, m.at[0], m.at[1], mate, c).wait()

    def col_send(src_of, dst, m):
        def go(k):
            q = lax.rem(c + k, nc)
            rc(src_of(q), dst, m.at[0], m.at[1], r, q).start()
        each(1, nc, go)

    y_of = c // planes
    mask_row = 2 * y_of + k_core
    mask_slot = jnp.where(y_of == y, 0, 1) * planes + lax.rem(c, planes)
    mask_self = y_of == y

    def mask_go_to(q):
        rc(masks_s.at[q], maskg.at[mask_slot], a_m.at[0], a_m.at[1], mask_row, q).start()

    near_z = z + 1 - 2 * lax.rem(z, 2)
    far_first = (jnp.where(z < 2, 3, 0), jnp.where(z < 2, 2, 1), near_z)
    row_send(p0g.at[r], p0g.at[r], p0_m)
    for q in far_first:
        for j in range(2):
            mask_go_to(2 * q + j)
    mask_go_to(xp)

    @pl.when(jnp.logical_not(mask_self))
    def _():
        mask_go_to(c)

    @pl.when(mask_self)
    def _():
        maskg[mask_slot] = masks_s[c]

    rc(v2.at[k_core], v2.at[k_core], v_m.at[0], v_m.at[1], mate, c).start()
    row_send(p1g.at[r], p1g.at[r], p1_m)
    row_send(pcg.at[r], pcg.at[r], pc_m)
    tmask_self = c // 2 == r

    def tmask_go(q):
        rc(tmask_s.at[q], tmask.at[r], tm_m.at[0], tm_m.at[1], c // 2, 2 * q + h).start()

    for k in range(1, planes):
        tmask_go(lax.rem(z + k, planes))

    @pl.when(jnp.logical_not(tmask_self))
    def _():
        tmask_go(z)

    @pl.when(tmask_self)
    def _():
        tmask[r] = tmask_s[z]

    col_send(lambda q: emask_s.at[q], emask.at[c], em_m)
    row_send(fac, facg.at[r], f_m)
    emask[c] = emask_s[c]
    facg[r] = fac[...]

    def line_of(ref, q, way, lanes=slice(None)):
        return ref[q, way:way + 1, lanes].astype(f32)

    def describe_own(rb, slot):
        describe(gall.at[slot], slice(None), line_of(p0g, rb, 0), line_of(p0g, rb, 1), support_fine)
        gfine[:16, pl.ds(pl.multiple_of(slot * R0, R0), R0)] = gall[slot].astype(bf16)

    strip = pl.ds(pl.multiple_of(c * S0, S0), S0)
    describe_own(r, k_core)
    row_wait(p0g, p0_m)
    describe_own(mate, 1 - k_core)
    describe(gstrip, slice(None), line_of(p0g, yp, 0, strip), line_of(p0g, yp, 1, strip), support_fine)
    fbuf[0:16, :S0] = flipped_side(gall[k_core, :, strip])
    fbuf[0:16, S0:] = flipped_side(gstrip[...])

    def wait_slots(ref, n, m):
        slots = ref.at[pl.ds(0, n)]
        rc(slots, slots, m.at[0], m.at[1], mate, c).wait()

    @pl.when(mask_self)
    def _():
        wait_slots(maskg, nc - 1, a_m)

    @pl.when(jnp.logical_not(mask_self))
    def _():
        wait_slots(maskg, nc, a_m)

    for s in range(2):
        for q in range(planes):
            rows = maskg[s * planes + q].astype(f32)
            for i in range(I0):
                fbuf[16 + q * B0:16 + (q + 1) * B0, (s * I0 + i) * TILE:(s * I0 + i + 1) * TILE] = rows[i * B0:(i + 1) * B0]
    side_a[...] = fbuf[...].T.astype(bf16)

    def build(put, side, sides, depth, columns, step):
        def go(k):
            lanes = pl.ds(pl.multiple_of(k * step, step), step)
            put(lanes, phi_of(dot(side[:, :depth], sides[:depth, lanes])))
        each(0, columns // step, go)

    def put_a0(s):
        def put(lanes, value):
            a0[s, :, lanes] = value
        return put

    KA = 16 + 2 * T0
    def product(s, lo, hi):
        total = None
        for k in range(2):
            lanes = slice(k * R0, (k + 1) * R0)
            a0[s, lo:hi, lanes] = phi_of(dot(side_a[s * S0 + lo:s * S0 + hi, :KA], gfine[:KA, lanes]))
            if s == 1 and lo == 0 and k == 0:
                rc(v2.at[1 - k_core], v2.at[1 - k_core], v_m.at[0], v_m.at[1], mate, c).wait()
            term = dot(a0[s, lo:hi, lanes], v2[k])
            total = term if total is None else total + term
        return total

    def other_copy(i):
        rows = pl.ds(i * TILE, TILE)
        return rc(other_s.at[rows], other_r.at[rows], ot_m.at[0], ot_m.at[1 + i], yp, c)

    for i in range(I0):
        other_s[i * TILE:(i + 1) * TILE] = product(1, i * TILE, (i + 1) * TILE).astype(bf16)
        other_copy(i).start()
    acc = product(0, 0, S0)
    own_vals = v2[k_core, strip, :].astype(f32)
    x_slot, y_slot, d_slot = 2 * r + 1 - h, 2 * yp + h, 2 * diag + 1 - h

    def plane_gather(at, m, base, mate_sem):
        def send(slot, sem, rr, cc):
            rc(at(slot), at(slot), m.at[0], m.at[sem], rr, cc).start()

        def start():
            send(own_b, base + 2, diag, xp)
            send(own_b, base + 1, yp, c)
            send(own_b, base, r, xp)
            send(own_b, mate_sem, mate, c)

        def relay(slot, sem):
            rc(at(slot), at(slot), m.at[0], m.at[sem], mate, c).wait_recv()
            send(slot, mate_sem, mate, c)

        return (start, functools.partial(relay, x_slot, base), functools.partial(relay, y_slot, base + 1),
                functools.partial(relay, d_slot, base + 2))

    def plane_end(ref, m, mate_sem):
        part = ref.at[pl.ds(0, 4)]
        rc(part, part, m.at[0], m.at[mate_sem], mate, c).wait_recv()

    def plane_drain(ref, m, mate_sem):
        part = ref.at[pl.ds(0, 7)]
        rc(part, part, m.at[0], m.at[mate_sem], mate, c).wait_send()

    def all_send(src_of, dst, m):
        def go(k):
            q = lax.rem(c + k, nc)
            for j in range(nr):
                p = lax.rem(r + j, nr)
                rc(src_of(p * nc + q), dst, m.at[0], m.at[1], p, q).start()
        each(1, nc, go)
        for j in range(1, nr):
            p = lax.rem(r + j, nr)
            rc(src_of(p * nc + c), dst, m.at[0], m.at[1], p, c).start()

    def res_part(i):
        return plane_gather(lambda slot: resg.at[slot, pl.ds(i * TILE, TILE)], re_m, 1 + 3 * i, 7)

    res_parts = [res_part(i) for i in range(I0)]
    for i in range(I0):
        other_copy(i).wait_recv()
        rows = slice(i * TILE, (i + 1) * TILE)
        resg[own_b, rows] = (own_vals[rows] - (0.5 * g["scale_a0"]) * (acc[rows] + other_r[rows].astype(f32))).astype(bf16)
        res_parts[i][0]()
    PL = PT * TILE
    plane_lanes = pl.ds(pl.multiple_of(z * PL, PL), PL)
    row_wait(p1g, p1_m)
    for q in range(nr):
        describe(gpl, slice(q * PL, (q + 1) * PL), line_of(p0g, q, 0, plane_lanes), line_of(p0g, q, 1, plane_lanes), support_mid)
        lanes = slice(q * R1, (q + 1) * R1)
        describe(gmid, lanes, line_of(p1g, q, 0), line_of(p1g, q, 1), support_mid)
    gplane[:16] = gpl[...].astype(bf16)
    gmids[:16] = gmid[...].astype(bf16)

    @pl.when(tmask_self)
    def _():
        wait_slots(tmask, nr - 1, tm_m)

    @pl.when(jnp.logical_not(tmask_self))
    def _():
        wait_slots(tmask, nr, tm_m)

    block = pl.ds(pl.multiple_of(own_b * C1, C1), C1)
    fbuf[0:16, :C1] = flipped_side(gmid[:, block])
    fbuf[0:16, C1:] = fbuf[0:16, :C1]
    for q in range(nr):
        for j in range(B1):
            fbuf[16 + q * PT:16 + (q + 1) * PT, j * TILE:(j + 1) * TILE] = tmask[q, j * PT:(j + 1) * PT, :]
            at = B1 * PT + j * T1
            fbuf[16 + q * T1:16 + (q + 1) * T1, C1 + j * TILE:C1 + (j + 1) * TILE] = tmask[q, at:at + T1, :]
    side_t[...] = fbuf[...].T.astype(bf16)

    def put_e1t(lanes, value):
        e1t[:, lanes] = value

    build(put_e1t, side_t.at[pl.ds(0, C1)], gplane, 16 + T0, R0, 2048)
    row_wait(pcg, pc_m)
    row_wait(facg, f_m)
    def put_a1t(lanes, value):
        a1t[:, lanes] = value

    build(put_a1t, side_t.at[pl.ds(C1, C1)], gmids, 16 + NT1, N1, 1024)
    for k in range(1, 4):
        res_parts[0][k]()
    strips = []
    per = TILE // R2
    for lane in range(NT2):
        total = facg[lane * per].astype(f32)
        for k in range(1, per):
            total = total + facg[lane * per + k].astype(f32)
        strips.append(total)
    gtg[c] = jnp.concatenate(strips, axis=1).astype(bf16)
    col_send(lambda q: gtg.at[c], gtg.at[c], g_m)
    for t in range(NT2):
        line = pcg[per * t] + pcg[per * t + 1]
        describe(gcoarse, slice(t * TILE, (t + 1) * TILE), line[0:1], line[1:2], support_coarse)
    gcs[...] = gcoarse[...].astype(bf16)
    for q in range(nr):
        describe(gmid2, slice(q * R1, (q + 1) * R1), line_of(p1g, q, 0), line_of(p1g, q, 1), support_coarse)
    wide = fbuf.shape[1]
    for q in range(N1 // wide):
        fbuf[0:16] = flipped_side(gmid2[:, q * wide:(q + 1) * wide])
        side_m[...] = fbuf[...].T.astype(bf16)
        e2t[q * wide:(q + 1) * wide] = phi_of(dot(side_m[:, :16], gcs[...]))
    for k in range(1, 4):
        res_parts[1][k]()
    restricted = jnp.zeros((C1, resg.shape[-1]), f32)
    square = jnp.zeros((16, resg.shape[-1]), f32)

    def restrict(slot):
        strip_data = resg[slot]
        held = strip_data.astype(f32)
        return (dot(e1t[:, pl.ds(pl.multiple_of(slot * S0, S0), S0)], strip_data),
                jnp.sum((held * held).reshape(S0 // 16, 16, -1), axis=0))

    for slot in (own_b, x_slot, y_slot, d_slot):
        term = restrict(slot)
        restricted, square = restricted + term[0], square + term[1]
    plane_end(resg, re_m, 7)
    for slot in (2 * mate + h, 2 * mate + 1 - h, 2 * diag + h, 2 * yp + 1 - h):
        term = restrict(slot)
        restricted, square = restricted + term[0], square + term[1]
    restricted = g["scale_e1"] * restricted
    for q in range(planes):
        part_buf[q] = restricted[q * Q1:(q + 1) * Q1].astype(bf16)

    def z_send(src_of, dst, m):
        for q in far_first:
            rc(src_of(q), dst, m.at[0], m.at[1], r, 2 * q + h).start()

    z_send(lambda q: part_buf.at[q], rsin.at[z], rs_m)
    rsin[z] = part_buf[z]
    square_g[z] = square.astype(bf16)
    turned_w = g["scale_e2"] * (e2t[block, :].astype(f32) - (0.5 * g["scale_a1"]) * dot(a1t[...], e2t[...]))
    w_high, w_low = halves(turned_w.T)
    for k, w in enumerate((w_high, w_low, w_high)):
        wcat[:, k * C1:(k + 1) * C1] = w

    part_high, part_low = halves(restricted)
    part = dot(wcat[...], jnp.concatenate([part_high, part_high, part_low], axis=0))
    csend[...] = part.reshape(D, CR, -1).astype(bf16)
    all_send(lambda q: csend.at[q], crecv.at[d], cr_m)
    crecv[d] = csend[d]
    wait_slots(emask, nc - 1, em_m)
    describe(gstrip, slice(None), line_of(p0g, r, 0, strip), line_of(p0g, r, 1, strip), support_mid)
    fbuf[0:16, :S0] = flipped_side(gstrip[...])
    for q in range(nc):
        for i in range(I0):
            fbuf[16 + q * B1:16 + (q + 1) * B1, i * TILE:(i + 1) * TILE] = emask[q, i * B1:(i + 1) * B1, :]
    side_e[...] = fbuf[:, :S0].T.astype(bf16)

    def put_e1own(lanes, value):
        e1own[:, lanes] = value

    build(put_e1own, side_e, gmids, 16 + NT1, N1, 2048)
    fine_gain = g["scale_e1"]
    wait_slots(rsin, planes - 1, rs_m)
    total = rsin[0].astype(f32)
    for q in range(1, planes):
        total = total + rsin[q].astype(f32)
    q_high = total.astype(bf16)
    mida[own_b, z] = q_high
    own_q = mida.at[own_b, z]
    rank = jnp.where((z == 0) | (z == planes - 1), 3, 2)
    for q, sem in ((far_first[0], rank), (far_first[1], rank), (near_z, 1)):
        rc(own_q, own_q, mz_m.at[0], mz_m.at[sem], r, 2 * q + h).start()
    order = (z,) + far_first[::-1]

    def batch(k):
        return plane_gather(lambda slot: mida.at[slot, order[k]], ma_m, 1 + 3 * k, 13)

    batches = [batch(k) for k in range(planes)]
    batches[0][0]()
    z_send(lambda q: square_g.at[z], square_g.at[z], sq_m)
    wait_slots(gtg, nc - 1, g_m)
    gt = gtg[...].reshape(N2, N2)
    gg_high, gg_low = halves(dot(gt.astype(f32).T.astype(bf16), gt))
    zcat[S0 + C1:, :N2] = gg_high
    zcat[S0 + C1:, N2:] = gg_low
    h_high, h_low = halves((fine_gain * g["scale_e2"]) * dot(e1own[...], e2t[...]))
    steps = (dot(h_high, gg_high) + dot(h_low, gg_high) + dot(h_high, gg_low),)
    rows_c = e2t[pl.ds(pl.multiple_of(c * C1, C1), C1), :]
    steps += (g["scale_e2"] * (dot(rows_c, gg_high) + dot(rows_c, gg_low)),)
    for k, step in enumerate(steps):
        high, low = halves(step)
        zcat[k * C1:(k + 1) * C1, :N2] = high
        zcat[k * C1:(k + 1) * C1, N2:] = low

    def z_take(k):
        piece = mida.at[own_b, order[k]]
        rc(piece, piece, mz_m.at[0], mz_m.at[k], mate, c).wait_recv()
        batches[k][0]()

    wait_slots(crecv, D - 1, cr_m)
    cg[d] = jnp.sum(crecv[...].astype(f32), axis=0).astype(bf16)
    all_send(lambda q: cg.at[d], cg.at[d], ca_m)
    for k in range(1, 4):
        batches[0][k]()
    z_take(1)
    z_take(2)
    z_take(3)
    wait_slots(square_g, planes - 1, sq_m)
    norm_o[...] = jnp.broadcast_to(jnp.sum(square_g[...].astype(f32), keepdims=True).reshape(1, 1) * g["norm_scale"], norm_o.shape)
    for b in batches[1:]:
        for k in range(1, 4):
            b[k]()
    wait_slots(cg, D - 1, ca_m)
    cd = cg[...].astype(f32).reshape(N2, -1).astype(bf16)
    both = jnp.concatenate([cd, cd], axis=0)
    coarse_o[...] = dot(zcat[pl.ds(pl.multiple_of(S0 + C1 + r * R2, R2), R2), :], both)
    step = dot(zcat[:S0 + C1, :], both)
    def prolong(slot):
        return dot(e1own[:, pl.ds(pl.multiple_of(slot * C1, C1), C1)], mida[slot].reshape(C1, -1))

    base = prolong(own_b) + prolong(x_slot) + prolong(y_slot) + prolong(d_slot)
    plane_end(mida, ma_m, 13)
    for slot in (2 * mate + h, 2 * mate + 1 - h, 2 * diag + h, 2 * yp + 1 - h):
        base = base + prolong(slot)
    mid_o[...] = 0.5 * mida[c].astype(f32).reshape(C1, -1) + step[S0:]
    fine_o[...] = 0.5 * own_vals + (0.5 * fine_gain) * base + step[:S0]
    rc(other_s, other_r, ot_m.at[0], ot_m.at[1], yp, c).wait_send()
    plane_drain(resg, re_m, 7)
    plane_drain(mida, ma_m, 13)
    held_z = mida.at[own_b, pl.ds(0, planes - 1)]
    rc(held_z, held_z, mz_m.at[0], mz_m.at[1], mate, c).wait_send()


def finish_kernel(fine, mid, coarse, norm, fine_o, mid_o, coarse_o, norm_o):
    fine_o[...] = fine[...]
    mid_o[...] = mid[...]
    coarse_o[...] = coarse[...]
    norm_o[...] = norm[0:1, 0:1]


def fits(nr, nc, R0, R1, R2):
    if nr != 4 or nc != 8:
        return False
    if R0 != R1 * nr or R0 != 2 * nc * TILE or 2 * R2 != TILE:
        return False
    return True


def fused(values, points0, points1, points2, tiles_a0, tiles_e1, tiles_a1, factor):
    nr, nc = lax.axis_size("row"), lax.axis_size("col")
    R0, R1, R2 = points0.shape[1], points1.shape[1], points2.shape[1]
    F = values.shape[-1]
    if not fits(nr, nc, R0, R1, R2) or F != TILE:
        return per_device(values, points0, points1, points2, tiles_a0, tiles_e1, tiles_a1, factor)
    D, N2 = nr * nc, nr * R2
    T0, T1 = R0 // TILE, R1 // TILE
    B0, B1 = R0 * nr // nc // TILE, R1 * nr // nc // TILE
    S0 = R0 // nc
    I0 = S0 // TILE
    C1, CR, Q1 = B1 * TILE, N2 // D, R1 * nr // nc // nr
    g = dict(nr=nr, nc=nc, R0=R0, R1=R1, R2=R2, N2=N2,
             scale_a0=(R0 / (nc * tiles_a0.shape[-1] * TILE * TILE)) ** 0.5,
             scale_e1=(R0 / (nc * tiles_e1.shape[-1] * TILE * TILE)) ** 0.5,
             scale_a1=(R1 / (nc * tiles_a1.shape[-1] * TILE * TILE)) ** 0.5,
             scale_e2=(1.0 / (R1 * nr)) ** 0.5,
             norm_scale=1.0 / (R0 * nr * F))
    f32, bf16, i32 = jnp.float32, jnp.bfloat16, jnp.int32
    V = pltpu.VMEM
    dma = pltpu.SemaphoreType.DMA
    wide = N2 // nc
    N1 = nr * R1
    planes = nc // 2
    scratch = [
        V(tiles_a0.shape, i32), V(tiles_e1.shape, i32), V(tiles_a1.shape, i32), V((wide, R2), bf16), V(points2.shape, bf16),
        V((2, R0, F), bf16), V((nr,) + points0.shape, bf16), V((nr,) + points1.shape, bf16), V((nr, 8, TILE), f32),
        V((nc, I0 * B0, TILE), bf16), V((nc, 8, TILE), f32), V((nr, 16, TILE), f32),
        V((nc, I0 * B0, TILE), bf16), V((nc, 8, TILE), f32), V((planes, 16, TILE), f32),
        V((wide, TILE), bf16), V((nr, wide, TILE), bf16), V((nc, wide, N2), bf16),
        V((2, 16, R0), f32), V((16, S0), f32), V((16, R0), f32), V((16, N1), f32), V((16, N1), f32), V((16, N2), f32),
        V((16 + 2 * T0, 2 * R0), bf16), V((16 + T0, R0), bf16), V((16 + nr * T1, N1), bf16), V((16, N2), bf16),
        V((TILE, 2 * S0), f32), V((2 * S0, TILE), bf16), V((S0, TILE), bf16), V((2 * S0, TILE), bf16),
        V((8, TILE), bf16), V((2 * S0, TILE), bf16),
        V((2, S0, 2 * R0), bf16), V((S0, N1), bf16), V((C1, R0), bf16), V((N1, N2), bf16), V((C1, N1), bf16),
        V((S0, F), bf16), V((S0, F), bf16), V((nc, S0, F), bf16),
        V((planes, Q1, F), bf16), V((planes, Q1, F), bf16), V((planes, 16, F), bf16), V((nc, planes, Q1, F), bf16),
        V((D, CR, F), bf16), V((D, CR, F), bf16), V((D, CR, F), bf16), V((N2, 3 * C1), bf16),
        V((S0 + C1 + N2, 2 * N2), bf16),
    ]
    for n in (8, 2, 2, 2, 2, 2, 2, 2, 2, 2, 1 + I0, 2 + 3 * I0, 2, 2, 4, 14, 2, 2):
        scratch += [dma((n,))]
    vm = pl.BlockSpec(memory_space=pltpu.VMEM)
    shapes = ((S0, F), (C1, F), (R2, F))
    parts = pl.pallas_call(
        functools.partial(cycle_kernel, g),
        out_shape=tuple(jax.ShapeDtypeStruct(s, f32) for s in shapes + ((8, TILE),)),
        in_specs=[pl.BlockSpec(memory_space=pltpu.HBM)] * 8,
        out_specs=[vm] * 4,
        scratch_shapes=scratch,
        compiler_params=pltpu.CompilerParams(collective_id=0, has_side_effects=True, vmem_limit_bytes=48 << 20),
    )(*[pltpu.with_memory_space_constraint(x, pltpu.HBM) for x in (
        values, points0, points1, points2, tiles_a0, tiles_e1, tiles_a1, factor.T)])
    fine, mid, coarse, norm = pl.pallas_call(
        finish_kernel,
        grid=(1,),
        out_shape=tuple(jax.ShapeDtypeStruct(s, f32) for s in shapes + ((1, 1),)),
        in_specs=[vm] * 4,
        out_specs=[pl.BlockSpec(s, lambda i: (0, 0)) for s in shapes + ((1, 1),)],
        compiler_params=pltpu.CompilerParams(vmem_limit_bytes=4 << 20),
    )(*parts)
    return (fine, mid, coarse, norm.reshape(1))


def solution(mesh):
    return jax.shard_map(
        fused,
        mesh=mesh,
        in_specs=(
            P("row", None),
            P(None, "row"),
            P(None, "row"),
            P(None, "row"),
            P("row", "col", None, None),
            P("row", "col", None, None),
            P("row", "col", None, None),
            P("row", "col"),
        ),
        out_specs=(P(("row", "col"), None), P("col", None), P("row", None), P()),
        check_vma=False,
    )
```
